128 devices in a mesh: batch: 1, seq: 128 (over z, y, x, core).
Axes of the slice: x: 4, y: 4, z: 4, core: 2. Of those that a mesh axis runs over, the one named last changes fastest.
Arguments:
- tokens: bfloat16 [32768, 2048], P(('batch', 'seq'))
- w_query: bfloat16 [2048, 2048], replicated
- w_key: bfloat16 [2048, 2048], replicated
- w_value: bfloat16 [2048, 2048], replicated
- w_out: bfloat16 [2048, 2048], replicated
- rand_idx: int32 [512, 3], P(('batch', 'seq'))
Outputs:
- output: bfloat16 [32768, 2048], P(('batch', 'seq'))
All inputs are finite; a program needn't handle non-finite values.
Results may differ from the reference program's by a relative error of at most 0.00340356.
Values are sent between devices in bfloat16 or wider.
A program may use at most 1 GiB of HBM per device.

```python
import jax
import jax.numpy as jnp
from jax import lax

D = 2048
HEADS = 32
HEAD = 64
BLOCK_LEN = 64
RAND_BLOCKS = 3
GLOBAL = 2
HOT_BLOCKS = 12
SEQ_LEN = 32768

N_BLOCKS = SEQ_LEN // BLOCK_LEN
ATTN_WIDTH = HEADS * HEAD
KEY_COUNT = (3 + GLOBAL + RAND_BLOCKS) * BLOCK_LEN


def draw_rand_idx(idx_key):
    hot_key, score_key = jax.random.split(idx_key)
    hot_ids = jax.random.permutation(hot_key, N_BLOCKS - GLOBAL)[:HOT_BLOCKS] + GLOBAL
    row_ids = jnp.arange(N_BLOCKS)
    base_score = jax.random.randint(score_key, (N_BLOCKS, HOT_BLOCKS), 0, 65536, dtype=jnp.int32)
    near_row = jnp.abs(hot_ids[None, :] - row_ids[:, None]) <= 1
    favored = jnp.arange(HOT_BLOCKS)[None, :] == (row_ids % HOT_BLOCKS)[:, None]
    full_score = base_score + jnp.where(near_row, 0, 262144) + jnp.where(favored, 131072, 0)
    full_score = full_score * HOT_BLOCKS + jnp.arange(HOT_BLOCKS)[None, :]
    top_vals, pick_cols = lax.top_k(full_score, RAND_BLOCKS)
    return hot_ids[pick_cols].astype(jnp.int32)


def setup_inputs(seed: int = 0, part: int = 0) -> dict:
    part_key = jax.random.fold_in(jax.random.key(seed), part)
    token_key, idx_key = jax.random.split(part_key)
    wq_key, wk_key, wv_key, wo_key = jax.random.split(jax.random.key(seed + 1), 4)
    tokens = jax.random.normal(token_key, (SEQ_LEN, D), jnp.float32).astype(jnp.bfloat16)
    in_scale = D ** -0.5
    out_scale = (KEY_COUNT / (3.0 * ATTN_WIDTH)) ** 0.5
    w_query = (jax.random.normal(wq_key, (D, ATTN_WIDTH), jnp.float32) * in_scale).astype(jnp.bfloat16)
    w_key = (jax.random.normal(wk_key, (D, ATTN_WIDTH), jnp.float32) * in_scale).astype(jnp.bfloat16)
    w_value = (jax.random.normal(wv_key, (D, ATTN_WIDTH), jnp.float32) * in_scale).astype(jnp.bfloat16)
    w_out = (jax.random.normal(wo_key, (D, ATTN_WIDTH), jnp.float32) * out_scale).astype(jnp.bfloat16)
    rand_idx = draw_rand_idx(idx_key)
    return {"tokens": tokens, "w_query": w_query, "w_key": w_key, "w_value": w_value, "w_out": w_out, "rand_idx": rand_idx}


def reference(tokens, w_query, w_key, w_value, w_out, rand_idx):
    def project(weight):
        return jnp.dot(tokens, weight, preferred_element_type=jnp.float32).astype(jnp.bfloat16)

    queries = project(w_query).reshape(N_BLOCKS, BLOCK_LEN, HEADS, HEAD)
    keys_all = project(w_key).reshape(N_BLOCKS, BLOCK_LEN, HEADS, HEAD)
    values_all = project(w_value).reshape(N_BLOCKS, BLOCK_LEN, HEADS, HEAD)

    def sparse_row(row_args):
        row_id, rand_row = row_args
        block_ids = jnp.concatenate([jnp.stack([row_id - 1, row_id, jnp.minimum(row_id + 1, N_BLOCKS - 1)]), jnp.arange(GLOBAL), rand_row])
        key_valid = jnp.concatenate([jnp.stack([row_id - 1 >= GLOBAL, row_id >= 0, row_id + 1 < N_BLOCKS]), jnp.arange(GLOBAL + RAND_BLOCKS) >= 0])
        key_rows = keys_all[block_ids].reshape(KEY_COUNT, HEADS, HEAD).astype(jnp.float32)
        val_rows = values_all[block_ids].reshape(KEY_COUNT, HEADS, HEAD).astype(jnp.float32)
        scores = jnp.einsum("qhd,khd->hqk", queries[row_id].astype(jnp.float32), key_rows) * HEAD ** -0.5
        scores = jnp.where(jnp.repeat(key_valid, BLOCK_LEN)[None, None, :], scores, -1e30)
        attn_probs = jax.nn.softmax(scores, axis=-1).astype(jnp.bfloat16).astype(jnp.float32)
        return jnp.einsum("hqk,khd->qhd", attn_probs, val_rows).astype(jnp.bfloat16)

    sparse_out = lax.map(sparse_row, (jnp.arange(GLOBAL, N_BLOCKS), rand_idx[GLOBAL:]))
    sparse_out = sparse_out.reshape((N_BLOCKS - GLOBAL) * BLOCK_LEN, ATTN_WIDTH)

    glob_q = jnp.moveaxis(queries[:GLOBAL].reshape(GLOBAL * BLOCK_LEN, HEADS, HEAD), 1, 0).astype(jnp.float32)
    head_keys = jnp.moveaxis(keys_all.reshape(SEQ_LEN, HEADS, HEAD), 1, 0)
    head_vals = jnp.moveaxis(values_all.reshape(SEQ_LEN, HEADS, HEAD), 1, 0)

    def global_head(head_args):
        q_head, k_head, v_head = head_args
        scores = jnp.dot(q_head, k_head.astype(jnp.float32).T) * HEAD ** -0.5
        attn_probs = jax.nn.softmax(scores, axis=-1).astype(jnp.bfloat16).astype(jnp.float32)
        return jnp.dot(attn_probs, v_head.astype(jnp.float32)).astype(jnp.bfloat16)

    glob_out = lax.map(global_head, (glob_q, head_keys, head_vals))
    glob_out = jnp.moveaxis(glob_out, 0, 1).reshape(GLOBAL * BLOCK_LEN, ATTN_WIDTH)
    attn_all = jnp.concatenate([glob_out, sparse_out], axis=0)
    return jnp.dot(attn_all, w_out.T, preferred_element_type=jnp.float32).astype(jnp.bfloat16)
```

```python
import jax
import jax.numpy as jnp
from jax import lax
from jax.experimental import pallas as pl
from jax.experimental.pallas import tpu as pltpu
from jax.sharding import PartitionSpec as P

HEAD_DIM = 64
GLOBAL_BLOCKS = 2
HOT = 12
SLOTS = 16
BLK = 64
WIDTH = 2048
HALF = 1024
CHIPS = 64
NEG = -1e30
MESH = pl.DeviceIdType.MESH
VMEM = pltpu.VMEM
ANY = pl.ANY
PARTS = ((0, 768, (0, 1, 2)), (768, 640, (1, 2, 0)), (1408, 640, (2, 0, 1)))


def vspec():
    return pl.BlockSpec(memory_space=VMEM)


def params(effects=True, mib=60):
    return pltpu.CompilerParams(has_side_effects=effects, vmem_limit_bytes=mib * 1024 * 1024)


def where_am_i():
    dev = lax.axis_index("seq")
    return dev, dev // 2, dev % 2


def scatter_kernel(xs_ref, x_ref, idx_ref, recv_ref, xc_ref, idxall_ref, s_send, s_recv, i_send, i_recv, x_send, x_recv, h_send, h_recv, loc):
    dev, chip, core = where_am_i()

    def row_copy(dst_chip, slot):
        return pltpu.make_async_remote_copy(
            src_ref=xs_ref.at[dst_chip], dst_ref=recv_ref.at[slot], send_sem=s_send, recv_sem=s_recv.at[slot],
            device_id={"seq": 2 * dst_chip + core}, device_id_type=MESH)

    def idx_copy(dst, slot):
        return pltpu.make_async_remote_copy(
            src_ref=idx_ref, dst_ref=idxall_ref.at[slot], send_sem=i_send, recv_sem=i_recv.at[slot],
            device_id={"seq": dst}, device_id_type=MESH)

    own = pl.ds(1 + 4 * core, 4)
    part = pltpu.make_async_remote_copy(
        src_ref=x_ref, dst_ref=xc_ref.at[own], send_sem=x_send, recv_sem=x_recv,
        device_id={"seq": dev + 1 - 2 * core}, device_id_type=MESH)
    part.start()

    def start_idx(i, carry):
        idx_copy(dev ^ i, dev).start()
        return carry
    lax.fori_loop(1, 128, start_idx, 0)

    def start_row(i, carry):
        row_copy(chip ^ i, chip).start()
        return carry
    lax.fori_loop(1, CHIPS, start_row, 0)

    nbr = lax.rem(chip + 2 * core - 1 + CHIPS, CHIPS)
    halos = [pltpu.make_async_remote_copy(
        src_ref=x_ref.at[3 * core], dst_ref=xc_ref.at[9 * (1 - core)], send_sem=h_send.at[k], recv_sem=h_recv.at[1 - core],
        device_id={"seq": 2 * nbr + k}, device_id_type=MESH) for k in range(2)]
    for h in halos:
        h.start()
    locs = [pltpu.make_async_copy(xs_ref.at[chip], recv_ref.at[chip], loc.at[0]),
            pltpu.make_async_copy(x_ref, xc_ref.at[own], loc.at[1]),
            pltpu.make_async_copy(idx_ref, idxall_ref.at[dev], loc.at[2])]
    for l in locs:
        l.start()
    for l in locs:
        l.wait()
    part.wait_send()
    other = pl.ds(5 - 4 * core, 4)
    pltpu.make_async_remote_copy(
        src_ref=x_ref, dst_ref=xc_ref.at[other], send_sem=x_send, recv_sem=x_recv,
        device_id={"seq": dev + 1 - 2 * core}, device_id_type=MESH).wait_recv()
    for k in range(2):
        halos[k].wait_send()
        pltpu.make_async_remote_copy(
            src_ref=x_ref.at[0], dst_ref=xc_ref.at[9 * k], send_sem=h_send.at[0], recv_sem=h_recv.at[k],
            device_id={"seq": 2 * nbr + k}, device_id_type=MESH).wait_recv()

    def wait_idx(i, carry):
        idx_copy(dev ^ i, dev ^ i).wait()
        return carry
    lax.fori_loop(1, 128, wait_idx, 0)

    def wait_row(i, carry):
        row_copy(chip ^ i, chip ^ i).wait()
        return carry
    lax.fori_loop(1, CHIPS, wait_row, 0)


def scatter_rows(xs, x, idx):
    return pl.pallas_call(
        scatter_kernel,
        out_shape=(jax.ShapeDtypeStruct((CHIPS, BLK, 128), jnp.bfloat16),
                   jax.ShapeDtypeStruct((10, BLK, WIDTH), jnp.bfloat16),
                   jax.ShapeDtypeStruct((128, 1, 128), jnp.int32)),
        in_specs=[vspec()] * 3, out_specs=(vspec(),) * 3,
        scratch_shapes=[pltpu.SemaphoreType.DMA, pltpu.SemaphoreType.DMA((CHIPS,)),
                        pltpu.SemaphoreType.DMA, pltpu.SemaphoreType.DMA((128,)),
                        pltpu.SemaphoreType.DMA, pltpu.SemaphoreType.DMA,
                        pltpu.SemaphoreType.DMA((2,)), pltpu.SemaphoreType.DMA((2,)), pltpu.SemaphoreType.DMA((3,))],
        compiler_params=params(), name="scatter_rows",
    )(xs, x, idx)


def project_kernel(core_ref, x_ref, wq_ref, wk_ref, wv_ref, q_ref, k_ref, v_ref):
    q_ref[...] = (jnp.dot(x_ref[64:576, :], wq_ref[...], preferred_element_type=jnp.float32)).astype(jnp.bfloat16)
    k_ref[...] = jnp.dot(x_ref[...], wk_ref[...], preferred_element_type=jnp.float32).astype(jnp.bfloat16)
    v_ref[...] = jnp.dot(x_ref[...], wv_ref[...], preferred_element_type=jnp.float32).astype(jnp.bfloat16)


def project_rows(core, xc, wq, wk, wv):
    tile = 256
    steps = HALF // tile
    wspec = pl.BlockSpec((WIDTH, tile), lambda j, c: (0, c[0] * steps + j))
    return pl.pallas_call(
        project_kernel,
        grid_spec=pltpu.PrefetchScalarGridSpec(
            num_scalar_prefetch=1, grid=(steps,),
            in_specs=[pl.BlockSpec((640, WIDTH), lambda j, c: (0, 0)), wspec, wspec, wspec],
            out_specs=[pl.BlockSpec((512, tile), lambda j, c: (0, j)),
                       pl.BlockSpec((640, tile), lambda j, c: (0, j)),
                       pl.BlockSpec((640, tile), lambda j, c: (0, j))]),
        out_shape=(jax.ShapeDtypeStruct((512, HALF), jnp.bfloat16),
                   jax.ShapeDtypeStruct((640, HALF), jnp.bfloat16),
                   jax.ShapeDtypeStruct((640, HALF), jnp.bfloat16)),
        compiler_params=params(False), name="project_rows",
        cost_estimate=pl.CostEstimate(flops=2 * 1792 * WIDTH * HALF, bytes_accessed=20 << 20, transcendentals=0),
    )(core, xc, wq, wk, wv)


def gather_kernel(sel_ref, wq_ref, wk_ref, wv_ref, g_ref, w_buf, other, w_sem, p_sem, g_send, g_recv):
    dev, chip, core = where_am_i()
    cx, cy, cz = chip % 4, (chip // 4) % 4, chip // 16
    loads = [pltpu.make_async_copy(w.at[:, pl.ds(core * HALF, HALF)], w_buf.at[i], w_sem.at[i])
             for i, w in enumerate((wk_ref, wv_ref, wq_ref))]
    for l in loads:
        l.start()
    swap = pltpu.make_async_remote_copy(
        src_ref=sel_ref, dst_ref=other, send_sem=p_sem.at[0], recv_sem=p_sem.at[1],
        device_id={"seq": dev + 1 - 2 * core}, device_id_type=MESH)
    swap.start()
    swap.wait()
    rows = sel_ref[...] + other[...]
    out = []
    for i in range(3):
        loads[i].wait()
        out.append(jnp.dot(rows, w_buf[i], preferred_element_type=jnp.float32))
    kv = jnp.concatenate([out[0], out[1]], axis=1)
    glob_q = jnp.concatenate([out[2][0:1], out[2][1:2]], axis=1)
    row_id = lax.broadcasted_iota(jnp.int32, (SLOTS, WIDTH), 0)
    kv = jnp.where(row_id == 14, jnp.broadcast_to(glob_q, (SLOTS, WIDTH)), kv)
    g_ref[cz, cy, cx] = kv.astype(jnp.bfloat16)

    coord = (cx, cy, cz)
    scale = (1, 4, 16)

    def block(axes_done, at, cols):
        idx = []
        for axis in (2, 1, 0):
            idx.append(slice(None) if axis in axes_done else at[axis])
        return tuple(idx) + (slice(None), cols)

    def copies(part, stage, receive):
        start, size, order = PARTS[part]
        axis = order[stage]
        out = []
        for k in (1, 2, 3):
            to = lax.rem(coord[axis] + k, 4)
            frm = lax.rem(coord[axis] + 4 - k, 4)
            at = list(coord)
            if receive:
                at[axis] = frm
            ref = g_ref.at[block(order[:stage], at, slice(start, start + size))]
            out.append(pltpu.make_async_remote_copy(
                src_ref=ref, dst_ref=ref, send_sem=g_send.at[part, stage, k - 1], recv_sem=g_recv.at[part, stage, k - 1],
                device_id={"seq": dev + 2 * scale[axis] * (to - coord[axis])}, device_id_type=MESH))
        return out

    for stage in range(3):
        for part in range(3):
            if stage:
                for c in copies(part, stage - 1, True):
                    c.wait_recv()
            for c in copies(part, stage, False):
                c.start()
    for part in range(3):
        for c in copies(part, 2, True):
            c.wait_recv()
    for stage in range(3):
        for part in range(3):
            for c in copies(part, stage, False):
                c.wait_send()


def gather_rows(sel, wq, wk, wv):
    anyspec = pl.BlockSpec(memory_space=ANY)
    return pl.pallas_call(
        gather_kernel,
        out_shape=jax.ShapeDtypeStruct((4, 4, 4, SLOTS, WIDTH), jnp.bfloat16),
        in_specs=[vspec(), anyspec, anyspec, anyspec], out_specs=vspec(),
        scratch_shapes=[VMEM((3, WIDTH, HALF), jnp.bfloat16), VMEM((SLOTS, WIDTH), jnp.bfloat16),
                        pltpu.SemaphoreType.DMA((3,)), pltpu.SemaphoreType.DMA((2,)),
                        pltpu.SemaphoreType.DMA((3, 3, 3)), pltpu.SemaphoreType.DMA((3, 3, 3))],
        compiler_params=params(), name="gather_rows",
    )(sel, wq, wk, wv)


def split_heads(pair, rows):
    lane = lax.broadcasted_iota(jnp.int32, (rows, 128), 1)
    zero = jnp.zeros_like(pair)
    return jnp.concatenate([jnp.where(lane < HEAD_DIM, pair, zero), jnp.where(lane < HEAD_DIM, zero, pair)], axis=0)


def join_heads(out, rows):
    lane = lax.broadcasted_iota(jnp.int32, (rows, 128), 1)
    return jnp.where(lane < HEAD_DIM, out[:rows], out[rows:])


def attention_kernel(info_ref, q_ref, k_ref, v_ref, g_ref, o_ref, part_ref, hot):
    nt = (((1,), (1,)), ((), ()))
    row = lax.broadcasted_iota(jnp.int32, (256, 256), 0)
    col = lax.broadcasted_iota(jnp.int32, (256, 256), 1)
    perm = jnp.where(col == (row % 16) * 16 + row // 16, 1.0, 0.0).astype(jnp.bfloat16)

    def unpack(step, carry):
        z = step // 8
        cols = pl.ds(pl.multiple_of((step % 8) * 256, 256), 256)
        rows = g_ref[pl.ds(pl.multiple_of(z * 256, 256), 256), cols]
        moved = jnp.dot(perm, rows, preferred_element_type=jnp.float32).astype(jnp.bfloat16)
        for s in range(SLOTS):
            hot[pl.ds(pl.multiple_of(s * BLK + z * 16, 16), 16), cols] = moved[s * 16:s * 16 + 16]
        return carry
    lax.fori_loop(0, 32, unpack, 0)

    def one_block(b, carry):
        slots = [pl.multiple_of(info_ref[b * 3 + t] * BLK, BLK) for t in range(3)]
        left_bad = info_ref[32 + b]
        right_bad = info_ref[40 + b]
        key = lax.broadcasted_iota(jnp.int32, (1, 256), 1)
        bias = jnp.where((key < BLK) & (left_bad > 0), NEG, 0.0) + jnp.where((key >= 2 * BLK) & (key < 3 * BLK) & (right_bad > 0), NEG, 0.0)
        base = pl.multiple_of(b * BLK, BLK)
        for j in range(8):
            cols = slice(j * 128, j * 128 + 128)
            vcols = slice(HALF + j * 128, HALF + j * 128 + 128)
            queries = split_heads(q_ref[pl.ds(base, BLK), cols], BLK) * jnp.bfloat16(0.125)
            keys = jnp.concatenate([k_ref[pl.ds(base, 3 * BLK), cols], hot[0:2 * BLK, cols]] + [hot[pl.ds(s, BLK), cols] for s in slots], axis=0)
            vals = jnp.concatenate([v_ref[pl.ds(base, 3 * BLK), cols], hot[0:2 * BLK, vcols]] + [hot[pl.ds(s, BLK), vcols] for s in slots], axis=0)
            scores = lax.dot_general(queries, keys, nt, preferred_element_type=jnp.float32)
            scores = jnp.concatenate([scores[:, :256] + bias, scores[:, 256:]], axis=1)
            top = jnp.max(scores, axis=1, keepdims=True)
            probs = jnp.exp(scores - top)
            probs = probs * (1.0 / jnp.sum(probs, axis=1, keepdims=True))
            out = jnp.dot(probs.astype(jnp.bfloat16), vals, preferred_element_type=jnp.float32)
            o_ref[pl.ds(base, BLK), cols] = join_heads(out, BLK).astype(jnp.bfloat16)
        return carry
    lax.fori_loop(0, 8, one_block, 0)

    lane = lax.broadcasted_iota(jnp.int32, (128, 128), 1)
    stats = None
    for j in range(8):
        cols = slice(j * 128, j * 128 + 128)
        vcols = slice(HALF + j * 128, HALF + j * 128 + 128)
        glob = jnp.concatenate([hot[14 * BLK:15 * BLK, cols], hot[14 * BLK:15 * BLK, vcols]], axis=0)
        queries = split_heads(glob, 128) * jnp.bfloat16(0.125)
        scores = lax.dot_general(queries, k_ref[BLK:9 * BLK, cols], nt, preferred_element_type=jnp.float32)
        top = jnp.max(scores, axis=1, keepdims=True)
        probs = jnp.exp(scores - top)
        total = jnp.sum(probs, axis=1, keepdims=True)
        out = jnp.dot(probs.astype(jnp.bfloat16), v_ref[BLK:9 * BLK, cols], preferred_element_type=jnp.float32)
        g, t = j // 2, 2 * (j % 2)
        part_ref[:, 384 * g + 64 * t:384 * g + 64 * t + 128] = join_heads(out, 128)
        if t == 0:
            stats = jnp.zeros((128, 128), jnp.float32)
        for h in range(2):
            rows = slice(128 * h, 128 * h + 128)
            stats = jnp.where(lane == t + h, total[rows], stats)
            stats = jnp.where(lane == 4 + t + h, top[rows], stats)
        if t:
            part_ref[:, 384 * g + 256:384 * g + 384] = stats


def attention(info, q, k, v, g):
    return pl.pallas_call(
        attention_kernel,
        grid_spec=pltpu.PrefetchScalarGridSpec(
            num_scalar_prefetch=1, grid=(1,),
            in_specs=[vspec()] * 4, out_specs=[vspec()] * 2,
            scratch_shapes=[VMEM((SLOTS * BLK, WIDTH), jnp.bfloat16)]),
        out_shape=(jax.ShapeDtypeStruct((512, HALF), jnp.bfloat16), jax.ShapeDtypeStruct((128, 1536), jnp.float32)),
        compiler_params=params(False), name="attention",
        cost_estimate=pl.CostEstimate(flops=2 << 30, bytes_accessed=16 << 20, transcendentals=10 << 20),
    )(info, q, k, v, g)


def combine_kernel(part_ref, o_ref, full_ref, recv, glob, piece, c_send, c_recv, o_send, o_recv, g_send, g_recv, loc):
    dev, chip, core = where_am_i()

    def part_copy(dst_chip, slot):
        rows = pl.ds(pl.multiple_of((dst_chip % 16) * 8, 8), 8)
        cols = pl.ds(pl.multiple_of((dst_chip // 16) * 384, 128), 384)
        return pltpu.make_async_remote_copy(
            src_ref=part_ref.at[rows, cols], dst_ref=recv.at[slot], send_sem=c_send, recv_sem=c_recv.at[slot],
            device_id={"seq": 2 * dst_chip + core}, device_id_type=MESH)

    def start(i, carry):
        part_copy(chip ^ i, chip).start()
        return carry
    lax.fori_loop(1, CHIPS, start, 0)

    def o_copy(rows_of, cols_of):
        return pltpu.make_async_remote_copy(
            src_ref=o_ref.at[pl.ds(pl.multiple_of(rows_of * 256, 256), 256)],
            dst_ref=full_ref.at[:, pl.ds(pl.multiple_of(cols_of * HALF, HALF), HALF)],
            send_sem=o_send, recv_sem=o_recv, device_id={"seq": dev + 1 - 2 * core}, device_id_type=MESH)
    o_copy(1 - core, core).start()
    mine = [pltpu.make_async_copy(o_ref.at[pl.ds(pl.multiple_of(core * 256, 256), 256)],
                                  full_ref.at[:, pl.ds(pl.multiple_of(core * HALF, HALF), HALF)], loc.at[0]),
            pltpu.make_async_copy(part_ref.at[pl.ds(pl.multiple_of((chip % 16) * 8, 8), 8), pl.ds(pl.multiple_of((chip // 16) * 384, 128), 384)],
                                  recv.at[chip], loc.at[1])]
    for m in mine:
        m.start()
    for m in mine:
        m.wait()

    def wait(i, carry):
        part_copy(chip ^ i, chip ^ i).wait()
        return carry
    lax.fori_loop(1, CHIPS, wait, 0)

    top = lax.fori_loop(0, CHIPS, lambda i, t: jnp.maximum(t, recv[i, :, 256:384]), jnp.full((8, 128), NEG, jnp.float32), unroll=8)

    def add(i, carry):
        num, den = carry
        weight = pltpu.roll(jnp.exp(recv[i, :, 256:384] - top), 124, 1)
        wide = jnp.concatenate([jnp.broadcast_to(weight[:, t:t + 1], (8, HEAD_DIM)) for t in range(4)], axis=1)
        return num + wide * recv[i, :, 0:256], den + weight * recv[i, :, 256:384]
    num, den = lax.fori_loop(0, CHIPS, add, (jnp.zeros((8, 256), jnp.float32), jnp.zeros((8, 128), jnp.float32)), unroll=8)
    wide = jnp.concatenate([jnp.broadcast_to(den[:, t:t + 1], (8, HEAD_DIM)) for t in range(4)], axis=1)
    piece[...] = (num / wide).astype(jnp.bfloat16)

    def glob_slice(src_chip, src_core):
        return glob.at[pl.ds(pl.multiple_of((src_chip % 16) * 8, 8), 8),
                       pl.ds(pl.multiple_of(src_core * HALF + (src_chip // 16) * 256, 256), 256)]

    def glob_copy(src_chip, src_core):
        return pltpu.make_async_remote_copy(
            src_ref=piece, dst_ref=glob_slice(src_chip, src_core), send_sem=g_send,
            recv_sem=g_recv.at[2 * src_chip + src_core], device_id={"seq": 0}, device_id_type=MESH)

    o_copy(1 - core, core).wait_send()
    o_copy(core, 1 - core).wait_recv()

    @pl.when(dev != 0)
    def _():
        copy = glob_copy(chip, core)
        copy.start()
        copy.wait_send()

    @pl.when(dev == 0)
    def _():
        copy = pltpu.make_async_copy(piece, glob_slice(0, 0), loc.at[0])
        copy.start()
        copy.wait()

        def wait_glob(i, carry):
            glob_copy(i // 2, i % 2).wait_recv()
            return carry
        lax.fori_loop(1, 128, wait_glob, 0)
        full_ref[0:128, :] = glob[...]


def combine(part, o):
    return pl.pallas_call(
        combine_kernel,
        out_shape=jax.ShapeDtypeStruct((256, WIDTH), jnp.bfloat16),
        in_specs=[vspec()] * 2, out_specs=vspec(),
        scratch_shapes=[VMEM((CHIPS, 8, 384), jnp.float32), VMEM((128, WIDTH), jnp.bfloat16), VMEM((8, 256), jnp.bfloat16),
                        pltpu.SemaphoreType.DMA, pltpu.SemaphoreType.DMA((CHIPS,)),
                        pltpu.SemaphoreType.DMA, pltpu.SemaphoreType.DMA,
                        pltpu.SemaphoreType.DMA, pltpu.SemaphoreType.DMA((128,)), pltpu.SemaphoreType.DMA((2,))],
        compiler_params=params(), name="combine",
    )(part, o)


def solution(mesh):
    row_spec = P(("batch", "seq"), None)
    rep_spec = P(None, None)

    def local_fn(tokens, w_query, w_key, w_value, w_out, rand_idx):
        dev = lax.axis_index("seq")
        chip, core = dev // 2, dev % 2
        xs = tokens.reshape(4, BLK, 16, 128).transpose(1, 0, 2, 3).reshape(BLK, 64, 128)
        idx = jnp.pad(rand_idx.reshape(1, 12), ((0, 0), (0, 116)))
        recv, xc, idx_all = scatter_rows(xs, tokens.reshape(4, BLK, WIDTH), idx)

        ids = idx_all[:, 0, :12]
        blocks = jnp.arange(512, dtype=jnp.int32)
        present = jnp.any(ids.reshape(-1, 1) == blocks[None, :], axis=0)
        rank = jnp.sum(jnp.where((blocks[None, :] < blocks[:, None]) & present[None, :], 1, 0), axis=1)
        hot_ids = jnp.sum(jnp.where((rank[None, :] == jnp.arange(HOT)[:, None]) & present[None, :], blocks[None, :], 0), axis=1)
        pub = jnp.concatenate([jnp.arange(GLOBAL_BLOCKS), hot_ids, jnp.zeros((2,), jnp.int32)]).astype(jnp.int32)
        sel = jnp.take(recv.reshape(256, WIDTH), (pub // 8) * 4 + pub % 4, axis=0)
        sel = jnp.where((((pub // 4) % 2 == core) & (jnp.arange(SLOTS) < 14))[:, None], sel, jnp.zeros_like(sel))
        near = lax.dynamic_slice_in_dim(ids, 2 * chip, 2).reshape(8, 3)
        below = jnp.sum(jnp.where(hot_ids[None, None, :] < near[:, :, None], 1, 0), axis=2)
        own = chip * 8 + jnp.arange(8)
        info = jnp.concatenate([(GLOBAL_BLOCKS + below).reshape(24), jnp.zeros((8,), jnp.int32),
                                (own - 1 < GLOBAL_BLOCKS).astype(jnp.int32), (own + 1 >= 512).astype(jnp.int32)]).astype(jnp.int32)

        q, k, v = project_rows(core.reshape(1), xc.reshape(640, WIDTH), w_query, w_key, w_value)
        g = gather_rows(sel, w_query, w_key, w_value)
        o, part = attention(info, q, k, v, g.reshape(CHIPS * SLOTS, WIDTH))
        full = combine(part, o)
        out = lax.dot_general(full, w_out, (((1,), (1,)), ((), ())), preferred_element_type=jnp.float32)
        return out.astype(jnp.bfloat16)

    return jax.shard_map(local_fn, mesh=mesh, in_specs=(row_spec, rep_spec, rep_spec, rep_spec, rep_spec, row_spec), out_specs=row_spec, check_vma=False)
```

```python
import jax
import jax.numpy as jnp
from jax import lax
from jax.experimental import pallas as pl
from jax.experimental.pallas import tpu as pltpu
from jax.sharding import PartitionSpec as P

HEAD_DIM = 64
GLOBAL_BLOCKS = 2
HOT = 12
SLOTS = 16
BLK = 64
WIDTH = 2048
HALF = 1024
CHIPS = 64
NEG = -1e30
MESH = pl.DeviceIdType.MESH
VMEM = pltpu.VMEM
ANY = pl.ANY
PARTS = ((0, 768, (0, 1, 2)), (768, 640, (1, 2, 0)), (1408, 640, (2, 0, 1)))


def permutation():
    row = lax.broadcasted_iota(jnp.int32, (256, 256), 0)
    col = lax.broadcasted_iota(jnp.int32, (256, 256), 1)
    return jnp.where(col == (row & 15) * 16 + (row >> 4), 1.0, 0.0).astype(jnp.bfloat16)


def vspec():
    return pl.BlockSpec(memory_space=VMEM)


def params(effects=True, mib=60):
    return pltpu.CompilerParams(has_side_effects=effects, vmem_limit_bytes=mib * 1024 * 1024)


def where_am_i():
    dev = lax.axis_index("seq")
    return dev, dev // 2, dev % 2


def front_kernel(xs_ref, x_ref, idx_ref, wq_ref, wk_ref, wv_ref,
                 q_ref, k_ref, v_ref, g_ref, hot_ref, idxall_ref,
                 xc, recv, w_buf, sel, other,
                 s_send, s_recv, i_send, i_recv, x_sem, h_send, h_recv, loc, w_sem, p_sem, g_send, g_recv):
    dev, chip, core = where_am_i()
    partner = dev + 1 - 2 * core
    cx, cy, cz = chip % 4, (chip // 4) % 4, chip // 16

    def rows64(i):
        return pl.ds(pl.multiple_of(i * BLK, BLK), BLK)

    def row_copy(dst_chip, slot):
        return pltpu.make_async_remote_copy(
            src_ref=xs_ref.at[dst_chip], dst_ref=recv.at[pl.ds(4 * slot, 4)], send_sem=s_send, recv_sem=s_recv.at[slot],
            device_id={"seq": 2 * dst_chip + core}, device_id_type=MESH)

    def idx_copy(dst_chip, slot):
        return pltpu.make_async_remote_copy(
            src_ref=idx_ref, dst_ref=idxall_ref.at[core, slot], send_sem=i_send.at[0], recv_sem=i_recv.at[slot],
            device_id={"seq": 2 * dst_chip + core}, device_id_type=MESH)

    def idx_swap(which):
        return pltpu.make_async_remote_copy(
            src_ref=idxall_ref.at[core], dst_ref=idxall_ref.at[which], send_sem=i_send.at[1], recv_sem=i_send.at[2],
            device_id={"seq": partner}, device_id_type=MESH)

    def x_swap(which):
        return pltpu.make_async_remote_copy(
            src_ref=x_ref, dst_ref=xc.at[pl.ds(pl.multiple_of(BLK + 256 * which, BLK), 256)],
            send_sem=x_sem.at[0], recv_sem=x_sem.at[1], device_id={"seq": partner}, device_id_type=MESH)

    x_swap(core).start()
    nbr = lax.rem(chip + 2 * core - 1 + CHIPS, CHIPS)

    def halo(dst_core, side):
        return pltpu.make_async_remote_copy(
            src_ref=x_ref.at[rows64(3 * core)], dst_ref=xc.at[rows64(9 * side)],
            send_sem=h_send.at[dst_core], recv_sem=h_recv.at[side],
            device_id={"seq": 2 * nbr + dst_core}, device_id_type=MESH)
    for t in range(2):
        halo(t, 1 - core).start()

    def start_idx(i, carry):
        idx_copy(chip ^ i, chip).start()
        return carry
    lax.fori_loop(1, CHIPS, start_idx, 0)

    def start_row(i, carry):
        row_copy(chip ^ i, chip).start()
        return carry
    lax.fori_loop(1, CHIPS, start_row, 0)

    def w_copy(i, t):
        w = (wq_ref, wk_ref, wv_ref)[i]
        return pltpu.make_async_copy(
            w.at[:, pl.ds(pl.multiple_of(core * HALF + t * 256, 256), 256)],
            w_buf.at[i, :, pl.ds(pl.multiple_of(t * 256, 256), 256)], w_sem.at[i, t])
    for t in range(4):
        for i in range(3):
            w_copy(i, t).start()

    locs = [pltpu.make_async_copy(xs_ref.at[chip], recv.at[pl.ds(4 * chip, 4)], loc.at[0]),
            pltpu.make_async_copy(x_ref, xc.at[pl.ds(pl.multiple_of(BLK + 256 * core, BLK), 256)], loc.at[1]),
            pltpu.make_async_copy(idx_ref, idxall_ref.at[core, chip], loc.at[2])]
    for l in locs:
        l.start()
    for l in locs:
        l.wait()
    x_swap(core).wait_send()
    x_swap(1 - core).wait_recv()
    for t in range(2):
        halo(t, 1 - core).wait_send()
        halo(t, t).wait_recv()

    def project(t, carry):
        cols = pl.ds(pl.multiple_of(t * 256, 256), 256)
        for i in range(3):
            w_copy(i, t).wait()
        q_ref[:, cols] = jnp.dot(xc[BLK:9 * BLK, :], w_buf[0, :, cols], preferred_element_type=jnp.float32).astype(jnp.bfloat16)
        k_ref[:, cols] = jnp.dot(xc[...], w_buf[1, :, cols], preferred_element_type=jnp.float32).astype(jnp.bfloat16)
        v_ref[:, cols] = jnp.dot(xc[...], w_buf[2, :, cols], preferred_element_type=jnp.float32).astype(jnp.bfloat16)
        return carry
    lax.fori_loop(0, 4, project, 0)

    def wait_idx(i, carry):
        idx_copy(chip ^ i, chip ^ i).wait()
        return carry
    lax.fori_loop(1, CHIPS, wait_idx, 0)
    idx_swap(core).start()
    idx_swap(core).wait_send()
    idx_swap(1 - core).wait_recv()
    ids = jnp.concatenate([idxall_ref[0, :, 0, :], idxall_ref[1, :, 0, :]], axis=0)
    ids = jnp.where(lax.broadcasted_iota(jnp.int32, (128, 128), 1) < 12, ids, 1 << 20)
    slot = lax.broadcasted_iota(jnp.int32, (SLOTS, 128), 0)
    names = slot
    published = [jnp.int32(0), jnp.int32(1)]
    for s in range(2, 14):
        h = jnp.min(jnp.where(ids > published[-1], ids, 1 << 20)) if s > 2 else jnp.min(ids)
        published.append(h)
        names = jnp.where(slot == s, h, names)
    hot_ref[...] = names

    def wait_row(i, carry):
        row_copy(chip ^ i, chip ^ i).wait()
        return carry
    lax.fori_loop(1, CHIPS, wait_row, 0)

    for s in range(SLOTS):
        if s < 14:
            h = published[s]
            rows = recv[jnp.minimum((h >> 3) * 4 + (h & 3), 4 * CHIPS - 1)]
            sel[16 * s:16 * s + 16, :] = jnp.where(((h >> 2) & 1) == core, rows, jnp.zeros_like(rows))
        else:
            sel[16 * s:16 * s + 16, :] = jnp.zeros((16, 128), jnp.bfloat16)
    swap = pltpu.make_async_remote_copy(
        src_ref=sel, dst_ref=other, send_sem=p_sem.at[0], recv_sem=p_sem.at[1],
        device_id={"seq": partner}, device_id_type=MESH)
    swap.start()
    swap.wait()
    moved = jnp.dot(permutation(), sel[...] + other[...], preferred_element_type=jnp.float32).astype(jnp.bfloat16)
    rows = jnp.concatenate([moved[16 * j:16 * j + 16] for j in range(16)], axis=1)
    out = [jnp.dot(rows, w_buf[i], preferred_element_type=jnp.float32) for i in range(3)]
    kv = jnp.concatenate([out[1], out[2]], axis=1)
    glob_q = jnp.concatenate([out[0][0:1], out[0][1:2]], axis=1)
    row_id = lax.broadcasted_iota(jnp.int32, (SLOTS, WIDTH), 0)
    kv = jnp.where(row_id == 14, jnp.broadcast_to(glob_q, (SLOTS, WIDTH)), kv)
    g_ref[cz, cy, cx] = kv.astype(jnp.bfloat16)

    coord = (cx, cy, cz)
    scale = (1, 4, 16)

    def block(axes_done, at, cols):
        idx = []
        for axis in (2, 1, 0):
            idx.append(slice(None) if axis in axes_done else at[axis])
        return tuple(idx) + (slice(None), cols)

    def copies(part, stage, receive):
        start, size, order = PARTS[part]
        axis = order[stage]
        out = []
        for k in (1, 2, 3):
            to = lax.rem(coord[axis] + k, 4)
            frm = lax.rem(coord[axis] + 4 - k, 4)
            at = list(coord)
            if receive:
                at[axis] = frm
            ref = g_ref.at[block(order[:stage], at, slice(start, start + size))]
            out.append(pltpu.make_async_remote_copy(
                src_ref=ref, dst_ref=ref, send_sem=g_send.at[part, stage, k - 1], recv_sem=g_recv.at[part, stage, k - 1],
                device_id={"seq": dev + 2 * scale[axis] * (to - coord[axis])}, device_id_type=MESH))
        return out

    for stage in range(3):
        for part in range(3):
            if stage:
                for c in copies(part, stage - 1, True):
                    c.wait_recv()
            for c in copies(part, stage, False):
                c.start()
    for part in range(3):
        for c in copies(part, 2, True):
            c.wait_recv()
    for stage in range(3):
        for part in range(3):
            for c in copies(part, stage, False):
                c.wait_send()


def front(xs, x, idx, wq, wk, wv):
    anyspec = pl.BlockSpec(memory_space=ANY)
    dma = pltpu.SemaphoreType.DMA
    return pl.pallas_call(
        front_kernel,
        out_shape=(jax.ShapeDtypeStruct((512, HALF), jnp.bfloat16),
                   jax.ShapeDtypeStruct((640, HALF), jnp.bfloat16),
                   jax.ShapeDtypeStruct((640, HALF), jnp.bfloat16),
                   jax.ShapeDtypeStruct((4, 4, 4, SLOTS, WIDTH), jnp.bfloat16),
                   jax.ShapeDtypeStruct((SLOTS, 128), jnp.int32),
                   jax.ShapeDtypeStruct((2, CHIPS, 1, 128), jnp.int32)),
        in_specs=[vspec()] * 3 + [anyspec] * 3, out_specs=(vspec(),) * 6,
        scratch_shapes=[VMEM((640, WIDTH), jnp.bfloat16), VMEM((4 * CHIPS, 16, 128), jnp.bfloat16),
                        VMEM((3, WIDTH, HALF), jnp.bfloat16), VMEM((256, 128), jnp.bfloat16), VMEM((256, 128), jnp.bfloat16),
                        dma, dma((CHIPS,)), dma((3,)), dma((CHIPS,)), dma((2,)), dma((2,)), dma((2,)), dma((3,)), dma((3, 4)),
                        dma((2,)), dma((3, 3, 3)), dma((3, 3, 3))],
        compiler_params=params(), name="front",
    )(xs, x, idx, wq, wk, wv)


def split_heads(pair, rows):
    lane = lax.broadcasted_iota(jnp.int32, (rows, 128), 1)
    zero = jnp.zeros_like(pair)
    return jnp.concatenate([jnp.where(lane < HEAD_DIM, pair, zero), jnp.where(lane < HEAD_DIM, zero, pair)], axis=0)


def join_heads(out, rows):
    lane = lax.broadcasted_iota(jnp.int32, (rows, 128), 1)
    return jnp.where(lane < HEAD_DIM, out[:rows], out[rows:])


def back_kernel(info_ref, q_ref, k_ref, v_ref, g_ref, full_ref, hot, o_ref, part_ref, recv, glob, piece,
                c_send, c_recv, o_send, o_recv, g_send, g_recv, loc):
    dev, chip, core = where_am_i()
    nt = (((1,), (1,)), ((), ()))
    perm = permutation()

    def unpack(step, carry):
        z = step // 8
        cols = pl.ds(pl.multiple_of((step % 8) * 256, 256), 256)
        rows = g_ref[pl.ds(pl.multiple_of(z * 256, 256), 256), cols]
        moved = jnp.dot(perm, rows, preferred_element_type=jnp.float32).astype(jnp.bfloat16)
        for s in range(SLOTS):
            hot[s, pl.ds(pl.multiple_of(z * 16, 16), 16), cols] = moved[s * 16:s * 16 + 16]
        return carry
    lax.fori_loop(0, 32, unpack, 0)

    lane = lax.broadcasted_iota(jnp.int32, (128, 128), 1)
    stats = None
    for j in range(8):
        cols = slice(j * 128, j * 128 + 128)
        vcols = slice(HALF + j * 128, HALF + j * 128 + 128)
        gq = jnp.concatenate([hot[14, :, cols], hot[14, :, vcols]], axis=0)
        queries = split_heads(gq, 128) * jnp.bfloat16(0.125)
        scores = lax.dot_general(queries, k_ref[BLK:9 * BLK, cols], nt, preferred_element_type=jnp.float32)
        top = jnp.max(scores, axis=1, keepdims=True)
        probs = jnp.exp(scores - top)
        total = jnp.sum(probs, axis=1, keepdims=True)
        out = jnp.dot(probs.astype(jnp.bfloat16), v_ref[BLK:9 * BLK, cols], preferred_element_type=jnp.float32)
        g, t = j // 2, 2 * (j % 2)
        part_ref[:, 384 * g + 64 * t:384 * g + 64 * t + 128] = join_heads(out, 128)
        if t == 0:
            stats = jnp.zeros((128, 128), jnp.float32)
        for h in range(2):
            rows = slice(128 * h, 128 * h + 128)
            stats = jnp.where(lane == t + h, total[rows], stats)
            stats = jnp.where(lane == 4 + t + h, top[rows], stats)
        if t:
            part_ref[:, 384 * g + 256:384 * g + 384] = stats

    def part_copy(dst_chip, slot):
        rows = pl.ds(pl.multiple_of((dst_chip % 16) * 8, 8), 8)
        cols = pl.ds(pl.multiple_of((dst_chip // 16) * 384, 128), 384)
        return pltpu.make_async_remote_copy(
            src_ref=part_ref.at[rows, cols], dst_ref=recv.at[slot], send_sem=c_send, recv_sem=c_recv.at[slot],
            device_id={"seq": 2 * dst_chip + core}, device_id_type=MESH)

    def start(i, carry):
        part_copy(chip ^ i, chip).start()
        return carry
    lax.fori_loop(1, CHIPS, start, 0)

    def o_copy(rows_of, cols_of):
        return pltpu.make_async_remote_copy(
            src_ref=o_ref.at[pl.ds(pl.multiple_of(rows_of * 256, 256), 256)],
            dst_ref=full_ref.at[:, pl.ds(pl.multiple_of(cols_of * HALF, HALF), HALF)],
            send_sem=o_send, recv_sem=o_recv, device_id={"seq": dev + 1 - 2 * core}, device_id_type=MESH)

    def one_block(step, carry):
        b = (step + 4 * (1 - core)) & 7
        slots = [0, 1] + [info_ref[b * 3 + t] for t in range(3)]
        left_bad = info_ref[32 + b]
        right_bad = info_ref[40 + b]
        key = lax.broadcasted_iota(jnp.int32, (1, 256), 1)
        bias = jnp.where((key < BLK) & (left_bad > 0), NEG, 0.0) + jnp.where((key >= 2 * BLK) & (key < 3 * BLK) & (right_bad > 0), NEG, 0.0)
        base = pl.multiple_of(b * BLK, BLK)
        for j in range(8):
            cols = slice(j * 128, j * 128 + 128)
            vcols = slice(HALF + j * 128, HALF + j * 128 + 128)
            queries = split_heads(q_ref[pl.ds(base, BLK), cols], BLK) * jnp.bfloat16(0.125)
            keys = jnp.concatenate([k_ref[pl.ds(base, 3 * BLK), cols]] + [hot[s, :, cols] for s in slots], axis=0)
            vals = jnp.concatenate([v_ref[pl.ds(base, 3 * BLK), cols]] + [hot[s, :, vcols] for s in slots], axis=0)
            scores = lax.dot_general(queries, keys, nt, preferred_element_type=jnp.float32)
            scores = jnp.concatenate([scores[:, :256] + bias, scores[:, 256:]], axis=1)
            top = jnp.max(scores, axis=1, keepdims=True)
            probs = jnp.exp(scores - top)
            probs = probs * (1.0 / jnp.sum(probs, axis=1, keepdims=True))
            out = jnp.dot(probs.astype(jnp.bfloat16), vals, preferred_element_type=jnp.float32)
            o_ref[pl.ds(base, BLK), cols] = join_heads(out, BLK).astype(jnp.bfloat16)
        return carry
    lax.fori_loop(0, 4, one_block, 0)
    o_copy(1 - core, core).start()
    lax.fori_loop(4, 8, one_block, 0)

    mine = [pltpu.make_async_copy(o_ref.at[pl.ds(pl.multiple_of(core * 256, 256), 256)],
                                  full_ref.at[:, pl.ds(pl.multiple_of(core * HALF, HALF), HALF)], loc.at[0]),
            pltpu.make_async_copy(part_ref.at[pl.ds(pl.multiple_of((chip % 16) * 8, 8), 8), pl.ds(pl.multiple_of((chip // 16) * 384, 128), 384)],
                                  recv.at[chip], loc.at[1])]
    for m in mine:
        m.start()
    for m in mine:
        m.wait()

    def wait(i, carry):
        part_copy(chip ^ i, chip ^ i).wait()
        return carry
    lax.fori_loop(1, CHIPS, wait, 0)

    top = lax.fori_loop(0, CHIPS, lambda i, t: jnp.maximum(t, recv[i, :, 256:384]), jnp.full((8, 128), NEG, jnp.float32), unroll=8)

    def add(i, carry):
        num, den = carry
        weight = pltpu.roll(jnp.exp(recv[i, :, 256:384] - top), 124, 1)
        wide = jnp.concatenate([jnp.broadcast_to(weight[:, t:t + 1], (8, HEAD_DIM)) for t in range(4)], axis=1)
        return num + wide * recv[i, :, 0:256], den + weight * recv[i, :, 256:384]
    num, den = lax.fori_loop(0, CHIPS, add, (jnp.zeros((8, 256), jnp.float32), jnp.zeros((8, 128), jnp.float32)), unroll=8)
    wide = jnp.concatenate([jnp.broadcast_to(den[:, t:t + 1], (8, HEAD_DIM)) for t in range(4)], axis=1)
    piece[...] = (num / wide).astype(jnp.bfloat16)

    def glob_slice(src_chip, src_core):
        return glob.at[pl.ds(pl.multiple_of((src_chip % 16) * 8, 8), 8),
                       pl.ds(pl.multiple_of(src_core * HALF + (src_chip // 16) * 256, 256), 256)]

    def glob_copy(src_chip, src_core):
        return pltpu.make_async_remote_copy(
            src_ref=piece, dst_ref=glob_slice(src_chip, src_core), send_sem=g_send,
            recv_sem=g_recv.at[2 * src_chip + src_core], device_id={"seq": 0}, device_id_type=MESH)

    o_copy(1 - core, core).wait_send()
    o_copy(core, 1 - core).wait_recv()

    @pl.when(dev != 0)
    def _():
        copy = glob_copy(chip, core)
        copy.start()
        copy.wait_send()

    @pl.when(dev == 0)
    def _():
        copy = pltpu.make_async_copy(piece, glob_slice(0, 0), loc.at[0])
        copy.start()
        copy.wait()

        def wait_glob(i, carry):
            glob_copy(i // 2, i % 2).wait_recv()
            return carry
        lax.fori_loop(1, 128, wait_glob, 0)
        full_ref[0:128, :] = glob[...]


def back(info, q, k, v, g):
    dma = pltpu.SemaphoreType.DMA
    return pl.pallas_call(
        back_kernel,
        out_shape=jax.ShapeDtypeStruct((256, WIDTH), jnp.bfloat16),
        in_specs=[pl.BlockSpec(memory_space=pltpu.SMEM)] + [vspec()] * 4, out_specs=vspec(),
        scratch_shapes=[VMEM((SLOTS, BLK, WIDTH), jnp.bfloat16), VMEM((512, HALF), jnp.bfloat16), VMEM((128, 1536), jnp.float32),
                        VMEM((CHIPS, 8, 384), jnp.float32), VMEM((128, WIDTH), jnp.bfloat16), VMEM((8, 256), jnp.bfloat16),
                        dma, dma((CHIPS,)), dma, dma, dma, dma((128,)), dma((2,))],
        compiler_params=params(), name="back",
    )(info, q, k, v, g)


def solution(mesh):
    row_spec = P(("batch", "seq"), None)
    rep_spec = P(None, None)

    def local_fn(tokens, w_query, w_key, w_value, w_out, rand_idx):
        dev = lax.axis_index("seq")
        chip, core = dev // 2, dev % 2
        xs = tokens.reshape(4, BLK, 16, 128).transpose(1, 0, 2, 3)
        idx = jnp.pad(rand_idx.reshape(1, 12), ((0, 0), (0, 116)))
        q, k, v, g, hot_rows, idx_all = front(xs, tokens, idx, w_query, w_key, w_value)
        near = lax.dynamic_slice_in_dim(idx_all[:, :, 0, :12], chip, 1, axis=1).reshape(8, 3)
        hot_ids = hot_rows[2:14, 0]
        below = jnp.sum(jnp.where(hot_ids[None, None, :] < near[:, :, None], 1, 0), axis=2)
        own = chip * 8 + jnp.arange(8)
        info = jnp.concatenate([(GLOBAL_BLOCKS + below).reshape(24), jnp.zeros((8,), jnp.int32),
                                (own - 1 < GLOBAL_BLOCKS).astype(jnp.int32), (own + 1 >= 512).astype(jnp.int32)]).astype(jnp.int32)
        full = back(info, q, k, v, g.reshape(CHIPS * SLOTS, WIDTH))
        out = lax.dot_general(full, w_out, (((1,), (1,)), ((), ())), preferred_element_type=jnp.float32)
        return out.astype(jnp.bfloat16)

    return jax.shard_map(local_fn, mesh=mesh, in_specs=(row_spec, rep_spec, rep_spec, rep_spec, rep_spec, row_spec), out_specs=row_spec, check_vma=False)
```

```python
import jax
import jax.numpy as jnp
from jax import lax
from jax.experimental import pallas as pl
from jax.experimental.pallas import tpu as pltpu
from jax.sharding import PartitionSpec as P

HEAD_DIM = 64
BLK = 64
SLOTS = 16
WIDTH = 2048
HALF = 1024
CHIPS = 64
PAIRS = 8
NEG = -1e30
FAR = 1 << 20
MESH = pl.DeviceIdType.MESH
VMEM = pltpu.VMEM
ORDERS = ((0, 1, 2), (1, 2, 0), (2, 0, 1))
NT = (((1,), (1,)), ((), ()))


def permutation():
    row = lax.broadcasted_iota(jnp.int32, (256, 256), 0)
    col = lax.broadcasted_iota(jnp.int32, (256, 256), 1)
    return jnp.where(col == (row & 15) * 16 + (row >> 4), 1.0, 0.0).astype(jnp.bfloat16)


def split_heads(pair, rows):
    lane = lax.broadcasted_iota(jnp.int32, (rows, 128), 1)
    zero = jnp.zeros_like(pair)
    return jnp.concatenate([jnp.where(lane < HEAD_DIM, pair, zero), jnp.where(lane < HEAD_DIM, zero, pair)], axis=0)


def join_heads(out, rows):
    lane = lax.broadcasted_iota(jnp.int32, (rows, 128), 1)
    return jnp.where(lane < HEAD_DIM, out[:rows], out[rows:])


def aligned(i, n):
    return pl.ds(pl.multiple_of(i * n, n), n)


def remote(src, dst, send, recv, dev):
    return pltpu.make_async_remote_copy(src_ref=src, dst_ref=dst, send_sem=send, recv_sem=recv,
                                        device_id={"seq": dev}, device_id_type=MESH)


def kernel(x_ref, idx_ref, wq_ref, wk_ref, wv_ref, full_ref,
           xs, xc, recv, w_buf, idx_all, sel, other, q_ref, k_ref, v_ref, gath, hot, o_ref, part, parts, glob, piece, near_s, slot_s,
           s_send, s_recv, i_send, i_recv, x_sem, h_send, h_recv, loc, w_sem, p_sem, g_send, g_recv,
           c_send, c_recv, o_send, o_recv, e_send, e_recv):
    dev = lax.axis_index("seq")
    chip, core = dev // 2, dev % 2
    partner = dev + 1 - 2 * core
    coord = (chip % 4, (chip // 4) % 4, chip // 16)
    scale = (1, 4, 16)
    perm = permutation()

    def w_copy(i, t):
        w = (wq_ref, wk_ref, wv_ref)[i]
        return pltpu.make_async_copy(w.at[:, aligned(core * 4 + t, 256)], w_buf.at[i, :, aligned(t, 256)], w_sem.at[i, t])

    def x_swap(which):
        return remote(x_ref, xc.at[pl.ds(pl.multiple_of(BLK + 256 * which, BLK), 256)], x_sem.at[0], x_sem.at[1], partner)

    def idx_copy(dst_chip, slot):
        return remote(idx_ref, idx_all.at[core, slot], i_send.at[0], i_recv.at[slot], 2 * dst_chip + core)

    def idx_swap(which):
        return remote(idx_all.at[core], idx_all.at[which], i_send.at[1], i_send.at[2], partner)

    def row_copy(dst_chip, slot):
        return remote(xs.at[dst_chip], recv.at[pl.ds(4 * slot, 4)], s_send, s_recv.at[slot], 2 * dst_chip + core)

    nbr = lax.rem(chip + 2 * core - 1 + CHIPS, CHIPS)

    def halo(dst_core, side):
        return remote(x_ref.at[aligned(3 * core, BLK)], xc.at[aligned(9 * side, BLK)], h_send.at[dst_core], h_recv.at[side],
                      2 * nbr + dst_core)

    with jax.named_scope("issue"):
        x_swap(core).start()
        for t in range(4):
            for i in range(3):
                w_copy(i, t).start()
        locs = [pltpu.make_async_copy(x_ref, xc.at[pl.ds(pl.multiple_of(BLK + 256 * core, BLK), 256)], loc.at[1]),
                pltpu.make_async_copy(idx_ref, idx_all.at[core, chip], loc.at[2])]
        for l in locs:
            l.start()

        def start_idx(i, carry):
            idx_copy(chip ^ i, chip).start()
            return carry
        lax.fori_loop(1, CHIPS, start_idx, 0, unroll=7)

    def relayout(step, carry):
        blk, group = step >> 2, step & 3
        rows = x_ref[aligned(step, 16), :]
        rows = jnp.concatenate([rows[:, 128 * c:128 * c + 128] for c in range(16)], axis=0)
        moved = jnp.dot(perm, rows, preferred_element_type=jnp.float32).astype(jnp.bfloat16)
        for a in range(16):
            xs[16 * group + a, blk] = moved[16 * a:16 * a + 16]
        return carry
    with jax.named_scope("relayout"):
        lax.fori_loop(0, 16, relayout, 0)

    def start_row(i, carry):
        row_copy(chip ^ i, chip).start()
        return carry
    with jax.named_scope("issue_rows"):
        lax.fori_loop(1, CHIPS, start_row, 0, unroll=7)
        own_row = pltpu.make_async_copy(xs.at[chip], recv.at[pl.ds(4 * chip, 4)], loc.at[0])
        own_row.start()
        for t in range(2):
            halo(t, 1 - core).start()

    with jax.named_scope("wait_x"):
        for l in locs:
            l.wait()
        x_swap(core).wait_send()
        x_swap(1 - core).wait_recv()

    def project(t, carry):
        cols = aligned(t, 256)
        for i in range(3):
            w_copy(i, t).wait()
        rows = xc[BLK:9 * BLK, :]
        q_ref[:, cols] = jnp.dot(rows, w_buf[0, :, cols], preferred_element_type=jnp.float32).astype(jnp.bfloat16)
        k_ref[BLK:9 * BLK, cols] = jnp.dot(rows, w_buf[1, :, cols], preferred_element_type=jnp.float32).astype(jnp.bfloat16)
        v_ref[BLK:9 * BLK, cols] = jnp.dot(rows, w_buf[2, :, cols], preferred_element_type=jnp.float32).astype(jnp.bfloat16)
        return carry
    with jax.named_scope("project"):
        lax.fori_loop(0, 4, project, 0)

    def wait_idx(i, carry):
        idx_copy(chip ^ i, chip ^ i).wait()
        return carry
    with jax.named_scope("wait_idx"):
        lax.fori_loop(1, CHIPS, wait_idx, 0)
        idx_swap(core).start()
        idx_swap(core).wait_send()
        idx_swap(1 - core).wait_recv()
    with jax.named_scope("names"):
        ids = jnp.concatenate([idx_all[0, :, 0, :], idx_all[1, :, 0, :]], axis=0)
        ids = jnp.where(lax.broadcasted_iota(jnp.int32, (128, 128), 1) < 12, ids, FAR)
        published = [jnp.int32(0), jnp.int32(1), jnp.min(ids)]
        for s in range(3, 14):
            published.append(jnp.min(jnp.where(ids > published[-1], ids, FAR)))

    def wait_row(i, carry):
        row_copy(chip ^ i, chip ^ i).wait()
        return carry
    with jax.named_scope("wait_rows"):
        lax.fori_loop(1, CHIPS, wait_row, 0)
        own_row.wait()

    with jax.named_scope("select"):
        for s in range(SLOTS):
            if s < 14:
                h = published[s]
                rows = recv[jnp.minimum((h >> 3) * 4 + (h & 3), 4 * CHIPS - 1)]
                sel[16 * s:16 * s + 16, :] = jnp.where(((h >> 2) & 1) == core, rows, jnp.zeros_like(rows))
            else:
                sel[16 * s:16 * s + 16, :] = jnp.zeros((16, 128), jnp.bfloat16)
        swap = remote(sel, other, p_sem.at[0], p_sem.at[1], partner)
        swap.start()
        swap.wait()
    with jax.named_scope("publish"):
        moved = jnp.dot(perm, sel[...] + other[...], preferred_element_type=jnp.float32).astype(jnp.bfloat16)
        rows = jnp.concatenate([moved[16 * j:16 * j + 16] for j in range(16)], axis=1)
        out = [jnp.dot(rows, w_buf[i], preferred_element_type=jnp.float32) for i in range(3)]
        row_id = lax.broadcasted_iota(jnp.int32, (SLOTS, 256), 0)
        for j in range(PAIRS):
            cols = slice(128 * j, 128 * j + 128)
            kv = jnp.concatenate([out[1][:, cols], out[2][:, cols]], axis=1)
            gq = jnp.concatenate([out[0][0:1, cols], out[0][1:2, cols]], axis=1)
            kv = jnp.where(row_id == 14, jnp.broadcast_to(gq, (SLOTS, 256)), kv)
            gath[j, coord[2], coord[1], coord[0]] = kv.astype(jnp.bfloat16)

    def copies(j, stage, receive):
        order = ORDERS[j % 3]
        axis = order[stage]
        out = []
        for k in (1, 2, 3):
            to = lax.rem(coord[axis] + k, 4)
            at = list(coord)
            if receive:
                at[axis] = lax.rem(coord[axis] + 4 - k, 4)
            ref = gath.at[(j,) + tuple(slice(None) if a in order[:stage] else at[a] for a in (2, 1, 0))]
            out.append(remote(ref, ref, g_send.at[j, stage, k - 1], g_recv.at[j, stage, k - 1],
                              dev + 2 * scale[axis] * (to - coord[axis])))
        return out

    def advance(j, stage):
        if stage:
            for c in copies(j, stage - 1, True):
                c.wait_recv()
        if stage < 3:
            for c in copies(j, stage, False):
                c.start()

    with jax.named_scope("gather0"):
        for j in range(PAIRS):
            advance(j, 0)
    with jax.named_scope("halo"):
        for t in range(2):
            halo(t, 1 - core).wait_send()
            halo(t, t).wait_recv()

        def project_halo(t, carry):
            cols = aligned(t, 256)
            rows = jnp.concatenate([xc[0:BLK, :], xc[9 * BLK:10 * BLK, :]], axis=0)
            for i, ref in ((1, k_ref), (2, v_ref)):
                out = jnp.dot(rows, w_buf[i, :, cols], preferred_element_type=jnp.float32).astype(jnp.bfloat16)
                ref[0:BLK, cols] = out[0:BLK]
                ref[9 * BLK:10 * BLK, cols] = out[BLK:]
            return carry
        lax.fori_loop(0, 4, project_halo, 0)
    with jax.named_scope("gather1"):
        for j in range(PAIRS):
            advance(j, 1)
    with jax.named_scope("gather2"):
        for j in range(PAIRS):
            advance(j, 2)

    with jax.named_scope("slots"):
        near = [pltpu.make_async_copy(idx_all.at[c, chip], near_s.at[c], loc.at[c]) for c in range(2)]
        for n in near:
            n.start()
        for n in near:
            n.wait()
        for b in range(8):
            for t in range(3):
                named = near_s[b // 4, 0, 3 * (b % 4) + t]
                at = jnp.int32(2)
                for h in published[2:]:
                    at = at + jnp.where(h < named, 1, 0)
                slot_s[3 * b + t] = at

    lane = lax.broadcasted_iota(jnp.int32, (128, 128), 1)
    key = lax.broadcasted_iota(jnp.int32, (1, 256), 1)

    def part_copy(wave, i, slot):
        dst_chip = 16 * wave + i
        return remote(part.at[wave, aligned(i, 8)], parts.at[slot], c_send, c_recv.at[slot], 2 * dst_chip + core)

    def o_copy(wave, rows_of, cols_of):
        return remote(o_ref.at[aligned(rows_of, 256), pl.ds(256 * wave, 256)],
                      full_ref.at[:, aligned(cols_of * 4 + wave, 256)], o_send.at[wave], o_recv.at[wave], partner)

    for wave in range(4):
        with jax.named_scope("wait_wave"):
            for j in (2 * wave, 2 * wave + 1):
                advance(j, 3)

        def unpack(z, carry):
            for j in (2 * wave, 2 * wave + 1):
                rows = gath[j, z].reshape(256, 256)
                moved = jnp.dot(perm, rows, preferred_element_type=jnp.float32).astype(jnp.bfloat16)
                for s in range(15):
                    hot[j, s, aligned(z, 16), :] = moved[s * 16:s * 16 + 16]
            return carry
        with jax.named_scope("unpack"):
            lax.fori_loop(0, 4, unpack, 0)

        with jax.named_scope("globpart"):
            stats = jnp.zeros((128, 128), jnp.float32)
            for t, j in enumerate((2 * wave, 2 * wave + 1)):
                cols = slice(128 * j, 128 * j + 128)
                gq = jnp.concatenate([hot[j, 14, :, 0:128], hot[j, 14, :, 128:256]], axis=0)
                queries = split_heads(gq, 128) * jnp.bfloat16(0.125)
                scores = lax.dot_general(queries, k_ref[BLK:9 * BLK, cols], NT, preferred_element_type=jnp.float32)
                top = jnp.max(scores, axis=1, keepdims=True)
                probs = jnp.exp(scores - top)
                total = jnp.sum(probs, axis=1, keepdims=True)
                out = jnp.dot(probs.astype(jnp.bfloat16), v_ref[BLK:9 * BLK, cols], preferred_element_type=jnp.float32)
                part[wave, :, 128 * t:128 * t + 128] = join_heads(out, 128)
                for h in range(2):
                    rows = slice(128 * h, 128 * h + 128)
                    stats = jnp.where(lane == 2 * t + h, total[rows], stats)
                    stats = jnp.where(lane == 4 + 2 * t + h, top[rows], stats)
            part[wave, :, 256:384] = stats

        def start_part(i, carry):
            j = i ^ (chip & 15)

            @pl.when(16 * wave + j != chip)
            def _():
                part_copy(wave, j, chip).start()
            return carry
        with jax.named_scope("issue_parts"):
            lax.fori_loop(0, 16, start_part, 0)

        def one_block(step, carry):
            b = (step + 4 * (1 - core)) & 7
            named = [0, 1] + [slot_s[3 * b + t] for t in range(3)]
            block_id = chip * 8 + b
            bias = (jnp.where((key < BLK) & (block_id - 1 < 2), NEG, 0.0)
                    + jnp.where((key >= 2 * BLK) & (key < 3 * BLK) & (block_id + 1 >= 8 * CHIPS), NEG, 0.0))
            base = pl.multiple_of(b * BLK, BLK)
            for j in (2 * wave, 2 * wave + 1):
                cols = slice(j * 128, j * 128 + 128)
                queries = split_heads(q_ref[pl.ds(base, BLK), cols], BLK) * jnp.bfloat16(0.125)
                keys = jnp.concatenate([k_ref[pl.ds(base, 3 * BLK), cols]] + [hot[j, s, :, 0:128] for s in named], axis=0)
                vals = jnp.concatenate([v_ref[pl.ds(base, 3 * BLK), cols]] + [hot[j, s, :, 128:256] for s in named], axis=0)
                scores = lax.dot_general(queries, keys, NT, preferred_element_type=jnp.float32)
                scores = jnp.concatenate([scores[:, :256] + bias, scores[:, 256:]], axis=1)
                top = jnp.max(scores, axis=1, keepdims=True)
                probs = jnp.exp(scores - top)
                probs = probs * (1.0 / jnp.sum(probs, axis=1, keepdims=True))
                out = jnp.dot(probs.astype(jnp.bfloat16), vals, preferred_element_type=jnp.float32)
                o_ref[pl.ds(base, BLK), cols] = join_heads(out, BLK).astype(jnp.bfloat16)
            return carry
        with jax.named_scope("blocks"):
            lax.fori_loop(0, 8, one_block, 0)
        o_copy(wave, 1 - core, core).start()

    with jax.named_scope("local"):
        mine = [pltpu.make_async_copy(o_ref.at[aligned(core, 256)], full_ref.at[:, aligned(core, HALF)], loc.at[0]),
                pltpu.make_async_copy(part.at[chip >> 4, aligned(chip & 15, 8)], parts.at[chip], loc.at[1])]
        for m in mine:
            m.start()
        for j in range(PAIRS):
            for stage in range(3):
                for c in copies(j, stage, False):
                    c.wait_send()

        for m in mine:
            m.wait()

    def wait_part(i, carry):
        part_copy(chip >> 4, chip & 15, chip ^ i).wait()
        return carry
    with jax.named_scope("wait_parts"):
        lax.fori_loop(1, CHIPS, wait_part, 0)

    with jax.named_scope("combine"):
        top = lax.fori_loop(0, CHIPS, lambda i, t: jnp.maximum(t, parts[i, :, 256:384]), jnp.full((8, 128), NEG, jnp.float32), unroll=8)

        def add(i, carry):
            num, den = carry
            weight = pltpu.roll(jnp.exp(parts[i, :, 256:384] - top), 124, 1)
            wide = jnp.concatenate([jnp.broadcast_to(weight[:, t:t + 1], (8, HEAD_DIM)) for t in range(4)], axis=1)
            return num + wide * parts[i, :, 0:256], den + weight * parts[i, :, 256:384]
        num, den = lax.fori_loop(0, CHIPS, add, (jnp.zeros((8, 256), jnp.float32), jnp.zeros((8, 128), jnp.float32)), unroll=8)
        wide = jnp.concatenate([jnp.broadcast_to(den[:, t:t + 1], (8, HEAD_DIM)) for t in range(4)], axis=1)
        piece[...] = (num / wide).astype(jnp.bfloat16)

    def glob_slice(src_chip, src_core):
        return glob.at[aligned(src_chip % 16, 8), aligned(src_core * 4 + src_chip // 16, 256)]

    def glob_copy(src_chip, src_core):
        return remote(piece, glob_slice(src_chip, src_core), e_send, e_recv.at[2 * src_chip + src_core], 0)

    with jax.named_scope("tail"):
        @pl.when(dev != 0)
        def _():
            copy = glob_copy(chip, core)
            copy.start()
            copy.wait_send()

        for wave in range(4):
            o_copy(wave, 1 - core, core).wait_send()
            o_copy(wave, core, 1 - core).wait_recv()

        @pl.when(dev == 0)
        def _():
            copy = pltpu.make_async_copy(piece, glob_slice(0, 0), loc.at[0])
            copy.start()
            copy.wait()

            def wait_glob(i, carry):
                glob_copy(i // 2, i % 2).wait_recv()
                return carry
            lax.fori_loop(1, 128, wait_glob, 0)
            full_ref[0:128, :] = glob[...]


def attend(x, idx, wq, wk, wv):
    vmem = pl.BlockSpec(memory_space=VMEM)
    hbm = pl.BlockSpec(memory_space=pl.ANY)
    dma = pltpu.SemaphoreType.DMA
    bf16, f32 = jnp.bfloat16, jnp.float32
    return pl.pallas_call(
        kernel,
        out_shape=jax.ShapeDtypeStruct((256, WIDTH), bf16),
        in_specs=[vmem, vmem, hbm, hbm, hbm], out_specs=vmem,
        scratch_shapes=[
            VMEM((CHIPS, 4, 16, 128), bf16), VMEM((640, WIDTH), bf16), VMEM((4 * CHIPS, 16, 128), bf16),
            VMEM((3, WIDTH, HALF), bf16), VMEM((2, CHIPS, 1, 128), jnp.int32), VMEM((256, 128), bf16), VMEM((256, 128), bf16),
            VMEM((512, HALF), bf16), VMEM((640, HALF), bf16), VMEM((640, HALF), bf16),
            VMEM((PAIRS, 4, 4, 4, SLOTS, 256), bf16), VMEM((PAIRS, SLOTS, BLK, 256), bf16), VMEM((512, HALF), bf16),
            VMEM((4, 128, 384), f32), VMEM((CHIPS, 8, 384), f32), VMEM((128, WIDTH), bf16), VMEM((8, 256), bf16),
            pltpu.SMEM((2, 1, 128), jnp.int32), pltpu.SMEM((24,), jnp.int32),
            dma, dma((CHIPS,)), dma((3,)), dma((CHIPS,)), dma((2,)), dma((2,)), dma((2,)), dma((3,)), dma((3, 4)), dma((2,)),
            dma((PAIRS, 3, 3)), dma((PAIRS, 3, 3)), dma, dma((CHIPS,)), dma((4,)), dma((4,)), dma, dma((128,))],
        compiler_params=pltpu.CompilerParams(has_side_effects=True, vmem_limit_bytes=62 * 1024 * 1024), name="attend",
    )(x, idx, wq, wk, wv)


def solution(mesh):
    row_spec = P(("batch", "seq"), None)
    rep_spec = P(None, None)

    def local_fn(tokens, w_query, w_key, w_value, w_out, rand_idx):
        idx = jnp.pad(rand_idx.reshape(1, 12), ((0, 0), (0, 116)))
        full = attend(tokens, idx, w_query, w_key, w_value)
        out = lax.dot_general(full, w_out, NT, preferred_element_type=jnp.float32)
        return out.astype(jnp.bfloat16)

    return jax.shard_map(local_fn, mesh=mesh, in_specs=(row_spec, rep_spec, rep_spec, rep_spec, rep_spec, row_spec), out_specs=row_spec, check_vma=False)
```

```python
import jax
import jax.numpy as jnp
from jax import lax
from jax.experimental import pallas as pl
from jax.experimental.pallas import tpu as pltpu
from jax.sharding import PartitionSpec as P

HEAD_DIM = 64
BLK = 64
SLOTS = 16
WIDTH = 2048
HALF = 1024
CHIPS = 64
PAIRS = 8
NEG = -1e30
FAR = 1 << 20
MESH = pl.DeviceIdType.MESH
VMEM = pltpu.VMEM
ORDERS = ((0, 1, 2), (1, 2, 0), (2, 0, 1))
NT = (((1,), (1,)), ((), ()))


def permutation():
    row = lax.broadcasted_iota(jnp.int32, (256, 256), 0)
    col = lax.broadcasted_iota(jnp.int32, (256, 256), 1)
    return jnp.where(col == (row & 15) * 16 + (row >> 4), 1.0, 0.0).astype(jnp.bfloat16)


def split_heads(pair, rows):
    lane = lax.broadcasted_iota(jnp.int32, (rows, 128), 1)
    zero = jnp.zeros_like(pair)
    return jnp.concatenate([jnp.where(lane < HEAD_DIM, pair, zero), jnp.where(lane < HEAD_DIM, zero, pair)], axis=0)


def join_heads(out, rows):
    lane = lax.broadcasted_iota(jnp.int32, (rows, 128), 1)
    return jnp.where(lane < HEAD_DIM, out[:rows], out[rows:])


def aligned(i, n):
    return pl.ds(pl.multiple_of(i * n, n), n)


def remote(src, dst, send, recv, dev):
    return pltpu.make_async_remote_copy(src_ref=src, dst_ref=dst, send_sem=send, recv_sem=recv,
                                        device_id={"seq": dev}, device_id_type=MESH)


def kernel(x_ref, rand_ref, wq_ref, wk_ref, wv_ref, wo_ref, y_ref,
           idx_ref, full_ref, wo_buf, xs, xc, recv, w_buf, idx_all, sel, other, q_ref, k_ref, v_ref, gath, hot, o_ref, part, parts, glob, piece, near_s, slot_s,
           s_send, s_recv, i_send, i_recv, x_sem, h_send, h_recv, loc, w_sem, p_sem, g_send, g_recv,
           c_send, c_recv, o_send, o_recv, e_send, e_recv, wo_sem):
    dev = lax.axis_index("seq")
    chip, core = dev // 2, dev % 2
    partner = dev + 1 - 2 * core
    coord = (chip % 4, (chip // 4) % 4, chip // 16)
    scale = (1, 4, 16)
    perm = permutation()

    barrier = pltpu.get_barrier_semaphore()

    def greet(i, carry):
        pl.semaphore_signal(barrier, inc=1, device_id={"seq": dev ^ i}, device_id_type=MESH)
        return carry
    with jax.named_scope("greet"):
        lax.fori_loop(1, 128, greet, 0, unroll=8)

    def w_copy(i, t):
        w = (wq_ref, wk_ref, wv_ref)[i]
        return pltpu.make_async_copy(w.at[:, aligned(core * 4 + t, 256)], w_buf.at[i, :, aligned(t, 256)], w_sem.at[i, t])

    def x_swap(which):
        return remote(x_ref, xc.at[pl.ds(pl.multiple_of(BLK + 256 * which, BLK), 256)], x_sem.at[0], x_sem.at[1], partner)

    def idx_copy(dst_chip, slot):
        return remote(idx_ref, idx_all.at[core, slot], i_send.at[0], i_recv.at[slot], 2 * dst_chip + core)

    def idx_swap(which):
        return remote(idx_all.at[core], idx_all.at[which], i_send.at[1], i_send.at[2], partner)

    def row_copy(dst_chip, slot):
        return remote(xs.at[dst_chip], recv.at[pl.ds(4 * slot, 4)], s_send, s_recv.at[slot], 2 * dst_chip + core)

    nbr = lax.rem(chip + 2 * core - 1 + CHIPS, CHIPS)

    def halo(dst_core, side):
        return remote(x_ref.at[aligned(3 * core, BLK)], xc.at[aligned(9 * side, BLK)], h_send.at[dst_core], h_recv.at[side],
                      2 * nbr + dst_core)

    wo_copy = pltpu.make_async_copy(wo_ref, wo_buf, wo_sem)

    with jax.named_scope("issue"):
        for t in range(4):
            for i in range(3):
                w_copy(i, t).start()
        own_x = pltpu.make_async_copy(x_ref, xc.at[pl.ds(pl.multiple_of(BLK + 256 * core, BLK), 256)], loc.at[1])
        own_x.start()
        named_lane = lax.broadcasted_iota(jnp.int32, (1, 128), 1)
        line = jnp.full((1, 128), FAR, jnp.int32)
        for e in range(12):
            line = jnp.where(named_lane == e, rand_ref[e // 3, e % 3], line)
        idx_ref[...] = line
        idx_all[core, chip] = line

    def relayout(step, carry):
        blk, group = step >> 2, step & 3
        rows = x_ref[aligned(step, 16), :]
        rows = jnp.concatenate([rows[:, 128 * c:128 * c + 128] for c in range(16)], axis=0)
        moved = jnp.dot(perm, rows, preferred_element_type=jnp.float32).astype(jnp.bfloat16)
        for a in range(16):
            xs[16 * group + a, blk] = moved[16 * a:16 * a + 16]
        return carry
    with jax.named_scope("relayout"):
        lax.fori_loop(0, 16, relayout, 0)

    def start_idx(i, carry):
        idx_copy(chip ^ i, chip).start()
        return carry

    def start_row(i, carry):
        row_copy(chip ^ i, chip).start()
        return carry
    with jax.named_scope("barrier"):
        pl.semaphore_wait(barrier, 127)
    with jax.named_scope("issue_rows"):
        x_swap(core).start()
        lax.fori_loop(1, CHIPS, start_idx, 0, unroll=7)
        lax.fori_loop(1, CHIPS, start_row, 0, unroll=7)
        own_row = pltpu.make_async_copy(xs.at[chip], recv.at[pl.ds(4 * chip, 4)], loc.at[0])
        own_row.start()
        for t in range(2):
            halo(t, 1 - core).start()

    with jax.named_scope("wait_x"):
        own_x.wait()
        wo_copy.start()
        x_swap(core).wait_send()
        x_swap(1 - core).wait_recv()

    def project(t, carry):
        cols = aligned(t, 256)
        for i in range(3):
            w_copy(i, t).wait()
        rows = xc[BLK:9 * BLK, :]
        q_ref[:, cols] = jnp.dot(rows, w_buf[0, :, cols], preferred_element_type=jnp.float32).astype(jnp.bfloat16)
        k_ref[BLK:9 * BLK, cols] = jnp.dot(rows, w_buf[1, :, cols], preferred_element_type=jnp.float32).astype(jnp.bfloat16)
        v_ref[BLK:9 * BLK, cols] = jnp.dot(rows, w_buf[2, :, cols], preferred_element_type=jnp.float32).astype(jnp.bfloat16)
        return carry
    with jax.named_scope("project"):
        lax.fori_loop(0, 4, project, 0)

    def wait_idx(i, carry):
        idx_copy(chip ^ i, chip ^ i).wait()
        return carry
    with jax.named_scope("wait_idx"):
        lax.fori_loop(1, CHIPS, wait_idx, 0)
        idx_swap(core).start()
        idx_swap(core).wait_send()
        idx_swap(1 - core).wait_recv()
    with jax.named_scope("names"):
        ids = jnp.concatenate([idx_all[0, :, 0, :], idx_all[1, :, 0, :]], axis=0)
        published = [jnp.int32(0), jnp.int32(1), jnp.min(ids)]
        for s in range(3, 14):
            published.append(jnp.min(jnp.where(ids > published[-1], ids, FAR)))

    def wait_row(i, carry):
        row_copy(chip ^ i, chip ^ i).wait()
        return carry
    with jax.named_scope("wait_rows"):
        lax.fori_loop(1, CHIPS, wait_row, 0)
        own_row.wait()

    with jax.named_scope("select"):
        for s in range(SLOTS):
            if s < 14:
                h = published[s]
                rows = recv[jnp.minimum((h >> 3) * 4 + (h & 3), 4 * CHIPS - 1)]
                sel[16 * s:16 * s + 16, :] = jnp.where(((h >> 2) & 1) == core, rows, jnp.zeros_like(rows))
            else:
                sel[16 * s:16 * s + 16, :] = jnp.zeros((16, 128), jnp.bfloat16)
        swap = remote(sel, other, p_sem.at[0], p_sem.at[1], partner)
        swap.start()
        swap.wait()
    with jax.named_scope("publish"):
        moved = jnp.dot(perm, sel[...] + other[...], preferred_element_type=jnp.float32).astype(jnp.bfloat16)
        rows = jnp.concatenate([moved[16 * j:16 * j + 16] for j in range(16)], axis=1)
        out = [jnp.dot(rows, w_buf[i], preferred_element_type=jnp.float32) for i in range(3)]
        row_id = lax.broadcasted_iota(jnp.int32, (SLOTS, 256), 0)
        for j in range(PAIRS):
            cols = slice(128 * j, 128 * j + 128)
            kv = jnp.concatenate([out[1][:, cols], out[2][:, cols]], axis=1)
            gq = jnp.concatenate([out[0][0:1, cols], out[0][1:2, cols]], axis=1)
            kv = jnp.where(row_id == 14, jnp.broadcast_to(gq, (SLOTS, 256)), kv)
            gath[j, coord[2], coord[1], coord[0]] = kv.astype(jnp.bfloat16)

    def copies(j, stage, receive):
        order = ORDERS[j % 3]
        axis = order[stage]
        out = []
        for k in (1, 2, 3):
            to = lax.rem(coord[axis] + k, 4)
            at = list(coord)
            if receive:
                at[axis] = lax.rem(coord[axis] + 4 - k, 4)
            ref = gath.at[(j,) + tuple(slice(None) if a in order[:stage] else at[a] for a in (2, 1, 0))]
            out.append(remote(ref, ref, g_send.at[j, stage, k - 1], g_recv.at[j, stage, k - 1],
                              dev + 2 * scale[axis] * (to - coord[axis])))
        return out

    def advance(j, stage):
        if stage:
            for c in copies(j, stage - 1, True):
                c.wait_recv()
        if stage < 3:
            for c in copies(j, stage, False):
                c.start()

    with jax.named_scope("gather0"):
        for j in range(PAIRS):
            advance(j, 0)
    with jax.named_scope("halo"):
        for t in range(2):
            halo(t, 1 - core).wait_send()
            halo(t, t).wait_recv()

        def project_halo(t, carry):
            cols = aligned(t, 256)
            rows = jnp.concatenate([xc[0:BLK, :], xc[9 * BLK:10 * BLK, :]], axis=0)
            for i, ref in ((1, k_ref), (2, v_ref)):
                out = jnp.dot(rows, w_buf[i, :, cols], preferred_element_type=jnp.float32).astype(jnp.bfloat16)
                ref[0:BLK, cols] = out[0:BLK]
                ref[9 * BLK:10 * BLK, cols] = out[BLK:]
            return carry
        lax.fori_loop(0, 4, project_halo, 0)
    with jax.named_scope("gather1"):
        for j in range(PAIRS):
            advance(j, 1)
    with jax.named_scope("gather2"):
        for j in range(PAIRS):
            advance(j, 2)

    with jax.named_scope("slots"):
        near = [pltpu.make_async_copy(idx_all.at[c, chip], near_s.at[c], loc.at[c]) for c in range(2)]
        for n in near:
            n.start()
        for n in near:
            n.wait()
        for b in range(8):
            for t in range(3):
                named = near_s[b // 4, 0, 3 * (b % 4) + t]
                at = jnp.int32(2)
                for h in published[2:]:
                    at = at + jnp.where(h < named, 1, 0)
                slot_s[3 * b + t] = at

    lane = lax.broadcasted_iota(jnp.int32, (128, 128), 1)
    key = lax.broadcasted_iota(jnp.int32, (1, 256), 1)

    def part_copy(wave, i, slot):
        dst_chip = 16 * wave + i
        return remote(part.at[wave, aligned(i, 8)], parts.at[slot], c_send, c_recv.at[slot], 2 * dst_chip + core)

    def o_copy(wave, rows_of, cols_of):
        return remote(o_ref.at[aligned(rows_of, 256), pl.ds(256 * wave, 256)],
                      full_ref.at[:, aligned(cols_of * 4 + wave, 256)], o_send.at[wave], o_recv.at[wave], partner)

    for wave in range(4):
        with jax.named_scope("wait_wave"):
            for j in (2 * wave, 2 * wave + 1):
                advance(j, 3)

        def unpack(z, carry):
            for j in (2 * wave, 2 * wave + 1):
                rows = gath[j, z].reshape(256, 256)
                moved = jnp.dot(perm, rows, preferred_element_type=jnp.float32).astype(jnp.bfloat16)
                for s in range(15):
                    hot[j, s, aligned(z, 16), :] = moved[s * 16:s * 16 + 16]
            return carry
        with jax.named_scope("unpack"):
            lax.fori_loop(0, 4, unpack, 0)

        with jax.named_scope("globpart"):
            stats = jnp.zeros((128, 128), jnp.float32)
            for t, j in enumerate((2 * wave, 2 * wave + 1)):
                cols = slice(128 * j, 128 * j + 128)
                gq = jnp.concatenate([hot[j, 14, :, 0:128], hot[j, 14, :, 128:256]], axis=0)
                queries = split_heads(gq, 128) * jnp.bfloat16(0.125)
                scores = lax.dot_general(queries, k_ref[BLK:9 * BLK, cols], NT, preferred_element_type=jnp.float32)
                top = jnp.max(scores, axis=1, keepdims=True)
                probs = jnp.exp(scores - top)
                total = jnp.sum(probs, axis=1, keepdims=True)
                out = jnp.dot(probs.astype(jnp.bfloat16), v_ref[BLK:9 * BLK, cols], preferred_element_type=jnp.float32)
                part[wave, :, 128 * t:128 * t + 128] = join_heads(out, 128)
                for h in range(2):
                    rows = slice(128 * h, 128 * h + 128)
                    stats = jnp.where(lane == 2 * t + h, total[rows], stats)
                    stats = jnp.where(lane == 4 + 2 * t + h, top[rows], stats)
            part[wave, :, 256:384] = stats

        def start_part(i, carry):
            j = i ^ (chip & 15)

            @pl.when(16 * wave + j != chip)
            def _():
                part_copy(wave, j, chip).start()
            return carry
        with jax.named_scope("issue_parts"):
            lax.fori_loop(0, 16, start_part, 0)

        def one_block(step, carry):
            b = (step + 4 * (1 - core)) & 7
            named = [0, 1] + [slot_s[3 * b + t] for t in range(3)]
            block_id = chip * 8 + b
            bias = (jnp.where((key < BLK) & (block_id - 1 < 2), NEG, 0.0)
                    + jnp.where((key >= 2 * BLK) & (key < 3 * BLK) & (block_id + 1 >= 8 * CHIPS), NEG, 0.0))
            base = pl.multiple_of(b * BLK, BLK)
            for j in (2 * wave, 2 * wave + 1):
                cols = slice(j * 128, j * 128 + 128)
                queries = split_heads(q_ref[pl.ds(base, BLK), cols], BLK) * jnp.bfloat16(0.125)
                keys = jnp.concatenate([k_ref[pl.ds(base, 3 * BLK), cols]] + [hot[j, s, :, 0:128] for s in named], axis=0)
                vals = jnp.concatenate([v_ref[pl.ds(base, 3 * BLK), cols]] + [hot[j, s, :, 128:256] for s in named], axis=0)
                scores = lax.dot_general(queries, keys, NT, preferred_element_type=jnp.float32)
                scores = jnp.concatenate([scores[:, :256] + bias, scores[:, 256:]], axis=1)
                top = jnp.max(scores, axis=1, keepdims=True)
                probs = jnp.exp(scores - top)
                probs = probs * (1.0 / jnp.sum(probs, axis=1, keepdims=True))
                out = jnp.dot(probs.astype(jnp.bfloat16), vals, preferred_element_type=jnp.float32)
                o_ref[pl.ds(base, BLK), cols] = join_heads(out, BLK).astype(jnp.bfloat16)
            return carry
        with jax.named_scope("blocks"):
            lax.fori_loop(0, 8, one_block, 0)
        o_copy(wave, 1 - core, core).start()

    with jax.named_scope("local"):
        mine = [pltpu.make_async_copy(o_ref.at[aligned(core, 256)], full_ref.at[:, aligned(core, HALF)], loc.at[0]),
                pltpu.make_async_copy(part.at[chip >> 4, aligned(chip & 15, 8)], parts.at[chip], loc.at[1])]
        for m in mine:
            m.start()
        for j in range(PAIRS):
            for stage in range(3):
                for c in copies(j, stage, False):
                    c.wait_send()

        for m in mine:
            m.wait()

    def wait_part(i, carry):
        part_copy(chip >> 4, chip & 15, chip ^ i).wait()
        return carry
    with jax.named_scope("wait_parts"):
        lax.fori_loop(1, CHIPS, wait_part, 0)

    with jax.named_scope("combine"):
        top = lax.fori_loop(0, CHIPS, lambda i, t: jnp.maximum(t, parts[i, :, 256:384]), jnp.full((8, 128), NEG, jnp.float32), unroll=8)

        def add(i, carry):
            num, den = carry
            weight = pltpu.roll(jnp.exp(parts[i, :, 256:384] - top), 124, 1)
            wide = jnp.concatenate([jnp.broadcast_to(weight[:, t:t + 1], (8, HEAD_DIM)) for t in range(4)], axis=1)
            return num + wide * parts[i, :, 0:256], den + weight * parts[i, :, 256:384]
        num, den = lax.fori_loop(0, CHIPS, add, (jnp.zeros((8, 256), jnp.float32), jnp.zeros((8, 128), jnp.float32)), unroll=8)
        wide = jnp.concatenate([jnp.broadcast_to(den[:, t:t + 1], (8, HEAD_DIM)) for t in range(4)], axis=1)
        piece[...] = (num / wide).astype(jnp.bfloat16)

    def glob_slice(src_chip, src_core):
        return glob.at[aligned(src_chip % 16, 8), aligned(src_core * 4 + src_chip // 16, 256)]

    def glob_copy(src_chip, src_core):
        return remote(piece, glob_slice(src_chip, src_core), e_send, e_recv.at[2 * src_chip + src_core], 0)

    def project_out(t, carry):
        cols = aligned(t, 256)
        y_ref[:, cols] = lax.dot_general(full_ref[...], wo_buf[cols, :], NT, preferred_element_type=jnp.float32).astype(jnp.bfloat16)
        return carry

    def project_glob(t, carry):
        cols = aligned(t, 256)
        y_ref[0:128, cols] = lax.dot_general(glob[...], wo_buf[cols, :], NT, preferred_element_type=jnp.float32).astype(jnp.bfloat16)
        return carry

    with jax.named_scope("wait_o"):
        @pl.when(dev != 0)
        def _():
            glob_copy(chip, core).start()

        for wave in range(4):
            o_copy(wave, 1 - core, core).wait_send()
            o_copy(wave, core, 1 - core).wait_recv()
        wo_copy.wait()
    with jax.named_scope("out"):
        lax.fori_loop(0, 8, project_out, 0)

    with jax.named_scope("tail"):
        @pl.when(dev != 0)
        def _():
            glob_copy(chip, core).wait_send()

        @pl.when(dev == 0)
        def _():
            copy = pltpu.make_async_copy(piece, glob_slice(0, 0), loc.at[0])
            copy.start()
            copy.wait()

            def wait_glob(i, carry):
                glob_copy(i // 2, i % 2).wait_recv()
                return carry
            lax.fori_loop(1, 128, wait_glob, 0)
            lax.fori_loop(0, 8, project_glob, 0)


def attend(x, rand_idx, wq, wk, wv, wo):
    vmem = pl.BlockSpec(memory_space=VMEM)
    hbm = pl.BlockSpec(memory_space=pl.ANY)
    dma = pltpu.SemaphoreType.DMA
    bf16, f32 = jnp.bfloat16, jnp.float32
    return pl.pallas_call(
        kernel,
        out_shape=jax.ShapeDtypeStruct((256, WIDTH), bf16),
        in_specs=[vmem, pl.BlockSpec(memory_space=pltpu.SMEM), hbm, hbm, hbm, hbm], out_specs=vmem,
        scratch_shapes=[
            VMEM((1, 128), jnp.int32), VMEM((256, WIDTH), bf16), VMEM((WIDTH, WIDTH), bf16),
            VMEM((CHIPS, 4, 16, 128), bf16), VMEM((640, WIDTH), bf16), VMEM((4 * CHIPS, 16, 128), bf16),
            VMEM((3, WIDTH, HALF), bf16), VMEM((2, CHIPS, 1, 128), jnp.int32), VMEM((256, 128), bf16), VMEM((256, 128), bf16),
            VMEM((512, HALF), bf16), VMEM((640, HALF), bf16), VMEM((640, HALF), bf16),
            VMEM((PAIRS, 4, 4, 4, SLOTS, 256), bf16), VMEM((PAIRS, SLOTS, BLK, 256), bf16), VMEM((512, HALF), bf16),
            VMEM((4, 128, 384), f32), VMEM((CHIPS, 8, 384), f32), VMEM((128, WIDTH), bf16), VMEM((8, 256), bf16),
            pltpu.SMEM((2, 1, 128), jnp.int32), pltpu.SMEM((24,), jnp.int32),
            dma, dma((CHIPS,)), dma((3,)), dma((CHIPS,)), dma((2,)), dma((2,)), dma((2,)), dma((3,)), dma((3, 4)), dma((2,)),
            dma((PAIRS, 3, 3)), dma((PAIRS, 3, 3)), dma, dma((CHIPS,)), dma((4,)), dma((4,)), dma, dma((128,)), dma],
        compiler_params=pltpu.CompilerParams(has_side_effects=True, collective_id=0, vmem_limit_bytes=62 * 1024 * 1024), name="attend",
    )(x, rand_idx, wq, wk, wv, wo)


def solution(mesh):
    row_spec = P(("batch", "seq"), None)
    rep_spec = P(None, None)

    def local_fn(tokens, w_query, w_key, w_value, w_out, rand_idx):
        return attend(tokens, rand_idx, w_query, w_key, w_value, w_out)

    return jax.shard_map(local_fn, mesh=mesh, in_specs=(row_spec, rep_spec, rep_spec, rep_spec, rep_spec, row_spec), out_specs=row_spec, check_vma=False)
```

```python
import jax
import jax.numpy as jnp
from jax import lax
from jax.experimental import pallas as pl
from jax.experimental.pallas import tpu as pltpu
from jax.sharding import PartitionSpec as P

HEAD_DIM = 64
BLK = 64
SLOTS = 16
WIDTH = 2048
HALF = 1024
CHIPS = 64
PAIRS = 8
NEG = -1e30
FAR = 1 << 20
MESH = pl.DeviceIdType.MESH
VMEM = pltpu.VMEM
ORDERS = ((0, 1, 2), (1, 2, 0), (2, 0, 1))
NT = (((1,), (1,)), ((), ()))
TN = (((0,), (0,)), ((), ()))


def permutation():
    row = lax.broadcasted_iota(jnp.int32, (256, 256), 0)
    col = lax.broadcasted_iota(jnp.int32, (256, 256), 1)
    return jnp.where(col == (row & 15) * 16 + (row >> 4), 1.0, 0.0).astype(jnp.bfloat16)


def split_heads(pair, rows):
    lane = lax.broadcasted_iota(jnp.int32, (rows, 128), 1)
    zero = jnp.zeros_like(pair)
    return jnp.concatenate([jnp.where(lane < HEAD_DIM, pair, zero), jnp.where(lane < HEAD_DIM, zero, pair)], axis=0)


def join_heads(out, rows):
    lane = lax.broadcasted_iota(jnp.int32, (rows, 128), 1)
    return jnp.where(lane < HEAD_DIM, out[:rows], out[rows:])


def aligned(i, n):
    return pl.ds(pl.multiple_of(i * n, n), n)


def remote(src, dst, send, recv, dev):
    return pltpu.make_async_remote_copy(src_ref=src, dst_ref=dst, send_sem=send, recv_sem=recv,
                                        device_id={"seq": dev}, device_id_type=MESH)


def kernel(x_ref, rand_ref, wq_ref, wk_ref, wv_ref, wo_ref, y_ref,
           idx_ref, full_ref, wo_buf, xs, xc, recv, w_buf, idx_all, sel, other, q_ref, k_ref, v_ref, gath, hot, o_ref, part, parts, glob, piece, near_s, slot_s,
           s_send, s_recv, i_send, i_recv, x_sem, h_send, h_recv, loc, w_sem, p_sem, g_send, g_recv,
           c_send, c_recv, o_send, o_recv, e_send, e_recv, wo_sem):
    dev = lax.axis_index("seq")
    chip, core = dev // 2, dev % 2
    partner = dev + 1 - 2 * core
    coord = (chip % 4, (chip // 4) % 4, chip // 16)
    scale = (1, 4, 16)
    perm = permutation()

    barrier = pltpu.get_barrier_semaphore()

    def greet(i, carry):
        pl.semaphore_signal(barrier, inc=1, device_id={"seq": dev ^ i}, device_id_type=MESH)
        return carry
    with jax.named_scope("greet"):
        lax.fori_loop(1, 128, greet, 0, unroll=8)

    def w_copy(i, t):
        w = (wq_ref, wk_ref, wv_ref)[i]
        return pltpu.make_async_copy(w.at[:, aligned(core * 4 + t, 256)], w_buf.at[i, :, aligned(t, 256)], w_sem.at[i, t])

    def x_swap(which):
        return remote(x_ref, xc.at[aligned(which, 256)], x_sem.at[0], x_sem.at[1], partner)

    def idx_copy(dst_chip, slot):
        return remote(idx_ref, idx_all.at[core, slot], i_send.at[0], i_recv.at[slot], 2 * dst_chip + core)

    def idx_swap(which):
        return remote(idx_all.at[core], idx_all.at[which], i_send.at[1], i_send.at[2], partner)

    def row_copy(dst_chip, slot):
        return remote(xs.at[dst_chip], recv.at[pl.ds(4 * slot, 4)], s_send, s_recv.at[slot], 2 * dst_chip + core)

    def halo(kv, side):
        ref = (k_ref, v_ref)[kv]
        to = lax.rem(chip + 1 + side * (CHIPS - 2), CHIPS)
        return remote(ref.at[pl.ds((8 - 7 * side) * BLK, BLK)], ref.at[pl.ds(9 * side * BLK, BLK)],
                      h_send.at[kv, side], h_recv.at[kv, side], 2 * to + core)

    wo_copy = pltpu.make_async_copy(wo_ref, wo_buf, wo_sem)

    with jax.named_scope("issue"):
        for t in range(4):
            for i in range(3):
                w_copy(i, t).start()
        own_x = pltpu.make_async_copy(x_ref, xc.at[aligned(core, 256)], loc.at[1])
        own_x.start()
        named_lane = lax.broadcasted_iota(jnp.int32, (1, 128), 1)
        line = jnp.full((1, 128), FAR, jnp.int32)
        for e in range(12):
            line = jnp.where(named_lane == e, rand_ref[e // 3, e % 3], line)
        idx_ref[...] = line
        idx_all[core, chip] = line

    def relayout(step, carry):
        blk, group = step >> 2, step & 3
        rows = x_ref[aligned(step, 16), :]
        rows = jnp.concatenate([rows[:, 128 * c:128 * c + 128] for c in range(16)], axis=0)
        moved = jnp.dot(perm, rows, preferred_element_type=jnp.float32).astype(jnp.bfloat16)
        for a in range(16):
            xs[16 * group + a, blk] = moved[16 * a:16 * a + 16]
        return carry
    with jax.named_scope("relayout"):
        lax.fori_loop(0, 16, relayout, 0)

    def start_idx(i, carry):
        idx_copy(chip ^ i, chip).start()
        return carry

    def start_row(i, carry):
        row_copy(chip ^ i, chip).start()
        return carry
    with jax.named_scope("barrier"):
        pl.semaphore_wait(barrier, 127)
    with jax.named_scope("issue_rows"):
        x_swap(core).start()
        lax.fori_loop(1, CHIPS, start_idx, 0, unroll=7)
        lax.fori_loop(1, CHIPS, start_row, 0, unroll=7)
        own_row = pltpu.make_async_copy(xs.at[chip], recv.at[pl.ds(4 * chip, 4)], loc.at[0])
        own_row.start()

    with jax.named_scope("wait_x"):
        own_x.wait()
        wo_copy.start()
        x_swap(core).wait_send()
        x_swap(1 - core).wait_recv()

    def project(t, carry):
        cols = aligned(t, 256)
        for i in range(3):
            w_copy(i, t).wait()
        rows = xc[...]
        q_ref[:, cols] = jnp.dot(rows, w_buf[0, :, cols], preferred_element_type=jnp.float32).astype(jnp.bfloat16)
        k_ref[BLK:9 * BLK, cols] = jnp.dot(rows, w_buf[1, :, cols], preferred_element_type=jnp.float32).astype(jnp.bfloat16)
        v_ref[BLK:9 * BLK, cols] = jnp.dot(rows, w_buf[2, :, cols], preferred_element_type=jnp.float32).astype(jnp.bfloat16)
        return carry
    with jax.named_scope("project"):
        lax.fori_loop(0, 4, project, 0)

    def wait_idx(i, carry):
        idx_copy(chip ^ i, chip ^ i).wait()
        return carry
    with jax.named_scope("wait_idx"):
        lax.fori_loop(1, CHIPS, wait_idx, 0)
        idx_swap(core).start()
        idx_swap(core).wait_send()
        idx_swap(1 - core).wait_recv()
    with jax.named_scope("names"):
        ids = jnp.concatenate([idx_all[0, :, 0, :], idx_all[1, :, 0, :]], axis=0)
        published = [jnp.int32(0), jnp.int32(1), jnp.min(ids)]
        for s in range(3, 14):
            published.append(jnp.min(jnp.where(ids > published[-1], ids, FAR)))

    def wait_row(i, carry):
        row_copy(chip ^ i, chip ^ i).wait()
        return carry
    with jax.named_scope("wait_rows"):
        lax.fori_loop(1, CHIPS, wait_row, 0)
        own_row.wait()
        for kv in range(2):
            for side in range(2):
                halo(kv, side).start()

    with jax.named_scope("select"):
        for s in range(SLOTS):
            if s < 14:
                h = published[s]
                rows = recv[jnp.minimum((h >> 3) * 4 + (h & 3), 4 * CHIPS - 1)]
                sel[16 * s:16 * s + 16, :] = jnp.where(((h >> 2) & 1) == core, rows, jnp.zeros_like(rows))
            else:
                sel[16 * s:16 * s + 16, :] = jnp.zeros((16, 128), jnp.bfloat16)
        swap = remote(sel, other, p_sem.at[0], p_sem.at[1], partner)
        swap.start()
        swap.wait()
    with jax.named_scope("publish"):
        moved = jnp.dot(perm, sel[...] + other[...], preferred_element_type=jnp.float32).astype(jnp.bfloat16)
        rows = jnp.concatenate([moved[16 * j:16 * j + 16] for j in range(16)], axis=1)
        out = [jnp.dot(rows, w_buf[i], preferred_element_type=jnp.float32) for i in range(3)]
        row_id = lax.broadcasted_iota(jnp.int32, (SLOTS, 256), 0)
        for j in range(PAIRS):
            cols = slice(128 * j, 128 * j + 128)
            kv = jnp.concatenate([out[1][:, cols], out[2][:, cols]], axis=1)
            gq = jnp.concatenate([out[0][0:1, cols], out[0][1:2, cols]], axis=1)
            kv = jnp.where(row_id == 14, jnp.broadcast_to(gq, (SLOTS, 256)), kv)
            gath[j, coord[2], coord[1], coord[0]] = kv.astype(jnp.bfloat16)

    def copies(j, stage, receive):
        order = ORDERS[j % 3]
        axis = order[stage]
        out = []
        for k in (1, 2, 3):
            to = lax.rem(coord[axis] + k, 4)
            at = list(coord)
            if receive:
                at[axis] = lax.rem(coord[axis] + 4 - k, 4)
            ref = gath.at[(j,) + tuple(slice(None) if a in order[:stage] else at[a] for a in (2, 1, 0))]
            out.append(remote(ref, ref, g_send.at[j, stage, k - 1], g_recv.at[j, stage, k - 1],
                              dev + 2 * scale[axis] * (to - coord[axis])))
        return out

    def advance(j, stage):
        if stage:
            for c in copies(j, stage - 1, True):
                c.wait_recv()
        if stage < 3:
            for c in copies(j, stage, False):
                c.start()

    with jax.named_scope("gather0"):
        for j in range(PAIRS):
            advance(j, 0)
    with jax.named_scope("gather1"):
        for j in range(PAIRS):
            advance(j, 1)
    with jax.named_scope("gather2"):
        for j in range(PAIRS):
            advance(j, 2)

    with jax.named_scope("slots"):
        near = [pltpu.make_async_copy(idx_all.at[c, chip], near_s.at[c], loc.at[c]) for c in range(2)]
        for n in near:
            n.start()
        for n in near:
            n.wait()
        for b in range(8):
            for t in range(3):
                named = near_s[b // 4, 0, 3 * (b % 4) + t]
                at = jnp.int32(2)
                for h in published[2:]:
                    at = at + jnp.where(h < named, 1, 0)
                slot_s[3 * b + t] = at

    with jax.named_scope("halo"):
        for kv in range(2):
            for side in range(2):
                halo(kv, side).wait()

    key = lax.broadcasted_iota(jnp.int32, (3 * BLK, 1), 0)

    def part_copy(wave, i, slot):
        dst_chip = 16 * wave + i
        return remote(part.at[wave, aligned(i, 8)], parts.at[slot], c_send, c_recv.at[slot], 2 * dst_chip + core)

    def o_copy(wave, rows_of, cols_of):
        return remote(o_ref.at[aligned(rows_of, 256), aligned(wave, 256)],
                      full_ref.at[:, aligned(cols_of * 4 + wave, 256)], o_send.at[wave], o_recv.at[wave], partner)

    def one_wave(wave, carry):
        with jax.named_scope("wait_wave"):
            for w in range(4):
                @pl.when(wave == w)
                def _():
                    for j in (2 * w, 2 * w + 1):
                        advance(j, 3)

        def unpack(z, carry):
            for t in range(2):
                rows = gath[2 * wave + t, z].reshape(256, 256)
                moved = jnp.dot(perm, rows, preferred_element_type=jnp.float32).astype(jnp.bfloat16)
                for s in range(15):
                    hot[2 * wave + t, s, aligned(z, 16), :] = moved[s * 16:s * 16 + 16]
            return carry
        with jax.named_scope("unpack"):
            lax.fori_loop(0, 4, unpack, 0)

        with jax.named_scope("globpart"):
            sums, tops = [], []
            for t in range(2):
                j = 2 * wave + t
                cols = aligned(j, 128)
                gq = jnp.concatenate([hot[j, 14, :, 0:128], hot[j, 14, :, 128:256]], axis=0)
                queries = split_heads(gq, 128) * jnp.bfloat16(0.125)
                scores = lax.dot_general(k_ref[BLK:9 * BLK, cols], queries, NT, preferred_element_type=jnp.float32)
                top = jnp.max(scores, axis=0, keepdims=True)
                probs = jnp.exp(scores - top)
                total = jnp.sum(probs, axis=0, keepdims=True)
                out = lax.dot_general(probs.astype(jnp.bfloat16), v_ref[BLK:9 * BLK, cols], TN, preferred_element_type=jnp.float32)
                part[wave, :, 128 * t:128 * t + 128] = join_heads(out, 128)
                for h in range(2):
                    sums.append(total[:, 128 * h:128 * h + 128])
                    tops.append(top[:, 128 * h:128 * h + 128])
            stats = jnp.concatenate(sums + tops + [jnp.zeros((120, 128), jnp.float32)], axis=0)
            part[wave, :, 256:384] = stats.T

        def start_part(i, carry):
            j = i ^ (chip & 15)

            @pl.when(16 * wave + j != chip)
            def _():
                part_copy(wave, j, chip).start()
            return carry
        with jax.named_scope("issue_parts"):
            lax.fori_loop(0, 16, start_part, 0)

        with jax.named_scope("blocks"):
            for b in range(8):
                named = [0, 1] + [slot_s[3 * b + t] for t in range(3)]
                rows = slice(b * BLK, b * BLK + BLK)
                near = slice(b * BLK, b * BLK + 3 * BLK)
                for t in range(2):
                    j = 2 * wave + t
                    cols = aligned(j, 128)
                    queries = split_heads(q_ref[rows, cols], BLK) * jnp.bfloat16(0.125)
                    keys = jnp.concatenate([k_ref[near, cols]] + [hot[j, s, :, 0:128] for s in named], axis=0)
                    vals = jnp.concatenate([v_ref[near, cols]] + [hot[j, s, :, 128:256] for s in named], axis=0)
                    scores = lax.dot_general(keys, queries, NT, preferred_element_type=jnp.float32)
                    if b == 2:
                        bias = jnp.where((key < BLK) & (chip == 0), NEG, 0.0)
                    elif b == 7:
                        bias = jnp.where((key >= 2 * BLK) & (chip == CHIPS - 1), NEG, 0.0)
                    if b in (2, 7):
                        scores = jnp.concatenate([scores[:3 * BLK] + bias, scores[3 * BLK:]], axis=0)
                    top = jnp.max(scores, axis=0, keepdims=True)
                    probs = jnp.exp(scores - top)
                    probs = probs * (1.0 / jnp.sum(probs, axis=0, keepdims=True))
                    out = lax.dot_general(probs.astype(jnp.bfloat16), vals, TN, preferred_element_type=jnp.float32)
                    o_ref[rows, cols] = join_heads(out, BLK).astype(jnp.bfloat16)
        o_copy(wave, 1 - core, core).start()
        return carry
    lax.fori_loop(0, 4, one_wave, 0)

    with jax.named_scope("local"):
        mine = [pltpu.make_async_copy(o_ref.at[aligned(core, 256)], full_ref.at[:, aligned(core, HALF)], loc.at[0]),
                pltpu.make_async_copy(part.at[chip >> 4, aligned(chip & 15, 8)], parts.at[chip], loc.at[1])]
        for m in mine:
            m.start()
        for j in range(PAIRS):
            for stage in range(3):
                for c in copies(j, stage, False):
                    c.wait_send()

        for m in mine:
            m.wait()

    def wait_part(i, carry):
        part_copy(chip >> 4, chip & 15, chip ^ i).wait()
        return carry
    with jax.named_scope("wait_parts"):
        lax.fori_loop(1, CHIPS, wait_part, 0)

    with jax.named_scope("combine"):
        top = lax.fori_loop(0, CHIPS, lambda i, t: jnp.maximum(t, parts[i, :, 256:384]), jnp.full((8, 128), NEG, jnp.float32), unroll=8)

        def add(i, carry):
            num, den = carry
            weight = pltpu.roll(jnp.exp(parts[i, :, 256:384] - top), 124, 1)
            wide = jnp.concatenate([jnp.broadcast_to(weight[:, t:t + 1], (8, HEAD_DIM)) for t in range(4)], axis=1)
            return num + wide * parts[i, :, 0:256], den + weight * parts[i, :, 256:384]
        num, den = lax.fori_loop(0, CHIPS, add, (jnp.zeros((8, 256), jnp.float32), jnp.zeros((8, 128), jnp.float32)), unroll=8)
        wide = jnp.concatenate([jnp.broadcast_to(den[:, t:t + 1], (8, HEAD_DIM)) for t in range(4)], axis=1)
        piece[...] = (num / wide).astype(jnp.bfloat16)

    def glob_slice(src_chip, src_core):
        return glob.at[aligned(src_chip % 16, 8), aligned(src_core * 4 + src_chip // 16, 256)]

    def glob_copy(src_chip, src_core):
        return remote(piece, glob_slice(src_chip, src_core), e_send, e_recv.at[2 * src_chip + src_core], 0)

    def project_out(t, carry):
        cols = aligned(t, 256)
        y_ref[:, cols] = lax.dot_general(full_ref[...], wo_buf[cols, :], NT, preferred_element_type=jnp.float32).astype(jnp.bfloat16)
        return carry

    def project_glob(t, carry):
        cols = aligned(t, 256)
        y_ref[0:128, cols] = lax.dot_general(glob[...], wo_buf[cols, :], NT, preferred_element_type=jnp.float32).astype(jnp.bfloat16)
        return carry

    with jax.named_scope("wait_o"):
        @pl.when(dev != 0)
        def _():
            glob_copy(chip, core).start()

        for wave in range(4):
            o_copy(wave, 1 - core, core).wait_send()
            o_copy(wave, core, 1 - core).wait_recv()
        wo_copy.wait()
    with jax.named_scope("out"):
        lax.fori_loop(0, 8, project_out, 0)

    with jax.named_scope("tail"):
        @pl.when(dev != 0)
        def _():
            glob_copy(chip, core).wait_send()

        @pl.when(dev == 0)
        def _():
            copy = pltpu.make_async_copy(piece, glob_slice(0, 0), loc.at[0])
            copy.start()
            copy.wait()

            def wait_glob(i, carry):
                glob_copy(i // 2, i % 2).wait_recv()
                return carry
            lax.fori_loop(1, 128, wait_glob, 0)
            lax.fori_loop(0, 8, project_glob, 0)


def attend(x, rand_idx, wq, wk, wv, wo):
    vmem = pl.BlockSpec(memory_space=VMEM)
    hbm = pl.BlockSpec(memory_space=pl.ANY)
    dma = pltpu.SemaphoreType.DMA
    bf16, f32 = jnp.bfloat16, jnp.float32
    return pl.pallas_call(
        kernel,
        out_shape=jax.ShapeDtypeStruct((256, WIDTH), bf16),
        in_specs=[vmem, pl.BlockSpec(memory_space=pltpu.SMEM), hbm, hbm, hbm, hbm], out_specs=vmem,
        scratch_shapes=[
            VMEM((1, 128), jnp.int32), VMEM((256, WIDTH), bf16), VMEM((WIDTH, WIDTH), bf16),
            VMEM((CHIPS, 4, 16, 128), bf16), VMEM((512, WIDTH), bf16), VMEM((4 * CHIPS, 16, 128), bf16),
            VMEM((3, WIDTH, HALF), bf16), VMEM((2, CHIPS, 1, 128), jnp.int32), VMEM((256, 128), bf16), VMEM((256, 128), bf16),
            VMEM((512, HALF), bf16), VMEM((640, HALF), bf16), VMEM((640, HALF), bf16),
            VMEM((PAIRS, 4, 4, 4, SLOTS, 256), bf16), VMEM((PAIRS, SLOTS, BLK, 256), bf16), VMEM((512, HALF), bf16),
            VMEM((4, 128, 384), f32), VMEM((CHIPS, 8, 384), f32), VMEM((128, WIDTH), bf16), VMEM((8, 256), bf16),
            pltpu.SMEM((2, 1, 128), jnp.int32), pltpu.SMEM((24,), jnp.int32),
            dma, dma((CHIPS,)), dma((3,)), dma((CHIPS,)), dma((2,)), dma((2, 2)), dma((2, 2)), dma((3,)), dma((3, 4)), dma((2,)),
            dma((PAIRS, 3, 3)), dma((PAIRS, 3, 3)), dma, dma((CHIPS,)), dma((4,)), dma((4,)), dma, dma((128,)), dma],
        compiler_params=pltpu.CompilerParams(has_side_effects=True, collective_id=0, vmem_limit_bytes=62 * 1024 * 1024), name="attend",
    )(x, rand_idx, wq, wk, wv, wo)


def solution(mesh):
    row_spec = P(("batch", "seq"), None)
    rep_spec = P(None, None)

    def local_fn(tokens, w_query, w_key, w_value, w_out, rand_idx):
        return attend(tokens, rand_idx, w_query, w_key, w_value, w_out)

    return jax.shard_map(local_fn, mesh=mesh, in_specs=(row_spec, rep_spec, rep_spec, rep_spec, rep_spec, row_spec), out_specs=row_spec, check_vma=False)
```

```python
import jax
import jax.numpy as jnp
from jax import lax
from jax.experimental import pallas as pl
from jax.experimental.pallas import tpu as pltpu
from jax.sharding import PartitionSpec as P

HEAD_DIM = 64
BLK = 64
SLOTS = 16
WIDTH = 2048
HALF = 1024
CHIPS = 64
PAIRS = 8
NEG = -1e30
FAR = 1 << 20
MESH = pl.DeviceIdType.MESH
VMEM = pltpu.VMEM
ORDERS = ((0, 1, 2), (1, 2, 0), (2, 0, 1))
NT = (((1,), (1,)), ((), ()))
TN = (((0,), (0,)), ((), ()))


def permutation():
    row = lax.broadcasted_iota(jnp.int32, (256, 256), 0)
    col = lax.broadcasted_iota(jnp.int32, (256, 256), 1)
    return jnp.where(col == (row & 15) * 16 + (row >> 4), 1.0, 0.0).astype(jnp.bfloat16)


def split_heads(pair, rows):
    lane = lax.broadcasted_iota(jnp.int32, (rows, 128), 1)
    zero = jnp.zeros_like(pair)
    return jnp.concatenate([jnp.where(lane < HEAD_DIM, pair, zero), jnp.where(lane < HEAD_DIM, zero, pair)], axis=0)


def join_heads(out, rows):
    lane = lax.broadcasted_iota(jnp.int32, (rows, 128), 1)
    return jnp.where(lane < HEAD_DIM, out[:rows], out[rows:])


def aligned(i, n):
    return pl.ds(pl.multiple_of(i * n, n), n)


def remote(src, dst, send, recv, dev):
    return pltpu.make_async_remote_copy(src_ref=src, dst_ref=dst, send_sem=send, recv_sem=recv,
                                        device_id={"seq": dev}, device_id_type=MESH)


def kernel(x_ref, rand_ref, wq_ref, wk_ref, wv_ref, wo_ref, y_ref,
           idx_ref, full_ref, wo_buf, xs, xc, recv, w_buf, idx_all, sel, other, q_ref, k_ref, v_ref, gath, hot, o_ref, part, parts, glob, piece, near_s, slot_s, queries_in, queries_g,
           s_send, s_recv, i_send, i_recv, x_sem, h_send, h_recv, loc, w_sem, p_sem, g_send, g_recv,
           c_send, c_recv, o_send, o_recv, e_send, e_recv, wo_sem, b_send, b_recv):
    dev = lax.axis_index("seq")
    chip, core = dev // 2, dev % 2
    partner = dev + 1 - 2 * core
    coord = (chip % 4, (chip // 4) % 4, chip // 16)
    scale = (1, 4, 16)
    perm = permutation()

    barrier = pltpu.get_barrier_semaphore()

    def greet(i, carry):
        pl.semaphore_signal(barrier, inc=1, device_id={"seq": dev ^ i}, device_id_type=MESH)
        return carry
    with jax.named_scope("greet"):
        lax.fori_loop(1, 128, greet, 0, unroll=8)

    def w_copy(i, t):
        w = (wq_ref, wk_ref, wv_ref)[i]
        return pltpu.make_async_copy(w.at[:, aligned(core * 4 + t, 256)], w_buf.at[i, :, aligned(t, 256)], w_sem.at[i, t])

    def x_swap(which):
        return remote(x_ref, xc.at[aligned(which, 256)], x_sem.at[0], x_sem.at[1], partner)

    def idx_copy(dst_chip, slot):
        return remote(idx_ref, idx_all.at[core, slot], i_send.at[0], i_recv.at[slot], 2 * dst_chip + core)

    def idx_swap(which):
        return remote(idx_all.at[core], idx_all.at[which], i_send.at[1], i_send.at[2], partner)

    def row_copy(dst_chip, slot):
        return remote(xs.at[dst_chip], recv.at[pl.ds(4 * slot, 4)], s_send, s_recv.at[slot], 2 * dst_chip + core)

    def halo(kv, side):
        ref = (k_ref, v_ref)[kv]
        to = lax.rem(chip + 1 + side * (CHIPS - 2), CHIPS)
        return remote(ref.at[pl.ds((8 - 7 * side) * BLK, BLK)], ref.at[pl.ds(9 * side * BLK, BLK)],
                      h_send.at[kv, side], h_recv.at[kv, side], 2 * to + core)

    wo_copy = pltpu.make_async_copy(wo_ref, wo_buf, wo_sem)

    with jax.named_scope("issue"):
        for t in range(4):
            for i in range(3):
                w_copy(i, t).start()
        own_x = pltpu.make_async_copy(x_ref, xc.at[aligned(core, 256)], loc.at[1])
        own_x.start()
        named_lane = lax.broadcasted_iota(jnp.int32, (1, 128), 1)
        line = jnp.full((1, 128), FAR, jnp.int32)
        for e in range(12):
            line = jnp.where(named_lane == e, rand_ref[e // 3, e % 3], line)
        idx_ref[...] = line
        idx_all[core, chip] = line

    def relayout(step, carry):
        blk, group = step >> 2, step & 3
        rows = x_ref[aligned(step, 16), :]
        rows = jnp.concatenate([rows[:, 128 * c:128 * c + 128] for c in range(16)], axis=0)
        moved = jnp.dot(perm, rows, preferred_element_type=jnp.float32).astype(jnp.bfloat16)
        for a in range(16):
            xs[16 * group + a, blk] = moved[16 * a:16 * a + 16]
        return carry
    with jax.named_scope("relayout"):
        lax.fori_loop(0, 16, relayout, 0)

    def start_idx(i, carry):
        idx_copy(chip ^ i, chip).start()
        return carry

    def start_row(i, carry):
        row_copy(chip ^ i, chip).start()
        return carry
    with jax.named_scope("barrier"):
        pl.semaphore_wait(barrier, 127)
    with jax.named_scope("issue_rows"):
        x_swap(core).start()
        lax.fori_loop(1, CHIPS, start_idx, 0, unroll=7)
        lax.fori_loop(1, CHIPS, start_row, 0, unroll=7)
        own_row = pltpu.make_async_copy(xs.at[chip], recv.at[pl.ds(4 * chip, 4)], loc.at[0])
        own_row.start()

    with jax.named_scope("wait_x"):
        own_x.wait()
        wo_copy.start()
        x_swap(core).wait_send()
        x_swap(1 - core).wait_recv()

    def project(t, carry):
        cols = aligned(t, 256)
        for i in range(3):
            w_copy(i, t).wait()
        rows = xc[...]
        q_ref[:, cols] = jnp.dot(rows, w_buf[0, :, cols], preferred_element_type=jnp.float32).astype(jnp.bfloat16)
        k_ref[BLK:9 * BLK, cols] = jnp.dot(rows, w_buf[1, :, cols], preferred_element_type=jnp.float32).astype(jnp.bfloat16)
        v_ref[BLK:9 * BLK, cols] = jnp.dot(rows, w_buf[2, :, cols], preferred_element_type=jnp.float32).astype(jnp.bfloat16)
        return carry
    with jax.named_scope("project"):
        lax.fori_loop(0, 4, project, 0)

    def wait_idx(i, carry):
        idx_copy(chip ^ i, chip ^ i).wait()
        return carry
    with jax.named_scope("wait_idx"):
        lax.fori_loop(1, CHIPS, wait_idx, 0)
        idx_swap(core).start()
        idx_swap(core).wait_send()
        idx_swap(1 - core).wait_recv()
    with jax.named_scope("names"):
        ids = jnp.concatenate([idx_all[0, :, 0, :], idx_all[1, :, 0, :]], axis=0)
        published = [jnp.int32(0), jnp.int32(1), jnp.min(ids)]
        for s in range(3, 14):
            published.append(jnp.min(jnp.where(ids > published[-1], ids, FAR)))

    with jax.named_scope("slots"):
        near = [pltpu.make_async_copy(idx_all.at[c, chip], near_s.at[c], loc.at[1 + c]) for c in range(2)]
        for n in near:
            n.start()
        for n in near:
            n.wait()
        for b in range(8):
            for t in range(3):
                named = near_s[b // 4, 0, 3 * (b % 4) + t]
                at = jnp.int32(2)
                for h in published[2:]:
                    at = at + jnp.where(h < named, 1, 0)
                slot_s[3 * b + t] = at

    def wait_row(i, carry):
        row_copy(chip ^ i, chip ^ i).wait()
        return carry
    with jax.named_scope("wait_rows"):
        lax.fori_loop(1, CHIPS, wait_row, 0)
        own_row.wait()
        for kv in range(2):
            for side in range(2):
                halo(kv, side).start()

    def query_copy(dst_chip, src_chip):
        return remote(queries_in.at[chip], queries_in.at[src_chip], b_send, b_recv.at[src_chip], 2 * dst_chip + core)

    with jax.named_scope("select"):
        for s in range(SLOTS):
            if s < 14:
                h = published[s]
                rows = recv[jnp.minimum((h >> 3) * 4 + (h & 3), 4 * CHIPS - 1)]
                sel[16 * s:16 * s + 16, :] = jnp.where(((h >> 2) & 1) == core, rows, jnp.zeros_like(rows))
            else:
                sel[16 * s:16 * s + 16, :] = jnp.zeros((16, 128), jnp.bfloat16)
        swap = remote(sel, other, p_sem.at[0], p_sem.at[1], partner)
        swap.start()
        swap.wait()
    with jax.named_scope("publish"):
        moved = jnp.dot(perm, sel[...] + other[...], preferred_element_type=jnp.float32).astype(jnp.bfloat16)
        rows = jnp.concatenate([moved[16 * j:16 * j + 16] for j in range(16)], axis=1)
        gq = jnp.dot(rows, w_buf[0], preferred_element_type=jnp.float32)
        gq = jnp.concatenate([gq[t:t + 1, 128 * j:128 * j + 128] for t in range(2) for j in range(PAIRS)], axis=0)
        queries_in[chip] = gq.astype(jnp.bfloat16)

        def start_query(i, carry):
            query_copy(chip ^ i, chip).start()
            return carry
        lax.fori_loop(1, CHIPS, start_query, 0, unroll=7)
        out = [jnp.dot(rows, w_buf[i], preferred_element_type=jnp.float32) for i in (1, 2)]
        for j in range(PAIRS):
            cols = slice(128 * j, 128 * j + 128)
            kv = jnp.concatenate([out[0][:, cols], out[1][:, cols]], axis=1)
            gath[j, coord[2], coord[1], coord[0]] = kv.astype(jnp.bfloat16)

    def copies(j, stage, receive):
        order = ORDERS[j % 3]
        axis = order[stage]
        out = []
        for k in (1, 2, 3):
            to = lax.rem(coord[axis] + k, 4)
            at = list(coord)
            if receive:
                at[axis] = lax.rem(coord[axis] + 4 - k, 4)
            ref = gath.at[(j,) + tuple(slice(None) if a in order[:stage] else at[a] for a in (2, 1, 0))]
            out.append(remote(ref, ref, g_send.at[j, stage, k - 1], g_recv.at[j, stage, k - 1],
                              dev + 2 * scale[axis] * (to - coord[axis])))
        return out

    def advance(j, stage):
        if stage:
            for c in copies(j, stage - 1, True):
                c.wait_recv()
        if stage < 3:
            for c in copies(j, stage, False):
                c.start()

    with jax.named_scope("gather0"):
        for j in range(PAIRS):
            advance(j, 0)
    with jax.named_scope("gather1"):
        for j in range(PAIRS):
            advance(j, 1)
    def wait_query(i, carry):
        query_copy(chip ^ i, chip ^ i).wait()
        return carry
    with jax.named_scope("wait_queries"):
        lax.fori_loop(1, CHIPS, wait_query, 0)

    def unpack_queries(z, carry):
        rows = queries_in[pl.ds(16 * z, 16)].reshape(256, 128)
        moved = jnp.dot(perm, rows, preferred_element_type=jnp.float32).astype(jnp.bfloat16)
        for s in range(16):
            queries_g[s, aligned(z, 16), :] = moved[16 * s:16 * s + 16]
        return carry

    def glob_part(wave, carry):
        sums, tops = [], []
        for t in range(2):
            j = 2 * wave + t
            cols = aligned(j, 128)
            gq = jnp.concatenate([queries_g[j], queries_g[PAIRS + j]], axis=0)
            queries = split_heads(gq, 128) * jnp.bfloat16(0.125)
            scores = lax.dot_general(k_ref[BLK:9 * BLK, cols], queries, NT, preferred_element_type=jnp.float32)
            top = jnp.max(scores, axis=0, keepdims=True)
            probs = jnp.exp(scores - top)
            total = jnp.sum(probs, axis=0, keepdims=True)
            out = lax.dot_general(probs.astype(jnp.bfloat16), v_ref[BLK:9 * BLK, cols], TN, preferred_element_type=jnp.float32)
            part[wave, :, 128 * t:128 * t + 128] = join_heads(out, 128)
            for h in range(2):
                sums.append(total[:, 128 * h:128 * h + 128])
                tops.append(top[:, 128 * h:128 * h + 128])
        stats = jnp.concatenate(sums + tops + [jnp.zeros((120, 128), jnp.float32)], axis=0)
        part[wave, :, 256:384] = stats.T
        return carry
    with jax.named_scope("globpart"):
        lax.fori_loop(0, 4, unpack_queries, 0)
        lax.fori_loop(0, 4, glob_part, 0)

    def part_copy(dst_chip, slot):
        return remote(part.at[dst_chip >> 4, aligned(dst_chip & 15, 8)], parts.at[slot], c_send, c_recv.at[slot], 2 * dst_chip + core)

    def start_part(i, carry):
        part_copy(chip ^ i, chip).start()
        return carry
    with jax.named_scope("gather2"):
        for j in range(4):
            advance(j, 2)
        lax.fori_loop(1, CHIPS, start_part, 0, unroll=7)
        own_part = pltpu.make_async_copy(part.at[chip >> 4, aligned(chip & 15, 8)], parts.at[chip], loc.at[1])
        own_part.start()
        for j in range(4, PAIRS):
            advance(j, 2)

    with jax.named_scope("halo"):
        for kv in range(2):
            for side in range(2):
                halo(kv, side).wait()

    key = lax.broadcasted_iota(jnp.int32, (3 * BLK, 1), 0)

    def o_copy(wave, rows_of, cols_of):
        return remote(o_ref.at[aligned(rows_of, 256), aligned(wave, 256)],
                      full_ref.at[:, aligned(cols_of * 4 + wave, 256)], o_send.at[wave], o_recv.at[wave], partner)

    def wait_part(i, carry):
        part_copy(chip ^ i, chip ^ i).wait()
        return carry

    def glob_slice(src_chip, src_core):
        return glob.at[aligned(src_chip % 16, 8), aligned(src_core * 4 + src_chip // 16, 256)]

    def glob_copy(src_chip, src_core):
        return remote(piece, glob_slice(src_chip, src_core), e_send, e_recv.at[2 * src_chip + src_core], 0)

    def combine():
        with jax.named_scope("wait_parts"):
            lax.fori_loop(1, CHIPS, wait_part, 0)
            own_part.wait()
        with jax.named_scope("combine"):
            top = lax.fori_loop(0, CHIPS, lambda i, t: jnp.maximum(t, parts[i, :, 256:384]), jnp.full((8, 128), NEG, jnp.float32), unroll=8)

            def add(i, carry):
                num, den = carry
                weight = pltpu.roll(jnp.exp(parts[i, :, 256:384] - top), 124, 1)
                wide = jnp.concatenate([jnp.broadcast_to(weight[:, t:t + 1], (8, HEAD_DIM)) for t in range(4)], axis=1)
                return num + wide * parts[i, :, 0:256], den + weight * parts[i, :, 256:384]
            num, den = lax.fori_loop(0, CHIPS, add, (jnp.zeros((8, 256), jnp.float32), jnp.zeros((8, 128), jnp.float32)), unroll=8)
            wide = jnp.concatenate([jnp.broadcast_to(den[:, t:t + 1], (8, HEAD_DIM)) for t in range(4)], axis=1)
            piece[...] = (num / wide).astype(jnp.bfloat16)

            @pl.when(dev != 0)
            def _():
                glob_copy(chip, core).start()

    def one_wave(wave, carry):
        pl.when(wave == 3)(combine)
        with jax.named_scope("wait_wave"):
            for w in range(4):
                @pl.when(wave == w)
                def _():
                    for j in (2 * w, 2 * w + 1):
                        advance(j, 3)

        def unpack(z, carry):
            for t in range(2):
                rows = gath[2 * wave + t, z].reshape(256, 256)
                moved = jnp.dot(perm, rows, preferred_element_type=jnp.float32).astype(jnp.bfloat16)
                for s in range(14):
                    hot[2 * wave + t, s, aligned(z, 16), :] = moved[s * 16:s * 16 + 16]
            return carry
        with jax.named_scope("unpack"):
            lax.fori_loop(0, 4, unpack, 0)

        with jax.named_scope("blocks"):
            for b in range(8):
                named = [0, 1] + [slot_s[3 * b + t] for t in range(3)]
                rows = slice(b * BLK, b * BLK + BLK)
                near = slice(b * BLK, b * BLK + 3 * BLK)
                for t in range(2):
                    j = 2 * wave + t
                    cols = aligned(j, 128)
                    queries = split_heads(q_ref[rows, cols], BLK) * jnp.bfloat16(0.125)
                    keys = jnp.concatenate([k_ref[near, cols]] + [hot[j, s, :, 0:128] for s in named], axis=0)
                    vals = jnp.concatenate([v_ref[near, cols]] + [hot[j, s, :, 128:256] for s in named], axis=0)
                    scores = lax.dot_general(keys, queries, NT, preferred_element_type=jnp.float32)
                    if b == 2:
                        bias = jnp.where((key < BLK) & (chip == 0), NEG, 0.0)
                    elif b == 7:
                        bias = jnp.where((key >= 2 * BLK) & (chip == CHIPS - 1), NEG, 0.0)
                    if b in (2, 7):
                        scores = jnp.concatenate([scores[:3 * BLK] + bias, scores[3 * BLK:]], axis=0)
                    top = jnp.max(scores, axis=0, keepdims=True)
                    probs = jnp.exp(scores - top)
                    probs = probs * (1.0 / jnp.sum(probs, axis=0, keepdims=True))
                    out = lax.dot_general(probs.astype(jnp.bfloat16), vals, TN, preferred_element_type=jnp.float32)
                    o_ref[rows, cols] = join_heads(out, BLK).astype(jnp.bfloat16)
        o_copy(wave, 1 - core, core).start()
        return carry
    lax.fori_loop(0, 4, one_wave, 0)

    with jax.named_scope("local"):
        mine = pltpu.make_async_copy(o_ref.at[aligned(core, 256)], full_ref.at[:, aligned(core, HALF)], loc.at[0])
        mine.start()
        for j in range(PAIRS):
            for stage in range(3):
                for c in copies(j, stage, False):
                    c.wait_send()
        mine.wait()

    with jax.named_scope("wait_o"):
        for wave in range(4):
            o_copy(wave, 1 - core, core).wait_send()
            o_copy(wave, core, 1 - core).wait_recv()
        wo_copy.wait()

        @pl.when(dev != 0)
        def _():
            glob_copy(chip, core).wait_send()

        @pl.when(dev == 0)
        def _():
            copy = pltpu.make_async_copy(piece, glob_slice(0, 0), loc.at[0])
            copy.start()
            copy.wait()

            def wait_glob(i, carry):
                glob_copy(i // 2, i % 2).wait_recv()
                return carry
            lax.fori_loop(1, 128, wait_glob, 0)
            full_ref[0:128, :] = glob[...]

    def project_out(t, carry):
        cols = aligned(t, 256)
        y_ref[:, cols] = lax.dot_general(full_ref[...], wo_buf[cols, :], NT, preferred_element_type=jnp.float32)
        return carry
    with jax.named_scope("out"):
        lax.fori_loop(0, 8, project_out, 0)


def attend(x, rand_idx, wq, wk, wv, wo):
    vmem = pl.BlockSpec(memory_space=VMEM)
    hbm = pl.BlockSpec(memory_space=pl.ANY)
    dma = pltpu.SemaphoreType.DMA
    bf16, f32 = jnp.bfloat16, jnp.float32
    return pl.pallas_call(
        kernel,
        out_shape=jax.ShapeDtypeStruct((256, WIDTH), f32),
        in_specs=[vmem, pl.BlockSpec(memory_space=pltpu.SMEM), hbm, hbm, hbm, hbm], out_specs=vmem,
        scratch_shapes=[
            VMEM((1, 128), jnp.int32), VMEM((256, WIDTH), bf16), VMEM((WIDTH, WIDTH), bf16),
            VMEM((CHIPS, 4, 16, 128), bf16), VMEM((512, WIDTH), bf16), VMEM((4 * CHIPS, 16, 128), bf16),
            VMEM((3, WIDTH, HALF), bf16), VMEM((2, CHIPS, 1, 128), jnp.int32), VMEM((256, 128), bf16), VMEM((256, 128), bf16),
            VMEM((512, HALF), bf16), VMEM((640, HALF), bf16), VMEM((640, HALF), bf16),
            VMEM((PAIRS, 4, 4, 4, SLOTS, 256), bf16), VMEM((PAIRS, SLOTS, BLK, 256), bf16), VMEM((512, HALF), bf16),
            VMEM((4, 128, 384), f32), VMEM((CHIPS, 8, 384), f32), VMEM((128, WIDTH), bf16), VMEM((8, 256), bf16),
            pltpu.SMEM((2, 1, 128), jnp.int32), pltpu.SMEM((24,), jnp.int32),
            VMEM((CHIPS, 16, 128), bf16), VMEM((16, BLK, 128), bf16),
            dma, dma((CHIPS,)), dma((3,)), dma((CHIPS,)), dma((2,)), dma((2, 2)), dma((2, 2)), dma((3,)), dma((3, 4)), dma((2,)),
            dma((PAIRS, 3, 3)), dma((PAIRS, 3, 3)), dma, dma((CHIPS,)), dma((4,)), dma((4,)), dma, dma((128,)), dma, dma, dma((CHIPS,))],
        compiler_params=pltpu.CompilerParams(has_side_effects=True, collective_id=0, vmem_limit_bytes=62 * 1024 * 1024), name="attend",
    )(x, rand_idx, wq, wk, wv, wo)


def solution(mesh):
    row_spec = P(("batch", "seq"), None)
    rep_spec = P(None, None)

    def local_fn(tokens, w_query, w_key, w_value, w_out, rand_idx):
        return attend(tokens, rand_idx, w_query, w_key, w_value, w_out).astype(jnp.bfloat16)

    return jax.shard_map(local_fn, mesh=mesh, in_specs=(row_spec, rep_spec, rep_spec, rep_spec, rep_spec, row_spec), out_specs=row_spec, check_vma=False)
```

```python
import jax
import jax.numpy as jnp
from jax import lax
from jax.experimental import pallas as pl
from jax.experimental.pallas import tpu as pltpu
from jax.sharding import PartitionSpec as P

HEAD_DIM = 64
BLK = 64
SLOTS = 16
WIDTH = 2048
HALF = 1024
CHIPS = 64
PAIRS = 8
NEG = -1e30
FAR = 1 << 20
MESH = pl.DeviceIdType.MESH
VMEM = pltpu.VMEM
ORDERS = ((0, 1, 2), (1, 2, 0), (2, 0, 1))
NT = (((1,), (1,)), ((), ()))
TN = (((0,), (0,)), ((), ()))


def permutation():
    row = lax.broadcasted_iota(jnp.int32, (256, 256), 0)
    col = lax.broadcasted_iota(jnp.int32, (256, 256), 1)
    return jnp.where(col == (row & 15) * 16 + (row >> 4), 1.0, 0.0).astype(jnp.bfloat16)


def split_heads(pair, rows):
    lane = lax.broadcasted_iota(jnp.int32, (rows, 128), 1)
    zero = jnp.zeros_like(pair)
    return jnp.concatenate([jnp.where(lane < HEAD_DIM, pair, zero), jnp.where(lane < HEAD_DIM, zero, pair)], axis=0)


def join_heads(out, rows):
    lane = lax.broadcasted_iota(jnp.int32, (rows, 128), 1)
    return jnp.where(lane < HEAD_DIM, out[:rows], out[rows:])


def aligned(i, n):
    return pl.ds(pl.multiple_of(i * n, n), n)


def remote(src, dst, send, recv, dev):
    return pltpu.make_async_remote_copy(src_ref=src, dst_ref=dst, send_sem=send, recv_sem=recv,
                                        device_id={"seq": dev}, device_id_type=MESH)


def kernel(x_ref, rand_ref, wq_ref, wk_ref, wv_ref, wo_ref, y_ref,
           idx_ref, full_ref, wo_buf, xs, xc, recv, w_buf, idx_all, sel, other, q_ref, k_ref, v_ref, gath, hot, o_ref, part, parts, glob, piece, near_s, slot_s, queries_in, queries_g, queries_t,
           s_send, s_recv, i_send, i_recv, x_sem, h_send, h_recv, loc, w_sem, p_sem, g_send, g_recv,
           c_send, c_recv, o_send, o_recv, e_send, e_recv, wo_sem, b_send, b_recv, f_sem):
    dev = lax.axis_index("seq")
    chip, core = dev // 2, dev % 2
    partner = dev + 1 - 2 * core
    coord = (chip % 4, (chip // 4) % 4, chip // 16)
    scale = (1, 4, 16)
    perm = permutation()

    barrier = pltpu.get_barrier_semaphore()

    def greet(i, carry):
        pl.semaphore_signal(barrier, inc=1, device_id={"seq": dev ^ i}, device_id_type=MESH)
        return carry
    with jax.named_scope("greet"):
        lax.fori_loop(1, 128, greet, 0, unroll=8)

    def w_copy(i, t):
        w = (wq_ref, wk_ref, wv_ref)[i]
        return pltpu.make_async_copy(w.at[:, aligned(core * 4 + t, 256)], w_buf.at[i, :, aligned(t, 256)], w_sem.at[i, t])

    def x_swap(which):
        return remote(x_ref, xc.at[aligned(which, 256)], x_sem.at[0], x_sem.at[1], partner)

    def idx_copy(dst_chip, slot):
        return remote(idx_ref, idx_all.at[core, slot], i_send.at[0], i_recv.at[slot], 2 * dst_chip + core)

    def idx_swap(which):
        return remote(idx_all.at[core], idx_all.at[which], i_send.at[1], i_send.at[2], partner)

    def row_copy(dst_chip, slot):
        return remote(xs.at[dst_chip], recv.at[pl.ds(4 * slot, 4)], s_send, s_recv.at[slot], 2 * dst_chip + core)

    def halo(kv, side):
        ref = (k_ref, v_ref)[kv]
        to = lax.rem(chip + 1 + side * (CHIPS - 2), CHIPS)
        return remote(ref.at[pl.ds((8 - 7 * side) * BLK, BLK)], ref.at[pl.ds(9 * side * BLK, BLK)],
                      h_send.at[kv, side], h_recv.at[kv, side], 2 * to + core)

    wo_copy = pltpu.make_async_copy(wo_ref, wo_buf, wo_sem)

    with jax.named_scope("issue"):
        for t in range(4):
            for i in range(3):
                w_copy(i, t).start()
        own_x = pltpu.make_async_copy(x_ref, xc.at[aligned(core, 256)], loc.at[1])
        own_x.start()
        named_lane = lax.broadcasted_iota(jnp.int32, (1, 128), 1)
        line = jnp.full((1, 128), FAR, jnp.int32)
        for e in range(12):
            line = jnp.where(named_lane == e, rand_ref[e // 3, e % 3], line)
        idx_ref[...] = line
        idx_all[core, chip] = line

    def relayout(step, carry):
        blk, group = step >> 2, step & 3
        rows = x_ref[aligned(step, 16), :]
        rows = jnp.concatenate([rows[:, 128 * c:128 * c + 128] for c in range(16)], axis=0)
        moved = jnp.dot(perm, rows, preferred_element_type=jnp.float32).astype(jnp.bfloat16)
        for a in range(16):
            xs[16 * group + a, blk] = moved[16 * a:16 * a + 16]
        return carry
    with jax.named_scope("relayout"):
        lax.fori_loop(0, 16, relayout, 0)

    def start_idx(i, carry):
        idx_copy(chip ^ i, chip).start()
        return carry

    def start_row(i, carry):
        row_copy(chip ^ i, chip).start()
        return carry
    with jax.named_scope("barrier"):
        pl.semaphore_wait(barrier, 127)
    with jax.named_scope("issue_rows"):
        x_swap(core).start()
        lax.fori_loop(1, CHIPS, start_idx, 0, unroll=7)
        lax.fori_loop(1, CHIPS, start_row, 0, unroll=7)
        own_row = pltpu.make_async_copy(xs.at[chip], recv.at[pl.ds(4 * chip, 4)], loc.at[0])
        own_row.start()

    with jax.named_scope("wait_x"):
        own_x.wait()
        wo_copy.start()
        x_swap(core).wait_send()
        x_swap(1 - core).wait_recv()

    def project(t, carry):
        cols = aligned(t, 256)
        for i in range(3):
            w_copy(i, t).wait()
        rows = xc[...]
        q_ref[:, cols] = jnp.dot(rows, w_buf[0, :, cols], preferred_element_type=jnp.float32).astype(jnp.bfloat16)
        k_ref[BLK:9 * BLK, cols] = jnp.dot(rows, w_buf[1, :, cols], preferred_element_type=jnp.float32).astype(jnp.bfloat16)
        v_ref[BLK:9 * BLK, cols] = jnp.dot(rows, w_buf[2, :, cols], preferred_element_type=jnp.float32).astype(jnp.bfloat16)
        return carry
    with jax.named_scope("project"):
        lax.fori_loop(0, 4, project, 0)

    def first_copy(dst_chip):
        return remote(queries_g.at[dst_chip], queries_in.at[dst_chip], f_sem.at[0], f_sem.at[1], 2 * dst_chip + core)

    def query_copy(dst_chip, src_chip):
        return remote(queries_in.at[chip], queries_in.at[src_chip], b_send, b_recv.at[src_chip], 2 * dst_chip + core)

    def relayout_queries(g, carry):
        rows = [q_ref[pl.ds(pl.multiple_of(BLK * t + 16 * g, 16), 16), 128 * j:128 * j + 128] for t in range(2) for j in range(PAIRS)]
        moved = jnp.dot(perm, jnp.concatenate(rows, axis=0), preferred_element_type=jnp.float32).astype(jnp.bfloat16)
        for a in range(16):
            queries_g[16 * g + a] = moved[16 * a:16 * a + 16]
        return carry

    def start_first(i, carry):
        first_copy(i).start()
        return carry

    def sent_first(i, carry):
        first_copy(i).wait_send()
        return carry

    with jax.named_scope("first"):
        @pl.when(chip == 0)
        def _():
            lax.fori_loop(0, 4, relayout_queries, 0)
            lax.fori_loop(1, CHIPS, start_first, 0, unroll=7)
            queries_in[0] = queries_g[0]

    def wait_idx(i, carry):
        idx_copy(chip ^ i, chip ^ i).wait()
        return carry
    with jax.named_scope("wait_idx"):
        lax.fori_loop(1, CHIPS, wait_idx, 0)
        idx_swap(core).start()
        idx_swap(core).wait_send()
        idx_swap(1 - core).wait_recv()
    with jax.named_scope("names"):
        ids = jnp.concatenate([idx_all[0, :, 0, :], idx_all[1, :, 0, :]], axis=0)
        published = [jnp.int32(0), jnp.int32(1), jnp.min(ids)]
        for s in range(3, 14):
            published.append(jnp.min(jnp.where(ids > published[-1], ids, FAR)))

    with jax.named_scope("slots"):
        near = [pltpu.make_async_copy(idx_all.at[c, chip], near_s.at[c], loc.at[1 + c]) for c in range(2)]
        for n in near:
            n.start()
        for n in near:
            n.wait()
        for b in range(8):
            for t in range(3):
                named = near_s[b // 4, 0, 3 * (b % 4) + t]
                at = jnp.int32(2)
                for h in published[2:]:
                    at = at + jnp.where(h < named, 1, 0)
                slot_s[3 * b + t] = at

    def start_query(i, carry):
        query_copy(chip ^ i, chip).start()
        return carry
    with jax.named_scope("pass_on"):
        @pl.when(chip == 0)
        def _():
            lax.fori_loop(1, CHIPS, sent_first, 0)

        @pl.when(chip != 0)
        def _():
            first_copy(chip).wait_recv()
        lax.fori_loop(1, CHIPS, start_query, 0, unroll=7)

    def wait_row(i, carry):
        row_copy(chip ^ i, chip ^ i).wait()
        return carry
    with jax.named_scope("wait_rows"):
        lax.fori_loop(1, CHIPS, wait_row, 0)
        own_row.wait()
        for kv in range(2):
            for side in range(2):
                halo(kv, side).start()

    with jax.named_scope("select"):
        for s in range(SLOTS):
            if s < 14:
                h = published[s]
                rows = recv[jnp.minimum((h >> 3) * 4 + (h & 3), 4 * CHIPS - 1)]
                sel[16 * s:16 * s + 16, :] = jnp.where(((h >> 2) & 1) == core, rows, jnp.zeros_like(rows))
            else:
                sel[16 * s:16 * s + 16, :] = jnp.zeros((16, 128), jnp.bfloat16)
        swap = remote(sel, other, p_sem.at[0], p_sem.at[1], partner)
        swap.start()
        swap.wait()
    with jax.named_scope("publish"):
        moved = jnp.dot(perm, sel[...] + other[...], preferred_element_type=jnp.float32).astype(jnp.bfloat16)
        rows = jnp.concatenate([moved[16 * j:16 * j + 16] for j in range(16)], axis=1)
        out = [jnp.dot(rows, w_buf[i], preferred_element_type=jnp.float32) for i in (1, 2)]
        for j in range(PAIRS):
            cols = slice(128 * j, 128 * j + 128)
            kv = jnp.concatenate([out[0][:, cols], out[1][:, cols]], axis=1)
            gath[j, coord[2], coord[1], coord[0]] = kv.astype(jnp.bfloat16)

    def copies(j, stage, receive):
        order = ORDERS[j % 3]
        axis = order[stage]
        out = []
        for k in (1, 2, 3):
            to = lax.rem(coord[axis] + k, 4)
            at = list(coord)
            if receive:
                at[axis] = lax.rem(coord[axis] + 4 - k, 4)
            ref = gath.at[(j,) + tuple(slice(None) if a in order[:stage] else at[a] for a in (2, 1, 0))]
            out.append(remote(ref, ref, g_send.at[j, stage, k - 1], g_recv.at[j, stage, k - 1],
                              dev + 2 * scale[axis] * (to - coord[axis])))
        return out

    def advance(j, stage):
        if stage:
            for c in copies(j, stage - 1, True):
                c.wait_recv()
        if stage < 3:
            for c in copies(j, stage, False):
                c.start()

    with jax.named_scope("gather0"):
        for j in range(PAIRS):
            advance(j, 0)
    def wait_query(i, carry):
        query_copy(chip ^ i, chip ^ i).wait()
        return carry
    with jax.named_scope("wait_queries"):
        lax.fori_loop(1, CHIPS, wait_query, 0)

    def unpack_queries(z, carry):
        rows = queries_in[pl.ds(16 * z, 16)].reshape(256, 128)
        moved = jnp.dot(perm, rows, preferred_element_type=jnp.float32).astype(jnp.bfloat16)
        for s in range(16):
            queries_t[s, aligned(z, 16), :] = moved[16 * s:16 * s + 16]
        return carry

    def glob_part(wave, carry):
        sums, tops = [], []
        for t in range(2):
            j = 2 * wave + t
            cols = aligned(j, 128)
            gq = jnp.concatenate([queries_t[j], queries_t[PAIRS + j]], axis=0)
            queries = split_heads(gq, 128) * jnp.bfloat16(0.125)
            scores = lax.dot_general(k_ref[BLK:9 * BLK, cols], queries, NT, preferred_element_type=jnp.float32)
            top = jnp.max(scores, axis=0, keepdims=True)
            probs = jnp.exp(scores - top)
            total = jnp.sum(probs, axis=0, keepdims=True)
            out = lax.dot_general(probs.astype(jnp.bfloat16), v_ref[BLK:9 * BLK, cols], TN, preferred_element_type=jnp.float32)
            part[wave, :, 128 * t:128 * t + 128] = join_heads(out, 128)
            for h in range(2):
                sums.append(total[:, 128 * h:128 * h + 128])
                tops.append(top[:, 128 * h:128 * h + 128])
        stats = jnp.concatenate(sums + tops + [jnp.zeros((120, 128), jnp.float32)], axis=0)
        part[wave, :, 256:384] = stats.T
        return carry
    def glob_waves(half, carry):
        with jax.named_scope("globpart"):
            lax.fori_loop(2 * half, 2 * half + 2, glob_part, 0)

        @pl.when(half == 0)
        def _():
            with jax.named_scope("gather1"):
                for j in range(PAIRS):
                    advance(j, 1)
        return carry
    with jax.named_scope("unpack_queries"):
        lax.fori_loop(0, 4, unpack_queries, 0)
    lax.fori_loop(0, 2, glob_waves, 0)

    def part_copy(dst_chip, slot):
        return remote(part.at[dst_chip >> 4, aligned(dst_chip & 15, 8)], parts.at[slot], c_send, c_recv.at[slot], 2 * dst_chip + core)

    def start_part(i, carry):
        part_copy(chip ^ i, chip).start()
        return carry
    with jax.named_scope("gather2"):
        for j in range(4):
            advance(j, 2)
        lax.fori_loop(1, CHIPS, start_part, 0, unroll=7)
        own_part = pltpu.make_async_copy(part.at[chip >> 4, aligned(chip & 15, 8)], parts.at[chip], loc.at[1])
        own_part.start()
        for j in range(4, PAIRS):
            advance(j, 2)

    with jax.named_scope("halo"):
        for kv in range(2):
            for side in range(2):
                halo(kv, side).wait()

    key = lax.broadcasted_iota(jnp.int32, (3 * BLK, 1), 0)

    def o_copy(wave, rows_of, cols_of):
        return remote(o_ref.at[aligned(rows_of, 256), aligned(wave, 256)],
                      full_ref.at[:, aligned(cols_of * 4 + wave, 256)], o_send.at[wave], o_recv.at[wave], partner)

    def wait_part(i, carry):
        part_copy(chip ^ i, chip ^ i).wait()
        return carry

    def glob_slice(src_chip, src_core):
        return glob.at[aligned(src_chip % 16, 8), aligned(src_core * 4 + src_chip // 16, 256)]

    def glob_copy(src_chip, src_core):
        return remote(piece, glob_slice(src_chip, src_core), e_send, e_recv.at[2 * src_chip + src_core], 0)

    def combine():
        with jax.named_scope("wait_parts"):
            lax.fori_loop(1, CHIPS, wait_part, 0)
            own_part.wait()
        with jax.named_scope("combine"):
            top = lax.fori_loop(0, CHIPS, lambda i, t: jnp.maximum(t, parts[i, :, 256:384]), jnp.full((8, 128), NEG, jnp.float32), unroll=8)

            def add(i, carry):
                num, den = carry
                weight = pltpu.roll(jnp.exp(parts[i, :, 256:384] - top), 124, 1)
                wide = jnp.concatenate([jnp.broadcast_to(weight[:, t:t + 1], (8, HEAD_DIM)) for t in range(4)], axis=1)
                return num + wide * parts[i, :, 0:256], den + weight * parts[i, :, 256:384]
            num, den = lax.fori_loop(0, CHIPS, add, (jnp.zeros((8, 256), jnp.float32), jnp.zeros((8, 128), jnp.float32)), unroll=8)
            wide = jnp.concatenate([jnp.broadcast_to(den[:, t:t + 1], (8, HEAD_DIM)) for t in range(4)], axis=1)
            piece[...] = (num / wide).astype(jnp.bfloat16)

            @pl.when(dev != 0)
            def _():
                glob_copy(chip, core).start()

    def one_wave(wave, carry):
        pl.when(wave == 3)(combine)
        with jax.named_scope("wait_wave"):
            for w in range(4):
                @pl.when(wave == w)
                def _():
                    for j in (2 * w, 2 * w + 1):
                        advance(j, 3)

        def unpack(z, carry):
            for t in range(2):
                rows = gath[2 * wave + t, z].reshape(256, 256)
                moved = jnp.dot(perm, rows, preferred_element_type=jnp.float32).astype(jnp.bfloat16)
                for s in range(14):
                    hot[2 * wave + t, s, aligned(z, 16), :] = moved[s * 16:s * 16 + 16]
            return carry
        with jax.named_scope("unpack"):
            lax.fori_loop(0, 4, unpack, 0)

        with jax.named_scope("blocks"):
            for b in range(8):
                named = [0, 1] + [slot_s[3 * b + t] for t in range(3)]
                rows = slice(b * BLK, b * BLK + BLK)
                near = slice(b * BLK, b * BLK + 3 * BLK)
                for t in range(2):
                    j = 2 * wave + t
                    cols = aligned(j, 128)
                    queries = split_heads(q_ref[rows, cols], BLK) * jnp.bfloat16(0.125)
                    keys = jnp.concatenate([k_ref[near, cols]] + [hot[j, s, :, 0:128] for s in named], axis=0)
                    vals = jnp.concatenate([v_ref[near, cols]] + [hot[j, s, :, 128:256] for s in named], axis=0)
                    scores = lax.dot_general(keys, queries, NT, preferred_element_type=jnp.float32)
                    if b == 2:
                        bias = jnp.where((key < BLK) & (chip == 0), NEG, 0.0)
                    elif b == 7:
                        bias = jnp.where((key >= 2 * BLK) & (chip == CHIPS - 1), NEG, 0.0)
                    if b in (2, 7):
                        scores = jnp.concatenate([scores[:3 * BLK] + bias, scores[3 * BLK:]], axis=0)
                    top = jnp.max(scores, axis=0, keepdims=True)
                    probs = jnp.exp(scores - top)
                    probs = probs * (1.0 / jnp.sum(probs, axis=0, keepdims=True))
                    out = lax.dot_general(probs.astype(jnp.bfloat16), vals, TN, preferred_element_type=jnp.float32)
                    o_ref[rows, cols] = join_heads(out, BLK).astype(jnp.bfloat16)
        o_copy(wave, 1 - core, core).start()
        return carry
    lax.fori_loop(0, 4, one_wave, 0)

    with jax.named_scope("local"):
        mine = pltpu.make_async_copy(o_ref.at[aligned(core, 256)], full_ref.at[:, aligned(core, HALF)], loc.at[0])
        mine.start()
        for j in range(PAIRS):
            for stage in range(3):
                for c in copies(j, stage, False):
                    c.wait_send()
        mine.wait()

    with jax.named_scope("wait_o"):
        for wave in range(4):
            o_copy(wave, 1 - core, core).wait_send()
            o_copy(wave, core, 1 - core).wait_recv()
        wo_copy.wait()

        @pl.when(dev != 0)
        def _():
            glob_copy(chip, core).wait_send()

        @pl.when(dev == 0)
        def _():
            copy = pltpu.make_async_copy(piece, glob_slice(0, 0), loc.at[0])
            copy.start()
            copy.wait()

            def wait_glob(i, carry):
                glob_copy(i // 2, i % 2).wait_recv()
                return carry
            lax.fori_loop(1, 128, wait_glob, 0)
            full_ref[0:128, :] = glob[...]

    def project_out(t, carry):
        cols = aligned(t, 256)
        y_ref[:, cols] = lax.dot_general(full_ref[...], wo_buf[cols, :], NT, preferred_element_type=jnp.float32).astype(jnp.bfloat16)
        return carry
    with jax.named_scope("out"):
        lax.fori_loop(0, 8, project_out, 0)


def attend(x, rand_idx, wq, wk, wv, wo):
    vmem = pl.BlockSpec(memory_space=VMEM)
    hbm = pl.BlockSpec(memory_space=pl.ANY)
    dma = pltpu.SemaphoreType.DMA
    bf16, f32 = jnp.bfloat16, jnp.float32
    return pl.pallas_call(
        kernel,
        out_shape=jax.ShapeDtypeStruct((256, WIDTH), bf16),
        in_specs=[vmem, pl.BlockSpec(memory_space=pltpu.SMEM), hbm, hbm, hbm, hbm], out_specs=vmem,
        scratch_shapes=[
            VMEM((1, 128), jnp.int32), VMEM((256, WIDTH), bf16), VMEM((WIDTH, WIDTH), bf16),
            VMEM((CHIPS, 4, 16, 128), bf16), VMEM((512, WIDTH), bf16), VMEM((4 * CHIPS, 16, 128), bf16),
            VMEM((3, WIDTH, HALF), bf16), VMEM((2, CHIPS, 1, 128), jnp.int32), VMEM((256, 128), bf16), VMEM((256, 128), bf16),
            VMEM((512, HALF), bf16), VMEM((640, HALF), bf16), VMEM((640, HALF), bf16),
            VMEM((PAIRS, 4, 4, 4, SLOTS, 256), bf16), VMEM((PAIRS, SLOTS, BLK, 256), bf16), VMEM((512, HALF), bf16),
            VMEM((4, 128, 384), f32), VMEM((CHIPS, 8, 384), f32), VMEM((128, WIDTH), bf16), VMEM((8, 256), bf16),
            pltpu.SMEM((2, 1, 128), jnp.int32), pltpu.SMEM((24,), jnp.int32),
            VMEM((CHIPS, 16, 128), bf16), VMEM((CHIPS, 16, 128), bf16), VMEM((16, BLK, 128), bf16),
            dma, dma((CHIPS,)), dma((3,)), dma((CHIPS,)), dma((2,)), dma((2, 2)), dma((2, 2)), dma((3,)), dma((3, 4)), dma((2,)),
            dma((PAIRS, 3, 3)), dma((PAIRS, 3, 3)), dma, dma((CHIPS,)), dma((4,)), dma((4,)), dma, dma((128,)), dma, dma, dma((CHIPS,)), dma((2,))],
        compiler_params=pltpu.CompilerParams(has_side_effects=True, collective_id=0, vmem_limit_bytes=62 * 1024 * 1024), name="attend",
    )(x, rand_idx, wq, wk, wv, wo)


def solution(mesh):
    row_spec = P(("batch", "seq"), None)
    rep_spec = P(None, None)

    def local_fn(tokens, w_query, w_key, w_value, w_out, rand_idx):
        return attend(tokens, rand_idx, w_query, w_key, w_value, w_out)

    return jax.shard_map(local_fn, mesh=mesh, in_specs=(row_spec, rep_spec, rep_spec, rep_spec, rep_spec, row_spec), out_specs=row_spec, check_vma=False)
```

```python
import jax
import jax.numpy as jnp
from jax import lax
from jax.experimental import pallas as pl
from jax.experimental.pallas import tpu as pltpu
from jax.sharding import PartitionSpec as P

HEAD_DIM = 64
BLK = 64
SLOTS = 16
WIDTH = 2048
HALF = 1024
CHIPS = 64
PAIRS = 8
ALL = (PAIRS,) + tuple(range(PAIRS))
NEG = -1e30
FAR = 1 << 20
MESH = pl.DeviceIdType.MESH
VMEM = pltpu.VMEM
ORDERS = ((0, 1, 2), (1, 2, 0), (2, 0, 1))
NT = (((1,), (1,)), ((), ()))
TN = (((0,), (0,)), ((), ()))


def permutation():
    row = lax.broadcasted_iota(jnp.int32, (256, 256), 0)
    col = lax.broadcasted_iota(jnp.int32, (256, 256), 1)
    return jnp.where(col == (row & 15) * 16 + (row >> 4), 1.0, 0.0).astype(jnp.bfloat16)


def split_heads(pair, rows):
    lane = lax.broadcasted_iota(jnp.int32, (rows, 128), 1)
    zero = jnp.zeros_like(pair)
    return jnp.concatenate([jnp.where(lane < HEAD_DIM, pair, zero), jnp.where(lane < HEAD_DIM, zero, pair)], axis=0)


def join_heads(out, rows):
    lane = lax.broadcasted_iota(jnp.int32, (rows, 128), 1)
    return jnp.where(lane < HEAD_DIM, out[:rows], out[rows:])


def aligned(i, n):
    return pl.ds(pl.multiple_of(i * n, n), n)


def remote(src, dst, send, recv, dev):
    return pltpu.make_async_remote_copy(src_ref=src, dst_ref=dst, send_sem=send, recv_sem=recv,
                                        device_id={"seq": dev}, device_id_type=MESH)


def kernel(x_ref, rand_ref, wq_ref, wk_ref, wv_ref, wo_ref, y_ref,
           idx_ref, full_ref, wo_buf, xs, xc, recv, w_buf, idx_all, sel, other, q_ref, k_ref, v_ref, gath, hot, o_ref, part, parts, glob, piece, near_s, slot_s, gath_q, queries_t, acc,
           s_send, s_recv, i_send, i_recv, x_sem, h_send, h_recv, loc, w_sem, p_sem, g_send, g_recv,
           c_send, c_recv, o_send, o_recv, e_send, e_recv, wo_sem):
    dev = lax.axis_index("seq")
    chip, core = dev // 2, dev % 2
    partner = dev + 1 - 2 * core
    coord = (chip % 4, (chip // 4) % 4, chip // 16)
    scale = (1, 4, 16)
    perm = permutation()

    barrier = pltpu.get_barrier_semaphore()

    def greet(i, carry):
        pl.semaphore_signal(barrier, inc=1, device_id={"seq": dev ^ i}, device_id_type=MESH)
        return carry
    with jax.named_scope("greet"):
        lax.fori_loop(1, 128, greet, 0, unroll=8)

    def w_copy(i, t):
        w = (wq_ref, wk_ref, wv_ref)[i]
        return pltpu.make_async_copy(w.at[:, aligned(core * 4 + t, 256)], w_buf.at[i, :, aligned(t, 256)], w_sem.at[i, t])

    def x_swap(which):
        return remote(x_ref, xc.at[aligned(which, 256)], x_sem.at[0], x_sem.at[1], partner)

    def idx_copy(dst_chip, slot):
        return remote(idx_ref, idx_all.at[core, slot], i_send.at[0], i_recv.at[slot], 2 * dst_chip + core)

    def idx_swap(which):
        return remote(idx_all.at[core], idx_all.at[which], i_send.at[1], i_send.at[2], partner)

    def row_copy(dst_chip, slot):
        return remote(xs.at[dst_chip], recv.at[pl.ds(4 * slot, 4)], s_send, s_recv.at[slot], 2 * dst_chip + core)

    def halo(kv, side):
        ref = (k_ref, v_ref)[kv]
        to = lax.rem(chip + 1 + side * (CHIPS - 2), CHIPS)
        return remote(ref.at[pl.ds((8 - 7 * side) * BLK, BLK)], ref.at[pl.ds(9 * side * BLK, BLK)],
                      h_send.at[kv, side], h_recv.at[kv, side], 2 * to + core)

    wo_copy = pltpu.make_async_copy(wo_ref, wo_buf, wo_sem)

    with jax.named_scope("issue"):
        for t in range(4):
            for i in range(3):
                w_copy(i, t).start()
        own_x = pltpu.make_async_copy(x_ref, xc.at[aligned(core, 256)], loc.at[1])
        own_x.start()
        named_lane = lax.broadcasted_iota(jnp.int32, (1, 128), 1)
        line = jnp.full((1, 128), FAR, jnp.int32)
        for e in range(12):
            line = jnp.where(named_lane == e, rand_ref[e // 3, e % 3], line)
        idx_ref[...] = line
        idx_all[core, chip] = line

    def relayout(step, carry):
        blk, group = step >> 2, step & 3
        rows = x_ref[aligned(step, 16), :]
        rows = jnp.concatenate([rows[:, 128 * c:128 * c + 128] for c in range(16)], axis=0)
        moved = jnp.dot(perm, rows, preferred_element_type=jnp.float32).astype(jnp.bfloat16)
        for a in range(16):
            xs[16 * group + a, blk] = moved[16 * a:16 * a + 16]
        return carry
    with jax.named_scope("relayout"):
        lax.fori_loop(0, 16, relayout, 0)

    def start_idx(i, carry):
        idx_copy(chip ^ i, chip).start()
        return carry

    def start_row(i, carry):
        row_copy(chip ^ i, chip).start()
        return carry
    with jax.named_scope("barrier"):
        pl.semaphore_wait(barrier, 127)
    with jax.named_scope("issue_rows"):
        x_swap(core).start()
        lax.fori_loop(1, CHIPS, start_idx, 0, unroll=7)
        lax.fori_loop(1, CHIPS, start_row, 0, unroll=7)
        own_row = pltpu.make_async_copy(xs.at[chip], recv.at[pl.ds(4 * chip, 4)], loc.at[0])
        own_row.start()

    with jax.named_scope("wait_x"):
        own_x.wait()
        wo_copy.start()
        x_swap(core).wait_send()
        x_swap(1 - core).wait_recv()

    def project(t, carry):
        cols = aligned(t, 256)
        for i in range(3):
            w_copy(i, t).wait()
        rows = xc[...]
        q_ref[:, cols] = jnp.dot(rows, w_buf[0, :, cols], preferred_element_type=jnp.float32).astype(jnp.bfloat16)
        k_ref[BLK:9 * BLK, cols] = jnp.dot(rows, w_buf[1, :, cols], preferred_element_type=jnp.float32).astype(jnp.bfloat16)
        v_ref[BLK:9 * BLK, cols] = jnp.dot(rows, w_buf[2, :, cols], preferred_element_type=jnp.float32).astype(jnp.bfloat16)
        return carry
    with jax.named_scope("project"):
        lax.fori_loop(0, 4, project, 0)

    def wait_idx(i, carry):
        idx_copy(chip ^ i, chip ^ i).wait()
        return carry
    with jax.named_scope("wait_idx"):
        lax.fori_loop(1, CHIPS, wait_idx, 0)
        idx_swap(core).start()
        idx_swap(core).wait_send()
        idx_swap(1 - core).wait_recv()
    with jax.named_scope("names"):
        ids = jnp.concatenate([idx_all[0, :, 0, :], idx_all[1, :, 0, :]], axis=0)
        published = [jnp.int32(0), jnp.int32(1), jnp.min(ids)]
        for s in range(3, 14):
            published.append(jnp.min(jnp.where(ids > published[-1], ids, FAR)))

    with jax.named_scope("slots"):
        near = [pltpu.make_async_copy(idx_all.at[c, chip], near_s.at[c], loc.at[1 + c]) for c in range(2)]
        for n in near:
            n.start()
        for n in near:
            n.wait()
        for b in range(8):
            for t in range(3):
                named = near_s[b // 4, 0, 3 * (b % 4) + t]
                at = jnp.int32(2)
                for h in published[2:]:
                    at = at + jnp.where(h < named, 1, 0)
                slot_s[3 * b + t] = at

    def wait_row(i, carry):
        row_copy(chip ^ i, chip ^ i).wait()
        return carry
    with jax.named_scope("wait_rows"):
        lax.fori_loop(1, CHIPS, wait_row, 0)
        own_row.wait()
        for kv in range(2):
            for side in range(2):
                halo(kv, side).start()

    with jax.named_scope("select"):
        for s in range(SLOTS):
            if s < 14:
                h = published[s]
                rows = recv[jnp.minimum((h >> 3) * 4 + (h & 3), 4 * CHIPS - 1)]
                sel[16 * s:16 * s + 16, :] = jnp.where(((h >> 2) & 1) == core, rows, jnp.zeros_like(rows))
            else:
                sel[16 * s:16 * s + 16, :] = jnp.zeros((16, 128), jnp.bfloat16)
        swap = remote(sel, other, p_sem.at[0], p_sem.at[1], partner)
        swap.start()
        swap.wait()
    with jax.named_scope("publish"):
        moved = jnp.dot(perm, sel[...] + other[...], preferred_element_type=jnp.float32).astype(jnp.bfloat16)
        rows = jnp.concatenate([moved[16 * j:16 * j + 16] for j in range(16)], axis=1)
        gq = jnp.dot(rows, w_buf[0], preferred_element_type=jnp.float32)
        gq = jnp.concatenate([gq[t:t + 1, 128 * j:128 * j + 128] for t in range(2) for j in range(PAIRS)], axis=0)
        gath_q[0, coord[2], coord[1], coord[0]] = gq.astype(jnp.bfloat16)
        out = [jnp.dot(rows, w_buf[i], preferred_element_type=jnp.float32) for i in (1, 2)]
        for j in range(PAIRS):
            cols = slice(128 * j, 128 * j + 128)
            kv = jnp.concatenate([out[0][:, cols], out[1][:, cols]], axis=1)
            gath[j, coord[2], coord[1], coord[0]] = kv.astype(jnp.bfloat16)

    def copies(j, stage, receive):
        order = ORDERS[j % 3]
        axis = order[stage]
        out = []
        for k in (1, 2, 3):
            to = lax.rem(coord[axis] + k, 4)
            at = list(coord)
            if receive:
                at[axis] = lax.rem(coord[axis] + 4 - k, 4)
            buf, at_j = (gath, j) if j < PAIRS else (gath_q, 0)
            ref = buf.at[(at_j,) + tuple(slice(None) if a in order[:stage] else at[a] for a in (2, 1, 0))]
            out.append(remote(ref, ref, g_send.at[j, stage, k - 1], g_recv.at[j, stage, k - 1],
                              dev + 2 * scale[axis] * (to - coord[axis])))
        return out

    def advance(j, stage):
        if stage:
            for c in copies(j, stage - 1, True):
                c.wait_recv()
        if stage < 3:
            for c in copies(j, stage, False):
                c.start()

    with jax.named_scope("gather0"):
        for j in ALL:
            advance(j, 0)
    with jax.named_scope("gather1"):
        for j in ALL:
            advance(j, 1)
    with jax.named_scope("gather2"):
        for j in ALL:
            advance(j, 2)

    with jax.named_scope("wait_queries"):
        advance(PAIRS, 3)

    def unpack_queries(z, carry):
        moved = jnp.dot(perm, gath_q[0, z].reshape(256, 128), preferred_element_type=jnp.float32).astype(jnp.bfloat16)
        for s in range(SLOTS):
            queries_t[s, aligned(z, 16), :] = moved[16 * s:16 * s + 16]
        return carry

    def glob_part(wave, carry):
        sums, tops = [], []
        for t in range(2):
            j = 2 * wave + t
            cols = aligned(j, 128)
            gq = jnp.concatenate([queries_t[j], queries_t[PAIRS + j]], axis=0)
            queries = split_heads(gq, 128) * jnp.bfloat16(0.125)
            scores = lax.dot_general(k_ref[BLK:9 * BLK, cols], queries, NT, preferred_element_type=jnp.float32)
            top = jnp.max(scores, axis=0, keepdims=True)
            probs = jnp.exp(scores - top)
            total = jnp.sum(probs, axis=0, keepdims=True)
            out = lax.dot_general(probs.astype(jnp.bfloat16), v_ref[BLK:9 * BLK, cols], TN, preferred_element_type=jnp.float32)
            part[wave, :, 128 * t:128 * t + 128] = join_heads(out, 128)
            for h in range(2):
                sums.append(total[:, 128 * h:128 * h + 128])
                tops.append(top[:, 128 * h:128 * h + 128])
        stats = jnp.concatenate(sums + tops + [jnp.zeros((120, 128), jnp.float32)], axis=0)
        part[wave, :, 256:384] = stats.T
        return carry

    def part_copy(dst_chip, slot):
        return remote(part.at[dst_chip >> 4, aligned(dst_chip & 15, 8)], parts.at[slot], c_send, c_recv.at[slot], 2 * dst_chip + core)

    def start_part(i, carry):
        part_copy(chip ^ i, chip).start()
        return carry
    with jax.named_scope("globpart"):
        lax.fori_loop(0, 4, unpack_queries, 0)
        lax.fori_loop(0, 4, glob_part, 0)
        lax.fori_loop(1, CHIPS, start_part, 0, unroll=7)
        own_part = pltpu.make_async_copy(part.at[chip >> 4, aligned(chip & 15, 8)], parts.at[chip], loc.at[1])
        own_part.start()

    with jax.named_scope("halo"):
        for kv in range(2):
            for side in range(2):
                halo(kv, side).wait()

    key = lax.broadcasted_iota(jnp.int32, (3 * BLK, 1), 0)

    def o_copy(wave, rows_of, cols_of):
        return remote(o_ref.at[aligned(rows_of, 256), aligned(wave, 256)],
                      full_ref.at[:, aligned(cols_of * 4 + wave, 256)], o_send.at[wave], o_recv.at[wave], partner)

    def one_wave(wave, carry):
        @pl.when(wave > 0)
        def _():
            with jax.named_scope("out_part"):
                project_out(wave - 1, False)
        with jax.named_scope("wait_wave"):
            for w in range(4):
                @pl.when(wave == w)
                def _():
                    for j in (2 * w, 2 * w + 1):
                        advance(j, 3)

        def unpack(z, carry):
            for t in range(2):
                rows = gath[2 * wave + t, z].reshape(256, 256)
                moved = jnp.dot(perm, rows, preferred_element_type=jnp.float32).astype(jnp.bfloat16)
                for s in range(14):
                    hot[2 * wave + t, s, aligned(z, 16), :] = moved[s * 16:s * 16 + 16]
            return carry
        with jax.named_scope("unpack"):
            lax.fori_loop(0, 4, unpack, 0)

        with jax.named_scope("blocks"):
            for b in range(8):
                named = [0, 1] + [slot_s[3 * b + t] for t in range(3)]
                rows = slice(b * BLK, b * BLK + BLK)
                near = slice(b * BLK, b * BLK + 3 * BLK)
                for t in range(2):
                    j = 2 * wave + t
                    cols = aligned(j, 128)
                    queries = split_heads(q_ref[rows, cols], BLK) * jnp.bfloat16(0.125)
                    keys = jnp.concatenate([k_ref[near, cols]] + [hot[j, s, :, 0:128] for s in named], axis=0)
                    vals = jnp.concatenate([v_ref[near, cols]] + [hot[j, s, :, 128:256] for s in named], axis=0)
                    scores = lax.dot_general(keys, queries, NT, preferred_element_type=jnp.float32)
                    if b == 2:
                        bias = jnp.where((key < BLK) & (chip == 0), NEG, 0.0)
                    elif b == 7:
                        bias = jnp.where((key >= 2 * BLK) & (chip == CHIPS - 1), NEG, 0.0)
                    if b in (2, 7):
                        scores = jnp.concatenate([scores[:3 * BLK] + bias, scores[3 * BLK:]], axis=0)
                    top = jnp.max(scores, axis=0, keepdims=True)
                    probs = jnp.exp(scores - top)
                    probs = probs * (1.0 / jnp.sum(probs, axis=0, keepdims=True))
                    out = lax.dot_general(probs.astype(jnp.bfloat16), vals, TN, preferred_element_type=jnp.float32)
                    o_ref[rows, cols] = join_heads(out, BLK).astype(jnp.bfloat16)
        own_o(wave).start()
        o_copy(wave, 1 - core, core).start()
        return carry

    def own_o(wave):
        return pltpu.make_async_copy(o_ref.at[aligned(core, 256), aligned(wave, 256)], full_ref.at[:, aligned(4 * core + wave, 256)], loc.at[0])

    def project_out(wave, last):
        own_o(wave).wait()
        o_copy(wave, 1 - core, core).wait_send()
        o_copy(wave, core, 1 - core).wait_recv()

        def tile(t, carry):
            cols = aligned(t, 256)
            total = acc[:, cols]
            for c in range(2):
                heads = aligned(4 * c + wave, 256)
                total = total + lax.dot_general(full_ref[:, heads], wo_buf[cols, heads], NT, preferred_element_type=jnp.float32)
            if last:
                y_ref[:, cols] = total.astype(jnp.bfloat16)
            else:
                acc[:, cols] = total
            return carry
        lax.fori_loop(0, PAIRS, tile, 0)

    with jax.named_scope("zero"):
        acc[...] = jnp.zeros_like(acc)
        wo_copy.wait()
    lax.fori_loop(0, 4, one_wave, 0)

    with jax.named_scope("local"):
        for j in ALL:
            for stage in range(3):
                for c in copies(j, stage, False):
                    c.wait_send()

    def wait_part(i, carry):
        part_copy(chip ^ i, chip ^ i).wait()
        return carry
    with jax.named_scope("wait_parts"):
        lax.fori_loop(1, CHIPS, wait_part, 0)
        own_part.wait()

    with jax.named_scope("combine"):
        top = lax.fori_loop(0, CHIPS, lambda i, t: jnp.maximum(t, parts[i, :, 256:384]), jnp.full((8, 128), NEG, jnp.float32), unroll=8)

        def add(i, carry):
            num, den = carry
            weight = pltpu.roll(jnp.exp(parts[i, :, 256:384] - top), 124, 1)
            wide = jnp.concatenate([jnp.broadcast_to(weight[:, t:t + 1], (8, HEAD_DIM)) for t in range(4)], axis=1)
            return num + wide * parts[i, :, 0:256], den + weight * parts[i, :, 256:384]
        num, den = lax.fori_loop(0, CHIPS, add, (jnp.zeros((8, 256), jnp.float32), jnp.zeros((8, 128), jnp.float32)), unroll=8)
        wide = jnp.concatenate([jnp.broadcast_to(den[:, t:t + 1], (8, HEAD_DIM)) for t in range(4)], axis=1)
        piece[...] = (num / wide).astype(jnp.bfloat16)

    def glob_slice(src_chip, src_core):
        return glob.at[aligned(src_chip % 16, 8), aligned(src_core * 4 + src_chip // 16, 256)]

    def glob_copy(src_chip, src_core):
        return remote(piece, glob_slice(src_chip, src_core), e_send, e_recv.at[2 * src_chip + src_core], 0)

    def project_glob(t, carry):
        cols = aligned(t, 256)
        y_ref[0:128, cols] = lax.dot_general(glob[...], wo_buf[cols, :], NT, preferred_element_type=jnp.float32).astype(jnp.bfloat16)
        return carry

    @pl.when(dev != 0)
    def _():
        glob_copy(chip, core).start()
    with jax.named_scope("out"):
        project_out(3, True)

    with jax.named_scope("tail"):
        @pl.when(dev != 0)
        def _():
            glob_copy(chip, core).wait_send()

        @pl.when(dev == 0)
        def _():
            copy = pltpu.make_async_copy(piece, glob_slice(0, 0), loc.at[0])
            copy.start()
            copy.wait()

            def wait_glob(i, carry):
                glob_copy(i // 2, i % 2).wait_recv()
                return carry
            lax.fori_loop(1, 128, wait_glob, 0)
            lax.fori_loop(0, PAIRS, project_glob, 0)


def attend(x, rand_idx, wq, wk, wv, wo):
    vmem = pl.BlockSpec(memory_space=VMEM)
    hbm = pl.BlockSpec(memory_space=pl.ANY)
    dma = pltpu.SemaphoreType.DMA
    bf16, f32 = jnp.bfloat16, jnp.float32
    return pl.pallas_call(
        kernel,
        out_shape=jax.ShapeDtypeStruct((256, WIDTH), bf16),
        in_specs=[vmem, pl.BlockSpec(memory_space=pltpu.SMEM), hbm, hbm, hbm, hbm], out_specs=vmem,
        scratch_shapes=[
            VMEM((1, 128), jnp.int32), VMEM((256, WIDTH), bf16), VMEM((WIDTH, WIDTH), bf16),
            VMEM((CHIPS, 4, 16, 128), bf16), VMEM((512, WIDTH), bf16), VMEM((4 * CHIPS, 16, 128), bf16),
            VMEM((3, WIDTH, HALF), bf16), VMEM((2, CHIPS, 1, 128), jnp.int32), VMEM((256, 128), bf16), VMEM((256, 128), bf16),
            VMEM((512, HALF), bf16), VMEM((640, HALF), bf16), VMEM((640, HALF), bf16),
            VMEM((PAIRS, 4, 4, 4, SLOTS, 256), bf16), VMEM((PAIRS, SLOTS, BLK, 256), bf16), VMEM((512, HALF), bf16),
            VMEM((4, 128, 384), f32), VMEM((CHIPS, 8, 384), f32), VMEM((128, WIDTH), bf16), VMEM((8, 256), bf16),
            pltpu.SMEM((2, 1, 128), jnp.int32), pltpu.SMEM((24,), jnp.int32),
            VMEM((1, 4, 4, 4, SLOTS, 128), bf16), VMEM((SLOTS, BLK, 128), bf16), VMEM((256, WIDTH), f32),
            dma, dma((CHIPS,)), dma((3,)), dma((CHIPS,)), dma((2,)), dma((2, 2)), dma((2, 2)), dma((3,)), dma((3, 4)), dma((2,)),
            dma((PAIRS + 1, 3, 3)), dma((PAIRS + 1, 3, 3)), dma, dma((CHIPS,)), dma((4,)), dma((4,)), dma, dma((128,)), dma],
        compiler_params=pltpu.CompilerParams(has_side_effects=True, collective_id=0, vmem_limit_bytes=62 * 1024 * 1024), name="attend",
    )(x, rand_idx, wq, wk, wv, wo)


def solution(mesh):
    row_spec = P(("batch", "seq"), None)
    rep_spec = P(None, None)

    def local_fn(tokens, w_query, w_key, w_value, w_out, rand_idx):
        return attend(tokens, rand_idx, w_query, w_key, w_value, w_out)

    return jax.shard_map(local_fn, mesh=mesh, in_specs=(row_spec, rep_spec, rep_spec, rep_spec, rep_spec, row_spec), out_specs=row_spec, check_vma=False)
```

```python
import jax
import jax.numpy as jnp
from jax import lax
from jax.experimental import pallas as pl
from jax.experimental.pallas import tpu as pltpu
from jax.sharding import PartitionSpec as P

HEAD_DIM = 64
BLK = 64
SLOTS = 16
WIDTH = 2048
HALF = 1024
CHIPS = 64
PAIRS = 8
ALL = (PAIRS,) + tuple(range(PAIRS))
NEG = -1e30
FAR = 1 << 20
MESH = pl.DeviceIdType.MESH
VMEM = pltpu.VMEM
ORDERS = ((0, 1, 2), (1, 2, 0), (2, 0, 1))
NT = (((1,), (1,)), ((), ()))
TN = (((0,), (0,)), ((), ()))


def permutation():
    row = lax.broadcasted_iota(jnp.int32, (256, 256), 0)
    col = lax.broadcasted_iota(jnp.int32, (256, 256), 1)
    return jnp.where(col == (row & 15) * 16 + (row >> 4), 1.0, 0.0).astype(jnp.bfloat16)


def split_heads(pair, rows):
    lane = lax.broadcasted_iota(jnp.int32, (rows, 128), 1)
    zero = jnp.zeros_like(pair)
    return jnp.concatenate([jnp.where(lane < HEAD_DIM, pair, zero), jnp.where(lane < HEAD_DIM, zero, pair)], axis=0)


def join_heads(out, rows):
    lane = lax.broadcasted_iota(jnp.int32, (rows, 128), 1)
    return jnp.where(lane < HEAD_DIM, out[:rows], out[rows:])


def aligned(i, n):
    return pl.ds(pl.multiple_of(i * n, n), n)


def remote(src, dst, send, recv, dev):
    return pltpu.make_async_remote_copy(src_ref=src, dst_ref=dst, send_sem=send, recv_sem=recv,
                                        device_id={"seq": dev}, device_id_type=MESH)


def kernel(x_ref, rand_ref, wq_ref, wk_ref, wv_ref, wo_ref, y_ref,
           idx_ref, full_ref, wo_buf, xs, xc, recv, w_buf, idx_all, sel, other, q_ref, k_ref, v_ref, gath, hot, o_ref, part, parts, glob, piece, near_s, slot_s, gath_q, queries_t, y_buf, wo_t,
           s_send, s_recv, i_send, i_recv, x_sem, h_send, h_recv, loc, w_sem, p_sem, g_send, g_recv,
           c_send, c_recv, o_send, o_recv, e_send, e_recv, wo_sem, own_sem, y_sem):
    dev = lax.axis_index("seq")
    chip, core = dev // 2, dev % 2
    partner = dev + 1 - 2 * core
    coord = (chip % 4, (chip // 4) % 4, chip // 16)
    scale = (1, 4, 16)
    perm = permutation()

    barrier = pltpu.get_barrier_semaphore()

    def greet(i, carry):
        pl.semaphore_signal(barrier, inc=1, device_id={"seq": dev ^ i}, device_id_type=MESH)
        return carry
    with jax.named_scope("greet"):
        lax.fori_loop(1, 128, greet, 0, unroll=8)

    def w_copy(i, t):
        w = (wq_ref, wk_ref, wv_ref)[i]
        return pltpu.make_async_copy(w.at[:, aligned(core * 4 + t, 256)], w_buf.at[i, :, aligned(t, 256)], w_sem.at[i, t])

    def x_swap(which):
        return remote(x_ref, xc.at[aligned(which, 256)], x_sem.at[0], x_sem.at[1], partner)

    def idx_copy(dst_chip, slot):
        return remote(idx_ref, idx_all.at[core, slot], i_send.at[0], i_recv.at[slot], 2 * dst_chip + core)

    def idx_swap(which):
        return remote(idx_all.at[core], idx_all.at[which], i_send.at[1], i_send.at[2], partner)

    def row_copy(dst_chip, slot):
        return remote(xs.at[dst_chip], recv.at[pl.ds(4 * slot, 4)], s_send, s_recv.at[slot], 2 * dst_chip + core)

    def halo(kv, side):
        ref = (k_ref, v_ref)[kv]
        to = lax.rem(chip + 1 + side * (CHIPS - 2), CHIPS)
        return remote(ref.at[pl.ds((8 - 7 * side) * BLK, BLK)], ref.at[pl.ds(9 * side * BLK, BLK)],
                      h_send.at[kv, side], h_recv.at[kv, side], 2 * to + core)

    wo_copy = pltpu.make_async_copy(wo_ref, wo_buf, wo_sem)

    with jax.named_scope("issue"):
        for t in range(4):
            for i in range(3):
                w_copy(i, t).start()
        own_x = pltpu.make_async_copy(x_ref, xc.at[aligned(core, 256)], loc.at[1])
        own_x.start()
        named_lane = lax.broadcasted_iota(jnp.int32, (1, 128), 1)
        line = jnp.full((1, 128), FAR, jnp.int32)
        for e in range(12):
            line = jnp.where(named_lane == e, rand_ref[e // 3, e % 3], line)
        idx_ref[...] = line
        idx_all[core, chip] = line

    def relayout(step, carry):
        blk, group = step >> 2, step & 3
        rows = x_ref[aligned(step, 16), :]
        rows = jnp.concatenate([rows[:, 128 * c:128 * c + 128] for c in range(16)], axis=0)
        moved = jnp.dot(perm, rows, preferred_element_type=jnp.float32).astype(jnp.bfloat16)
        for a in range(16):
            xs[16 * group + a, blk] = moved[16 * a:16 * a + 16]
        return carry
    with jax.named_scope("relayout"):
        lax.fori_loop(0, 16, relayout, 0)

    def start_idx(i, carry):
        idx_copy(chip ^ i, chip).start()
        return carry

    def start_row(i, carry):
        row_copy(chip ^ i, chip).start()
        return carry
    with jax.named_scope("barrier"):
        pl.semaphore_wait(barrier, 127)
    with jax.named_scope("issue_rows"):
        x_swap(core).start()
        lax.fori_loop(1, CHIPS, start_idx, 0, unroll=7)
        lax.fori_loop(1, CHIPS, start_row, 0, unroll=7)
        own_row = pltpu.make_async_copy(xs.at[chip], recv.at[pl.ds(4 * chip, 4)], loc.at[0])
        own_row.start()

    with jax.named_scope("wait_x"):
        own_x.wait()
        wo_copy.start()
        x_swap(core).wait_send()
        x_swap(1 - core).wait_recv()

    def project(t, carry):
        cols = aligned(t, 256)
        for i in range(3):
            w_copy(i, t).wait()
        rows = xc[...]
        q_ref[:, cols] = jnp.dot(rows, w_buf[0, :, cols], preferred_element_type=jnp.float32).astype(jnp.bfloat16)
        k_ref[BLK:9 * BLK, cols] = jnp.dot(rows, w_buf[1, :, cols], preferred_element_type=jnp.float32).astype(jnp.bfloat16)
        v_ref[BLK:9 * BLK, cols] = jnp.dot(rows, w_buf[2, :, cols], preferred_element_type=jnp.float32).astype(jnp.bfloat16)
        return carry
    with jax.named_scope("project"):
        lax.fori_loop(0, 4, project, 0)

    def wait_idx(i, carry):
        idx_copy(chip ^ i, chip ^ i).wait()
        return carry
    with jax.named_scope("wait_idx"):
        lax.fori_loop(1, CHIPS, wait_idx, 0)
        idx_swap(core).start()
        idx_swap(core).wait_send()
        idx_swap(1 - core).wait_recv()
    with jax.named_scope("names"):
        ids = jnp.concatenate([idx_all[0, :, 0, :], idx_all[1, :, 0, :]], axis=0)
        published = [jnp.int32(0), jnp.int32(1), jnp.min(ids)]
        for s in range(3, 14):
            published.append(jnp.min(jnp.where(ids > published[-1], ids, FAR)))

    with jax.named_scope("slots"):
        near = [pltpu.make_async_copy(idx_all.at[c, chip], near_s.at[c], loc.at[1 + c]) for c in range(2)]
        for n in near:
            n.start()
        for n in near:
            n.wait()
        for b in range(8):
            for t in range(3):
                named = near_s[b // 4, 0, 3 * (b % 4) + t]
                at = jnp.int32(2)
                for h in published[2:]:
                    at = at + jnp.where(h < named, 1, 0)
                slot_s[3 * b + t] = at

    def wait_row(i, carry):
        row_copy(chip ^ i, chip ^ i).wait()
        return carry
    with jax.named_scope("wait_rows"):
        lax.fori_loop(1, CHIPS, wait_row, 0)
        own_row.wait()
        for kv in range(2):
            for side in range(2):
                halo(kv, side).start()

    with jax.named_scope("select"):
        for s in range(SLOTS):
            if s < 14:
                h = published[s]
                rows = recv[jnp.minimum((h >> 3) * 4 + (h & 3), 4 * CHIPS - 1)]
                sel[16 * s:16 * s + 16, :] = jnp.where(((h >> 2) & 1) == core, rows, jnp.zeros_like(rows))
            else:
                sel[16 * s:16 * s + 16, :] = jnp.zeros((16, 128), jnp.bfloat16)
        swap = remote(sel, other, p_sem.at[0], p_sem.at[1], partner)
        swap.start()
        swap.wait()
    with jax.named_scope("publish"):
        moved = jnp.dot(perm, sel[...] + other[...], preferred_element_type=jnp.float32).astype(jnp.bfloat16)
        rows = jnp.concatenate([moved[16 * j:16 * j + 16] for j in range(16)], axis=1)
        gq = jnp.dot(rows, w_buf[0], preferred_element_type=jnp.float32)
        gq = jnp.concatenate([gq[t:t + 1, 128 * j:128 * j + 128] for t in range(2) for j in range(PAIRS)], axis=0)
        gath_q[0, coord[2], coord[1], coord[0]] = gq.astype(jnp.bfloat16)
        out = [jnp.dot(rows, w_buf[i], preferred_element_type=jnp.float32) for i in (1, 2)]
        for j in range(PAIRS):
            cols = slice(128 * j, 128 * j + 128)
            kv = jnp.concatenate([out[0][:, cols], out[1][:, cols]], axis=1)
            gath[j, coord[2], coord[1], coord[0]] = kv.astype(jnp.bfloat16)

    def copies(j, stage, receive):
        order = ORDERS[j % 3]
        axis = order[stage]
        out = []
        for k in (1, 2, 3):
            to = lax.rem(coord[axis] + k, 4)
            at = list(coord)
            if receive:
                at[axis] = lax.rem(coord[axis] + 4 - k, 4)
            buf, at_j = (gath, j) if j < PAIRS else (gath_q, 0)
            ref = buf.at[(at_j,) + tuple(slice(None) if a in order[:stage] else at[a] for a in (2, 1, 0))]
            out.append(remote(ref, ref, g_send.at[j, stage, k - 1], g_recv.at[j, stage, k - 1],
                              dev + 2 * scale[axis] * (to - coord[axis])))
        return out

    def advance(j, stage):
        if stage:
            for c in copies(j, stage - 1, True):
                c.wait_recv()
        if stage < 3:
            for c in copies(j, stage, False):
                c.start()

    with jax.named_scope("gather0"):
        for j in ALL:
            advance(j, 0)
    def turn(i, carry):
        a, b = aligned(i >> 3, 256), aligned(i & 7, 256)
        wo_t[a, b] = wo_buf[b, a].T
        return carry
    with jax.named_scope("turn"):
        wo_copy.wait()
        lax.fori_loop(0, 32, turn, 0)
    with jax.named_scope("gather1"):
        for j in ALL:
            advance(j, 1)
    with jax.named_scope("turn2"):
        lax.fori_loop(32, CHIPS, turn, 0)
    with jax.named_scope("gather2"):
        for j in ALL:
            advance(j, 2)

    with jax.named_scope("wait_queries"):
        advance(PAIRS, 3)

    def unpack_queries(z, carry):
        moved = jnp.dot(perm, gath_q[0, z].reshape(256, 128), preferred_element_type=jnp.float32).astype(jnp.bfloat16)
        for s in range(SLOTS):
            queries_t[s, aligned(z, 16), :] = moved[16 * s:16 * s + 16]
        return carry

    def glob_part(wave, carry):
        sums, tops = [], []
        for t in range(2):
            j = 2 * wave + t
            cols = aligned(j, 128)
            gq = jnp.concatenate([queries_t[j], queries_t[PAIRS + j]], axis=0)
            queries = split_heads(gq, 128) * jnp.bfloat16(0.125)
            scores = lax.dot_general(k_ref[BLK:9 * BLK, cols], queries, NT, preferred_element_type=jnp.float32)
            top = jnp.max(scores, axis=0, keepdims=True)
            probs = jnp.exp(scores - top)
            total = jnp.sum(probs, axis=0, keepdims=True)
            out = lax.dot_general(probs.astype(jnp.bfloat16), v_ref[BLK:9 * BLK, cols], TN, preferred_element_type=jnp.float32)
            part[wave, :, 128 * t:128 * t + 128] = join_heads(out, 128)
            for h in range(2):
                sums.append(total[:, 128 * h:128 * h + 128])
                tops.append(top[:, 128 * h:128 * h + 128])
        stats = jnp.concatenate(sums + tops + [jnp.zeros((120, 128), jnp.float32)], axis=0)
        part[wave, :, 256:384] = stats.T
        return carry

    def part_copy(dst_chip, slot):
        return remote(part.at[dst_chip >> 4, aligned(dst_chip & 15, 8)], parts.at[slot], c_send, c_recv.at[slot], 2 * dst_chip + core)

    def start_part(i, carry):
        part_copy(chip ^ i, chip).start()
        return carry
    with jax.named_scope("globpart"):
        lax.fori_loop(0, 4, unpack_queries, 0)
        lax.fori_loop(0, 4, glob_part, 0)
        lax.fori_loop(1, CHIPS, start_part, 0, unroll=7)
        own_part = pltpu.make_async_copy(part.at[chip >> 4, aligned(chip & 15, 8)], parts.at[chip], loc.at[1])
        own_part.start()

    with jax.named_scope("halo"):
        for kv in range(2):
            for side in range(2):
                halo(kv, side).wait()

    key = lax.broadcasted_iota(jnp.int32, (3 * BLK, 1), 0)

    def o_copy(wave, rows_of, cols_of):
        return remote(o_ref.at[aligned(rows_of, 256), aligned(wave, 256)],
                      full_ref.at[:, aligned(cols_of * 4 + wave, 256)], o_send.at[wave], o_recv.at[wave], partner)

    def one_wave(wave, carry):
        with jax.named_scope("wait_wave"):
            for w in range(4):
                @pl.when(wave == w)
                def _():
                    for j in (2 * w, 2 * w + 1):
                        advance(j, 3)

        def unpack(z, carry):
            for t in range(2):
                rows = gath[2 * wave + t, z].reshape(256, 256)
                moved = jnp.dot(perm, rows, preferred_element_type=jnp.float32).astype(jnp.bfloat16)
                for s in range(14):
                    hot[2 * wave + t, s, aligned(z, 16), :] = moved[s * 16:s * 16 + 16]
            return carry
        with jax.named_scope("unpack"):
            lax.fori_loop(0, 4, unpack, 0)

        with jax.named_scope("blocks"):
            for b in range(8):
                named = [0, 1] + [slot_s[3 * b + t] for t in range(3)]
                rows = slice(b * BLK, b * BLK + BLK)
                near = slice(b * BLK, b * BLK + 3 * BLK)
                for t in range(2):
                    j = 2 * wave + t
                    cols = aligned(j, 128)
                    queries = split_heads(q_ref[rows, cols], BLK) * jnp.bfloat16(0.125)
                    keys = jnp.concatenate([k_ref[near, cols]] + [hot[j, s, :, 0:128] for s in named], axis=0)
                    vals = jnp.concatenate([v_ref[near, cols]] + [hot[j, s, :, 128:256] for s in named], axis=0)
                    scores = lax.dot_general(keys, queries, NT, preferred_element_type=jnp.float32)
                    if b == 2:
                        bias = jnp.where((key < BLK) & (chip == 0), NEG, 0.0)
                    elif b == 7:
                        bias = jnp.where((key >= 2 * BLK) & (chip == CHIPS - 1), NEG, 0.0)
                    if b in (2, 7):
                        scores = jnp.concatenate([scores[:3 * BLK] + bias, scores[3 * BLK:]], axis=0)
                    top = jnp.max(scores, axis=0, keepdims=True)
                    probs = jnp.exp(scores - top)
                    probs = probs * (1.0 / jnp.sum(probs, axis=0, keepdims=True))
                    out = lax.dot_general(probs.astype(jnp.bfloat16), vals, TN, preferred_element_type=jnp.float32)
                    o_ref[rows, cols] = join_heads(out, BLK).astype(jnp.bfloat16)
        own_o(wave).start()
        o_copy(wave, 1 - core, core).start()
        return carry

    def own_o(wave):
        return pltpu.make_async_copy(o_ref.at[aligned(core, 256), aligned(wave, 256)], full_ref.at[:, aligned(4 * core + wave, 256)], own_sem.at[wave])

    lax.fori_loop(0, 4, one_wave, 0)

    with jax.named_scope("local"):
        for j in ALL:
            for stage in range(3):
                for c in copies(j, stage, False):
                    c.wait_send()

    def wait_part(i, carry):
        part_copy(chip ^ i, chip ^ i).wait()
        return carry
    with jax.named_scope("wait_parts"):
        lax.fori_loop(1, CHIPS, wait_part, 0)
        own_part.wait()

    with jax.named_scope("combine"):
        top = lax.fori_loop(0, CHIPS, lambda i, t: jnp.maximum(t, parts[i, :, 256:384]), jnp.full((8, 128), NEG, jnp.float32), unroll=8)

        def add(i, carry):
            num, den = carry
            weight = pltpu.roll(jnp.exp(parts[i, :, 256:384] - top), 124, 1)
            wide = jnp.concatenate([jnp.broadcast_to(weight[:, t:t + 1], (8, HEAD_DIM)) for t in range(4)], axis=1)
            return num + wide * parts[i, :, 0:256], den + weight * parts[i, :, 256:384]
        num, den = lax.fori_loop(0, CHIPS, add, (jnp.zeros((8, 256), jnp.float32), jnp.zeros((8, 128), jnp.float32)), unroll=8)
        wide = jnp.concatenate([jnp.broadcast_to(den[:, t:t + 1], (8, HEAD_DIM)) for t in range(4)], axis=1)
        piece[...] = (num / wide).astype(jnp.bfloat16)

    def glob_slice(src_chip, src_core):
        return glob.at[aligned(src_chip % 16, 8), aligned(src_core * 4 + src_chip // 16, 256)]

    def glob_copy(src_chip, src_core):
        return remote(piece, glob_slice(src_chip, src_core), e_send, e_recv.at[2 * src_chip + src_core], 0)

    @pl.when(dev != 0)
    def _():
        glob_copy(chip, core).start()

    def y_copy(half, t):
        at = (pl.ds(128 * half, 128), aligned(t, 256))
        return pltpu.make_async_copy(y_buf.at[at], y_ref.at[at], y_sem.at[half, t])

    def project_out(t, carry):
        cols = aligned(t, 256)
        y_buf[:, cols] = jnp.dot(full_ref[...], wo_t[:, cols], preferred_element_type=jnp.float32).astype(jnp.bfloat16)
        y_copy(1, t).start()

        @pl.when(dev != 0)
        def _():
            y_copy(0, t).start()
        return carry

    def project_glob(t, carry):
        cols = aligned(t, 256)
        y_buf[0:128, cols] = jnp.dot(glob[...], wo_t[:, cols], preferred_element_type=jnp.float32).astype(jnp.bfloat16)
        y_copy(0, t).start()
        return carry

    with jax.named_scope("wait_o"):
        for wave in range(4):
            own_o(wave).wait()
            o_copy(wave, 1 - core, core).wait_send()
            o_copy(wave, core, 1 - core).wait_recv()
    with jax.named_scope("out"):
        lax.fori_loop(0, PAIRS, project_out, 0)

    with jax.named_scope("tail"):
        @pl.when(dev != 0)
        def _():
            glob_copy(chip, core).wait_send()

        @pl.when(dev == 0)
        def _():
            copy = pltpu.make_async_copy(piece, glob_slice(0, 0), loc.at[0])
            copy.start()
            copy.wait()

            def wait_glob(i, carry):
                glob_copy(i // 2, i % 2).wait_recv()
                return carry
            lax.fori_loop(1, 128, wait_glob, 0)
            lax.fori_loop(0, PAIRS, project_glob, 0)

        def written(t, carry):
            y_copy(0, t).wait()
            y_copy(1, t).wait()
            return carry
        lax.fori_loop(0, PAIRS, written, 0)


def attend(x, rand_idx, wq, wk, wv, wo):
    vmem = pl.BlockSpec(memory_space=VMEM)
    hbm = pl.BlockSpec(memory_space=pl.ANY)
    dma = pltpu.SemaphoreType.DMA
    bf16, f32 = jnp.bfloat16, jnp.float32
    return pl.pallas_call(
        kernel,
        out_shape=jax.ShapeDtypeStruct((256, WIDTH), bf16),
        in_specs=[vmem, pl.BlockSpec(memory_space=pltpu.SMEM), hbm, hbm, hbm, hbm], out_specs=hbm,
        scratch_shapes=[
            VMEM((1, 128), jnp.int32), VMEM((256, WIDTH), bf16), VMEM((WIDTH, WIDTH), bf16),
            VMEM((CHIPS, 4, 16, 128), bf16), VMEM((512, WIDTH), bf16), VMEM((4 * CHIPS, 16, 128), bf16),
            VMEM((3, WIDTH, HALF), bf16), VMEM((2, CHIPS, 1, 128), jnp.int32), VMEM((256, 128), bf16), VMEM((256, 128), bf16),
            VMEM((512, HALF), bf16), VMEM((640, HALF), bf16), VMEM((640, HALF), bf16),
            VMEM((PAIRS, 4, 4, 4, SLOTS, 256), bf16), VMEM((PAIRS, SLOTS, BLK, 256), bf16), VMEM((512, HALF), bf16),
            VMEM((4, 128, 384), f32), VMEM((CHIPS, 8, 384), f32), VMEM((128, WIDTH), bf16), VMEM((8, 256), bf16),
            pltpu.SMEM((2, 1, 128), jnp.int32), pltpu.SMEM((24,), jnp.int32),
            VMEM((1, 4, 4, 4, SLOTS, 128), bf16), VMEM((SLOTS, BLK, 128), bf16), VMEM((256, WIDTH), bf16), VMEM((WIDTH, WIDTH), bf16),
            dma, dma((CHIPS,)), dma((3,)), dma((CHIPS,)), dma((2,)), dma((2, 2)), dma((2, 2)), dma((3,)), dma((3, 4)), dma((2,)),
            dma((PAIRS + 1, 3, 3)), dma((PAIRS + 1, 3, 3)), dma, dma((CHIPS,)), dma((4,)), dma((4,)), dma, dma((128,)), dma, dma((4,)), dma((2, PAIRS))],
        compiler_params=pltpu.CompilerParams(has_side_effects=True, collective_id=0, vmem_limit_bytes=62 * 1024 * 1024), name="attend",
    )(x, rand_idx, wq, wk, wv, wo)


def solution(mesh):
    row_spec = P(("batch", "seq"), None)
    rep_spec = P(None, None)

    def local_fn(tokens, w_query, w_key, w_value, w_out, rand_idx):
        return attend(tokens, rand_idx, w_query, w_key, w_value, w_out)

    return jax.shard_map(local_fn, mesh=mesh, in_specs=(row_spec, rep_spec, rep_spec, rep_spec, rep_spec, row_spec), out_specs=row_spec, check_vma=False)
```

```python
import jax
import jax.numpy as jnp
from jax import lax
from jax.experimental import pallas as pl
from jax.experimental.pallas import tpu as pltpu
from jax.sharding import PartitionSpec as P

HEAD_DIM = 64
BLK = 64
SLOTS = 16
WIDTH = 2048
HALF = 1024
CHIPS = 64
PAIRS = 8
ALL = (PAIRS,) + tuple(range(PAIRS))
NEG = -1e30
FAR = 1 << 20
MESH = pl.DeviceIdType.MESH
VMEM = pltpu.VMEM
ORDERS = ((0, 1, 2), (1, 2, 0), (2, 0, 1))
NT = (((1,), (1,)), ((), ()))
TN = (((0,), (0,)), ((), ()))


def permutation():
    row = lax.broadcasted_iota(jnp.int32, (256, 256), 0)
    col = lax.broadcasted_iota(jnp.int32, (256, 256), 1)
    return jnp.where(col == (row & 15) * 16 + (row >> 4), 1.0, 0.0).astype(jnp.bfloat16)


def split_heads(pair, rows):
    lane = lax.broadcasted_iota(jnp.int32, (rows, 128), 1)
    zero = jnp.zeros_like(pair)
    return jnp.concatenate([jnp.where(lane < HEAD_DIM, pair, zero), jnp.where(lane < HEAD_DIM, zero, pair)], axis=0)


def join_heads(out, rows):
    lane = lax.broadcasted_iota(jnp.int32, (rows, 128), 1)
    return jnp.where(lane < HEAD_DIM, out[:rows], out[rows:])


def aligned(i, n):
    return pl.ds(pl.multiple_of(i * n, n), n)


def remote(src, dst, send, recv, dev):
    return pltpu.make_async_remote_copy(src_ref=src, dst_ref=dst, send_sem=send, recv_sem=recv,
                                        device_id={"seq": dev}, device_id_type=MESH)


def kernel(x_ref, rand_ref, wq_ref, wk_ref, wv_ref, wo_ref, y_ref,
           idx_ref, full_ref, wo_buf, xs, xc, recv, w_buf, idx_all, sel, other, q_ref, k_ref, v_ref, gath, hot, o_ref, part, parts, glob, piece, near_s, slot_s, gath_q, queries_t, y_buf,
           s_send, s_recv, i_send, i_recv, x_sem, h_send, h_recv, loc, w_sem, p_sem, g_send, g_recv,
           c_send, c_recv, o_send, o_recv, e_send, e_recv, wo_sem, own_sem, y_sem):
    dev = lax.axis_index("seq")
    chip, core = dev // 2, dev % 2
    partner = dev + 1 - 2 * core
    coord = (chip % 4, (chip // 4) % 4, chip // 16)
    scale = (1, 4, 16)
    perm = permutation()

    barrier = pltpu.get_barrier_semaphore()

    def greet(i, carry):
        pl.semaphore_signal(barrier, inc=1, device_id={"seq": dev ^ i}, device_id_type=MESH)
        return carry
    with jax.named_scope("greet"):
        lax.fori_loop(1, 128, greet, 0, unroll=8)

    def w_copy(i, t):
        w = (wq_ref, wk_ref, wv_ref)[i]
        return pltpu.make_async_copy(w.at[:, aligned(core * 4 + t, 256)], w_buf.at[i, :, aligned(t, 256)], w_sem.at[i, t])

    def x_swap(which):
        return remote(x_ref, xc.at[aligned(which, 256)], x_sem.at[0], x_sem.at[1], partner)

    def idx_copy(dst_chip, slot):
        return remote(idx_ref, idx_all.at[core, slot], i_send.at[0], i_recv.at[slot], 2 * dst_chip + core)

    def idx_swap(which):
        return remote(idx_all.at[core], idx_all.at[which], i_send.at[1], i_send.at[2], partner)

    def row_copy(dst_chip, slot):
        return remote(xs.at[dst_chip], recv.at[pl.ds(4 * slot, 4)], s_send, s_recv.at[slot], 2 * dst_chip + core)

    def halo(kv, side):
        ref = (k_ref, v_ref)[kv]
        to = lax.rem(chip + 1 + side * (CHIPS - 2), CHIPS)
        return remote(ref.at[pl.ds((8 - 7 * side) * BLK, BLK)], ref.at[pl.ds(9 * side * BLK, BLK)],
                      h_send.at[kv, side], h_recv.at[kv, side], 2 * to + core)

    wo_copy = pltpu.make_async_copy(wo_ref, wo_buf, wo_sem)

    with jax.named_scope("issue"):
        for t in range(4):
            for i in range(3):
                w_copy(i, t).start()
        own_x = pltpu.make_async_copy(x_ref, xc.at[aligned(core, 256)], loc.at[1])
        own_x.start()
        named_lane = lax.broadcasted_iota(jnp.int32, (1, 128), 1)
        line = jnp.full((1, 128), FAR, jnp.int32)
        for e in range(12):
            line = jnp.where(named_lane == e, rand_ref[e // 3, e % 3], line)
        idx_ref[...] = line
        idx_all[core, chip] = line

    def relayout(step, carry):
        blk, group = step >> 2, step & 3
        rows = x_ref[aligned(step, 16), :]
        rows = jnp.concatenate([rows[:, 128 * c:128 * c + 128] for c in range(16)], axis=0)
        moved = jnp.dot(perm, rows, preferred_element_type=jnp.float32).astype(jnp.bfloat16)
        for a in range(16):
            xs[16 * group + a, blk] = moved[16 * a:16 * a + 16]
        return carry
    with jax.named_scope("relayout"):
        lax.fori_loop(0, 16, relayout, 0)

    def start_idx(i, carry):
        idx_copy(chip ^ i, chip).start()
        return carry

    def start_row(i, carry):
        row_copy(chip ^ i, chip).start()
        return carry
    with jax.named_scope("barrier"):
        pl.semaphore_wait(barrier, 127)
    with jax.named_scope("issue_rows"):
        x_swap(core).start()
        lax.fori_loop(1, CHIPS, start_idx, 0, unroll=7)
        lax.fori_loop(1, CHIPS, start_row, 0, unroll=7)
        own_row = pltpu.make_async_copy(xs.at[chip], recv.at[pl.ds(4 * chip, 4)], loc.at[0])
        own_row.start()

    with jax.named_scope("wait_x"):
        own_x.wait()
        wo_copy.start()
        x_swap(core).wait_send()
        x_swap(1 - core).wait_recv()

    def project(t, carry):
        cols = aligned(t, 256)
        for i in range(3):
            w_copy(i, t).wait()
        rows = xc[...]
        q_ref[:, cols] = jnp.dot(rows, w_buf[0, :, cols], preferred_element_type=jnp.float32).astype(jnp.bfloat16)
        k_ref[BLK:9 * BLK, cols] = jnp.dot(rows, w_buf[1, :, cols], preferred_element_type=jnp.float32).astype(jnp.bfloat16)
        v_ref[BLK:9 * BLK, cols] = jnp.dot(rows, w_buf[2, :, cols], preferred_element_type=jnp.float32).astype(jnp.bfloat16)
        return carry
    with jax.named_scope("project"):
        lax.fori_loop(0, 4, project, 0)

    def wait_idx(i, carry):
        idx_copy(chip ^ i, chip ^ i).wait()
        return carry
    with jax.named_scope("wait_idx"):
        lax.fori_loop(1, CHIPS, wait_idx, 0)
        idx_swap(core).start()
        idx_swap(core).wait_send()
        idx_swap(1 - core).wait_recv()
    with jax.named_scope("names"):
        ids = jnp.concatenate([idx_all[0, :, 0, :], idx_all[1, :, 0, :]], axis=0)
        published = [jnp.int32(0), jnp.int32(1), jnp.min(ids)]
        for s in range(3, 14):
            published.append(jnp.min(jnp.where(ids > published[-1], ids, FAR)))

    with jax.named_scope("slots"):
        near = [pltpu.make_async_copy(idx_all.at[c, chip], near_s.at[c], loc.at[1 + c]) for c in range(2)]
        for n in near:
            n.start()
        for n in near:
            n.wait()
        for b in range(8):
            for t in range(3):
                named = near_s[b // 4, 0, 3 * (b % 4) + t]
                at = jnp.int32(2)
                for h in published[2:]:
                    at = at + jnp.where(h < named, 1, 0)
                slot_s[3 * b + t] = at

    with jax.named_scope("issue_halos"):
        for kv in range(2):
            for side in range(2):
                halo(kv, side).start()

    def wait_row(i, carry):
        row_copy(chip ^ i, chip ^ i).wait()
        return carry
    with jax.named_scope("wait_rows"):
        lax.fori_loop(1, CHIPS, wait_row, 0)
        own_row.wait()

    with jax.named_scope("select"):
        for s in range(SLOTS):
            if s < 14:
                h = published[s]
                rows = recv[jnp.minimum((h >> 3) * 4 + (h & 3), 4 * CHIPS - 1)]
                sel[16 * s:16 * s + 16, :] = jnp.where(((h >> 2) & 1) == core, rows, jnp.zeros_like(rows))
            else:
                sel[16 * s:16 * s + 16, :] = jnp.zeros((16, 128), jnp.bfloat16)
        swap = remote(sel, other, p_sem.at[0], p_sem.at[1], partner)
        swap.start()
        swap.wait()
    with jax.named_scope("publish"):
        moved = jnp.dot(perm, sel[...] + other[...], preferred_element_type=jnp.float32).astype(jnp.bfloat16)
        rows = jnp.concatenate([moved[16 * j:16 * j + 16] for j in range(16)], axis=1)
        gq = jnp.dot(rows, w_buf[0], preferred_element_type=jnp.float32)
        gq = jnp.concatenate([gq[t:t + 1, 128 * j:128 * j + 128] for t in range(2) for j in range(PAIRS)], axis=0)
        gath_q[0, coord[2], coord[1], coord[0]] = gq.astype(jnp.bfloat16)
        out = [jnp.dot(rows, w_buf[i], preferred_element_type=jnp.float32) for i in (1, 2)]
        for j in range(PAIRS):
            cols = slice(128 * j, 128 * j + 128)
            kv = jnp.concatenate([out[0][:, cols], out[1][:, cols]], axis=1)
            gath[j, coord[2], coord[1], coord[0]] = kv.astype(jnp.bfloat16)

    def copies(j, stage, receive):
        order = ORDERS[j % 3]
        axis = order[stage]
        out = []
        for k in (1, 2, 3):
            to = lax.rem(coord[axis] + k, 4)
            at = list(coord)
            if receive:
                at[axis] = lax.rem(coord[axis] + 4 - k, 4)
            buf, at_j = (gath, j) if j < PAIRS else (gath_q, 0)
            ref = buf.at[(at_j,) + tuple(slice(None) if a in order[:stage] else at[a] for a in (2, 1, 0))]
            out.append(remote(ref, ref, g_send.at[j, stage, k - 1], g_recv.at[j, stage, k - 1],
                              dev + 2 * scale[axis] * (to - coord[axis])))
        return out

    def advance(j, stage):
        if stage:
            for c in copies(j, stage - 1, True):
                c.wait_recv()
        if stage < 3:
            for c in copies(j, stage, False):
                c.start()

    with jax.named_scope("gather0"):
        for j in ALL:
            advance(j, 0)
    with jax.named_scope("gather1"):
        for j in ALL:
            advance(j, 1)
    with jax.named_scope("gather2"):
        for j in ALL:
            advance(j, 2)

    with jax.named_scope("wait_queries"):
        advance(PAIRS, 3)

    def unpack_queries(z, carry):
        moved = jnp.dot(perm, gath_q[0, z].reshape(256, 128), preferred_element_type=jnp.float32).astype(jnp.bfloat16)
        for s in range(SLOTS):
            queries_t[s, aligned(z, 16), :] = moved[16 * s:16 * s + 16]
        return carry

    def glob_part(wave, carry):
        sums, tops = [], []
        for t in range(2):
            j = 2 * wave + t
            cols = aligned(j, 128)
            gq = jnp.concatenate([queries_t[j], queries_t[PAIRS + j]], axis=0)
            queries = split_heads(gq, 128) * jnp.bfloat16(0.125)
            scores = lax.dot_general(k_ref[BLK:9 * BLK, cols], queries, NT, preferred_element_type=jnp.float32)
            top = jnp.max(scores, axis=0, keepdims=True)
            probs = jnp.exp(scores - top)
            total = jnp.sum(probs, axis=0, keepdims=True)
            out = lax.dot_general(probs.astype(jnp.bfloat16), v_ref[BLK:9 * BLK, cols], TN, preferred_element_type=jnp.float32)
            part[wave, :, 128 * t:128 * t + 128] = join_heads(out, 128)
            for h in range(2):
                sums.append(total[:, 128 * h:128 * h + 128])
                tops.append(top[:, 128 * h:128 * h + 128])
        stats = jnp.concatenate(sums + tops + [jnp.zeros((120, 128), jnp.float32)], axis=0)
        part[wave, :, 256:384] = stats.T

        def start_part(i, carry):
            to = 16 * wave + (i ^ (chip & 15))

            @pl.when(to != chip)
            def _():
                part_copy(to, chip).start()
            return carry
        return lax.fori_loop(0, 16, start_part, carry)

    def part_copy(dst_chip, slot):
        return remote(part.at[dst_chip >> 4, aligned(dst_chip & 15, 8)], parts.at[slot], c_send, c_recv.at[slot], 2 * dst_chip + core)

    with jax.named_scope("globpart"):
        lax.fori_loop(0, 4, unpack_queries, 0)
        lax.fori_loop(0, 4, glob_part, 0)
        own_part = pltpu.make_async_copy(part.at[chip >> 4, aligned(chip & 15, 8)], parts.at[chip], loc.at[1])
        own_part.start()

    with jax.named_scope("halo"):
        for kv in range(2):
            for side in range(2):
                halo(kv, side).wait()

    key = lax.broadcasted_iota(jnp.int32, (3 * BLK, 1), 0)

    def o_copy(wave, rows_of, cols_of):
        return remote(o_ref.at[aligned(rows_of, 256), aligned(wave, 256)],
                      full_ref.at[:, aligned(cols_of * 4 + wave, 256)], o_send.at[wave], o_recv.at[wave], partner)

    def one_wave(wave, carry):
        with jax.named_scope("wait_wave"):
            for w in range(4):
                @pl.when(wave == w)
                def _():
                    for j in (2 * w, 2 * w + 1):
                        advance(j, 3)

        def unpack(z, carry):
            for t in range(2):
                rows = gath[2 * wave + t, z].reshape(256, 256)
                moved = jnp.dot(perm, rows, preferred_element_type=jnp.float32).astype(jnp.bfloat16)
                for s in range(14):
                    hot[2 * wave + t, s, aligned(z, 16), :] = moved[s * 16:s * 16 + 16]
            return carry
        with jax.named_scope("unpack"):
            lax.fori_loop(0, 4, unpack, 0)

        with jax.named_scope("blocks"):
            for b in range(8):
                named = [0, 1] + [slot_s[3 * b + t] for t in range(3)]
                rows = slice(b * BLK, b * BLK + BLK)
                near = slice(b * BLK, b * BLK + 3 * BLK)
                for t in range(2):
                    j = 2 * wave + t
                    cols = aligned(j, 128)
                    queries = split_heads(q_ref[rows, cols], BLK) * jnp.bfloat16(0.125)
                    keys = jnp.concatenate([k_ref[near, cols]] + [hot[j, s, :, 0:128] for s in named], axis=0)
                    vals = jnp.concatenate([v_ref[near, cols]] + [hot[j, s, :, 128:256] for s in named], axis=0)
                    scores = lax.dot_general(keys, queries, NT, preferred_element_type=jnp.float32)
                    if b == 2:
                        bias = jnp.where((key < BLK) & (chip == 0), NEG, 0.0)
                    elif b == 7:
                        bias = jnp.where((key >= 2 * BLK) & (chip == CHIPS - 1), NEG, 0.0)
                    if b in (2, 7):
                        scores = jnp.concatenate([scores[:3 * BLK] + bias, scores[3 * BLK:]], axis=0)
                    top = jnp.max(scores, axis=0, keepdims=True)
                    probs = jnp.exp(scores - top)
                    probs = probs * (1.0 / jnp.sum(probs, axis=0, keepdims=True))
                    out = lax.dot_general(probs.astype(jnp.bfloat16), vals, TN, preferred_element_type=jnp.float32)
                    o_ref[rows, cols] = join_heads(out, BLK).astype(jnp.bfloat16)
        own_o(wave).start()
        o_copy(wave, 1 - core, core).start()
        return carry

    def own_o(wave):
        return pltpu.make_async_copy(o_ref.at[aligned(core, 256), aligned(wave, 256)], full_ref.at[:, aligned(4 * core + wave, 256)], own_sem.at[wave])

    lax.fori_loop(0, 4, one_wave, 0)

    with jax.named_scope("local"):
        for j in ALL:
            for stage in range(3):
                for c in copies(j, stage, False):
                    c.wait_send()

    def wait_part(i, carry):
        part_copy(chip ^ i, chip ^ i).wait()
        return carry
    with jax.named_scope("wait_parts"):
        lax.fori_loop(1, CHIPS, wait_part, 0)
        own_part.wait()

    with jax.named_scope("combine"):
        top = lax.fori_loop(0, CHIPS, lambda i, t: jnp.maximum(t, parts[i, :, 256:384]), jnp.full((8, 128), NEG, jnp.float32), unroll=8)

        def add(i, carry):
            num, den = carry
            weight = pltpu.roll(jnp.exp(parts[i, :, 256:384] - top), 124, 1)
            wide = jnp.concatenate([jnp.broadcast_to(weight[:, t:t + 1], (8, HEAD_DIM)) for t in range(4)], axis=1)
            return num + wide * parts[i, :, 0:256], den + weight * parts[i, :, 256:384]
        num, den = lax.fori_loop(0, CHIPS, add, (jnp.zeros((8, 256), jnp.float32), jnp.zeros((8, 128), jnp.float32)), unroll=8)
        wide = jnp.concatenate([jnp.broadcast_to(den[:, t:t + 1], (8, HEAD_DIM)) for t in range(4)], axis=1)
        piece[...] = (num / wide).astype(jnp.bfloat16)

    def glob_slice(src_chip, src_core):
        return glob.at[aligned(src_chip % 16, 8), aligned(src_core * 4 + src_chip // 16, 256)]

    def glob_copy(src_chip, src_core):
        return remote(piece, glob_slice(src_chip, src_core), e_send, e_recv.at[2 * src_chip + src_core], 0)

    @pl.when(dev != 0)
    def _():
        glob_copy(chip, core).start()

    def y_copy(half, t):
        at = (pl.ds(128 * half, 128), aligned(t, 256))
        return pltpu.make_async_copy(y_buf.at[at], y_ref.at[at], y_sem.at[half, t])

    def project_out(t, carry):
        cols = aligned(t, 256)
        y_buf[:, cols] = lax.dot_general(full_ref[...], wo_buf[cols, :], NT, preferred_element_type=jnp.float32).astype(jnp.bfloat16)
        y_copy(1, t).start()

        @pl.when(dev != 0)
        def _():
            y_copy(0, t).start()
        return carry

    def project_glob(t, carry):
        cols = aligned(t, 256)
        y_buf[0:128, cols] = lax.dot_general(glob[...], wo_buf[cols, :], NT, preferred_element_type=jnp.float32).astype(jnp.bfloat16)
        y_copy(0, t).start()
        return carry

    with jax.named_scope("wait_o"):
        wo_copy.wait()
        for wave in range(4):
            own_o(wave).wait()
            o_copy(wave, 1 - core, core).wait_send()
            o_copy(wave, core, 1 - core).wait_recv()
    with jax.named_scope("out"):
        lax.fori_loop(0, PAIRS, project_out, 0)

    with jax.named_scope("tail"):
        @pl.when(dev != 0)
        def _():
            glob_copy(chip, core).wait_send()

        @pl.when(dev == 0)
        def _():
            copy = pltpu.make_async_copy(piece, glob_slice(0, 0), loc.at[0])
            copy.start()
            copy.wait()

            def wait_glob(i, carry):
                glob_copy(i // 2, i % 2).wait_recv()
                return carry
            lax.fori_loop(1, 128, wait_glob, 0)
            lax.fori_loop(0, PAIRS, project_glob, 0)

        def written(t, carry):
            y_copy(0, t).wait()
            y_copy(1, t).wait()
            return carry
        lax.fori_loop(0, PAIRS, written, 0)


def attend(x, rand_idx, wq, wk, wv, wo):
    vmem = pl.BlockSpec(memory_space=VMEM)
    hbm = pl.BlockSpec(memory_space=pl.ANY)
    dma = pltpu.SemaphoreType.DMA
    bf16, f32 = jnp.bfloat16, jnp.float32
    return pl.pallas_call(
        kernel,
        out_shape=jax.ShapeDtypeStruct((256, WIDTH), bf16),
        in_specs=[vmem, pl.BlockSpec(memory_space=pltpu.SMEM), hbm, hbm, hbm, hbm], out_specs=hbm,
        scratch_shapes=[
            VMEM((1, 128), jnp.int32), VMEM((256, WIDTH), bf16), VMEM((WIDTH, WIDTH), bf16),
            VMEM((CHIPS, 4, 16, 128), bf16), VMEM((512, WIDTH), bf16), VMEM((4 * CHIPS, 16, 128), bf16),
            VMEM((3, WIDTH, HALF), bf16), VMEM((2, CHIPS, 1, 128), jnp.int32), VMEM((256, 128), bf16), VMEM((256, 128), bf16),
            VMEM((512, HALF), bf16), VMEM((640, HALF), bf16), VMEM((640, HALF), bf16),
            VMEM((PAIRS, 4, 4, 4, SLOTS, 256), bf16), VMEM((PAIRS, SLOTS, BLK, 256), bf16), VMEM((512, HALF), bf16),
            VMEM((4, 128, 384), f32), VMEM((CHIPS, 8, 384), f32), VMEM((128, WIDTH), bf16), VMEM((8, 256), bf16),
            pltpu.SMEM((2, 1, 128), jnp.int32), pltpu.SMEM((24,), jnp.int32),
            VMEM((1, 4, 4, 4, SLOTS, 128), bf16), VMEM((SLOTS, BLK, 128), bf16), VMEM((256, WIDTH), bf16),
            dma, dma((CHIPS,)), dma((3,)), dma((CHIPS,)), dma((2,)), dma((2, 2)), dma((2, 2)), dma((3,)), dma((3, 4)), dma((2,)),
            dma((PAIRS + 1, 3, 3)), dma((PAIRS + 1, 3, 3)), dma, dma((CHIPS,)), dma((4,)), dma((4,)), dma, dma((128,)), dma, dma((4,)), dma((2, PAIRS))],
        compiler_params=pltpu.CompilerParams(has_side_effects=True, collective_id=0, vmem_limit_bytes=62 * 1024 * 1024), name="attend",
    )(x, rand_idx, wq, wk, wv, wo)


def solution(mesh):
    row_spec = P(("batch", "seq"), None)
    rep_spec = P(None, None)

    def local_fn(tokens, w_query, w_key, w_value, w_out, rand_idx):
        return attend(tokens, rand_idx, w_query, w_key, w_value, w_out)

    return jax.shard_map(local_fn, mesh=mesh, in_specs=(row_spec, rep_spec, rep_spec, rep_spec, rep_spec, row_spec), out_specs=row_spec, check_vma=False)
```

```python
import jax
import jax.numpy as jnp
from jax import lax
from jax.experimental import pallas as pl
from jax.experimental.pallas import tpu as pltpu
from jax.sharding import PartitionSpec as P

HEAD_DIM = 64
BLK = 64
SLOTS = 16
WIDTH = 2048
HALF = 1024
CHIPS = 64
PAIRS = 8
ALL = (PAIRS,) + tuple(range(PAIRS))
NEG = -1e30
FAR = 1 << 20
MESH = pl.DeviceIdType.MESH
VMEM = pltpu.VMEM
ORDERS = ((0, 1, 2), (1, 2, 0), (2, 0, 1))
TILE = 256
LANES = 128
NEAR = (1, 3)
NT = (((1,), (1,)), ((), ()))
TN = (((0,), (0,)), ((), ()))


def permutation():
    row = lax.broadcasted_iota(jnp.int32, (TILE, TILE), 0)
    col = lax.broadcasted_iota(jnp.int32, (TILE, TILE), 1)
    return jnp.where(col == (row & 15) * 16 + (row >> 4), 1.0, 0.0).astype(jnp.bfloat16)


def split_heads(pair, rows):
    lane = lax.broadcasted_iota(jnp.int32, (rows, LANES), 1)
    zero = jnp.zeros_like(pair)
    return jnp.concatenate([jnp.where(lane < HEAD_DIM, pair, zero), jnp.where(lane < HEAD_DIM, zero, pair)], axis=0)


def join_heads(out, rows):
    lane = lax.broadcasted_iota(jnp.int32, (rows, LANES), 1)
    return jnp.where(lane < HEAD_DIM, out[:rows], out[rows:])


def aligned(i, n):
    return pl.ds(pl.multiple_of(i * n, n), n)


def remote(src, dst, send, recv, dev):
    return pltpu.make_async_remote_copy(src_ref=src, dst_ref=dst, send_sem=send, recv_sem=recv,
                                        device_id={"seq": dev}, device_id_type=MESH)


def kernel(x_ref, rand_ref, wq_ref, wk_ref, wv_ref, wo_ref, y_ref,
           idx_ref, full_ref, wo_buf, xs, xc, recv, w_buf, idx_all, sel, other, q_ref, k_ref, v_ref, gath, hot, o_ref, part, parts, glob, piece, near_s, slot_s, gath_q, queries_t, y_buf,
           s_send, s_recv, i_send, i_recv, x_sem, h_send, h_recv, loc, w_sem, p_sem, g_send, g_recv,
           c_send, c_recv, o_send, o_recv, e_send, e_recv, wo_sem, own_sem, y_sem):
    dev = lax.axis_index("seq")
    chip, core = dev // 2, dev % 2
    partner = dev + 1 - 2 * core
    coord = (chip % 4, (chip // 4) % 4, chip // 16)
    scale = (1, 4, 16)
    perm = permutation()

    barrier = pltpu.get_barrier_semaphore()

    def greet(i, carry):
        pl.semaphore_signal(barrier, inc=1, device_id={"seq": dev ^ i}, device_id_type=MESH)
        return carry
    with jax.named_scope("greet"):
        lax.fori_loop(1, LANES, greet, 0, unroll=8)

    def w_copy(i, t):
        w = (wq_ref, wk_ref, wv_ref)[i]
        return pltpu.make_async_copy(w.at[:, aligned(core * 4 + t, TILE)], w_buf.at[i, :, aligned(t, TILE)], w_sem.at[i, t])

    def x_swap(which):
        return remote(x_ref, xc.at[aligned(which, TILE)], x_sem.at[0], x_sem.at[1], partner)

    def idx_copy(dst_chip, slot):
        return remote(idx_ref, idx_all.at[core, slot], i_send.at[0], i_recv.at[slot], 2 * dst_chip + core)

    def idx_swap(which):
        return remote(idx_all.at[core], idx_all.at[which], i_send.at[1], i_send.at[2], partner)

    def row_copy(dst_chip, slot):
        return remote(xs.at[dst_chip], recv.at[pl.ds(4 * slot, 4)], s_send, s_recv.at[slot], 2 * dst_chip + core)

    def halo(kv, side):
        ref = (k_ref, v_ref)[kv]
        to = lax.rem(chip + 1 + side * (CHIPS - 2), CHIPS)
        return remote(ref.at[pl.ds((8 - 7 * side) * BLK, BLK)], ref.at[pl.ds(9 * side * BLK, BLK)],
                      h_send.at[kv, side], h_recv.at[kv, side], 2 * to + core)

    wo_copy = pltpu.make_async_copy(wo_ref, wo_buf, wo_sem)

    with jax.named_scope("issue"):
        for t in range(4):
            for i in range(3):
                w_copy(i, t).start()
        own_x = pltpu.make_async_copy(x_ref, xc.at[aligned(core, TILE)], loc.at[1])
        own_x.start()
        named_lane = lax.broadcasted_iota(jnp.int32, (1, LANES), 1)
        line = jnp.full((1, LANES), FAR, jnp.int32)
        for e in range(12):
            line = jnp.where(named_lane == e, rand_ref[e // 3, e % 3], line)
        idx_ref[...] = line
        idx_all[core, chip] = line

    def relayout(step, carry):
        blk, group = step >> 2, step & 3
        rows = x_ref[aligned(step, 16), :]
        rows = jnp.concatenate([rows[:, LANES * c:LANES * c + LANES] for c in range(16)], axis=0)
        moved = jnp.dot(perm, rows, preferred_element_type=jnp.float32).astype(jnp.bfloat16)
        for a in range(16):
            xs[16 * group + a, blk] = moved[16 * a:16 * a + 16]
        return carry
    with jax.named_scope("relayout"):
        lax.fori_loop(0, 16, relayout, 0)

    def start_idx(i, carry):
        idx_copy(chip ^ i, chip).start()
        return carry

    def start_row(i, carry):
        row_copy(chip ^ i, chip).start()
        return carry
    with jax.named_scope("barrier"):
        pl.semaphore_wait(barrier, 127)
    with jax.named_scope("issue_rows"):
        x_swap(core).start()
        lax.fori_loop(1, CHIPS, start_idx, 0, unroll=7)
        lax.fori_loop(1, CHIPS, start_row, 0, unroll=7)
        own_row = pltpu.make_async_copy(xs.at[chip], recv.at[pl.ds(4 * chip, 4)], loc.at[0])
        own_row.start()

    with jax.named_scope("wait_x"):
        own_x.wait()
        wo_copy.start()
        x_swap(core).wait_send()
        x_swap(1 - core).wait_recv()

    def project(t, carry):
        cols = aligned(t, TILE)
        for i in range(3):
            w_copy(i, t).wait()
        rows = xc[...]
        q_ref[:, cols] = jnp.dot(rows, w_buf[0, :, cols], preferred_element_type=jnp.float32).astype(jnp.bfloat16)
        k_ref[BLK:9 * BLK, cols] = jnp.dot(rows, w_buf[1, :, cols], preferred_element_type=jnp.float32).astype(jnp.bfloat16)
        v_ref[BLK:9 * BLK, cols] = jnp.dot(rows, w_buf[2, :, cols], preferred_element_type=jnp.float32).astype(jnp.bfloat16)
        return carry
    with jax.named_scope("project"):
        lax.fori_loop(0, 4, project, 0)

    def wait_idx(i, carry):
        idx_copy(chip ^ i, chip ^ i).wait()
        return carry
    with jax.named_scope("wait_idx"):
        lax.fori_loop(1, CHIPS, wait_idx, 0)
        idx_swap(core).start()
        idx_swap(core).wait_send()
        idx_swap(1 - core).wait_recv()
    with jax.named_scope("names"):
        ids = jnp.concatenate([idx_all[0, :, 0, :], idx_all[1, :, 0, :]], axis=0)
        published = [jnp.int32(0), jnp.int32(1), jnp.min(ids)]
        for s in range(3, 14):
            published.append(jnp.min(jnp.where(ids > published[-1], ids, FAR)))

    with jax.named_scope("slots"):
        near = [pltpu.make_async_copy(idx_all.at[c, chip], near_s.at[c], loc.at[1 + c]) for c in range(2)]
        for n in near:
            n.start()
        for n in near:
            n.wait()
        for b in range(8):
            for t in range(3):
                named = near_s[b // 4, 0, 3 * (b % 4) + t]
                at = jnp.int32(2)
                for h in published[2:]:
                    at = at + jnp.where(h < named, 1, 0)
                slot_s[3 * b + t] = at

    with jax.named_scope("issue_halos"):
        for kv in range(2):
            for side in range(2):
                halo(kv, side).start()

    def wait_row(i, carry):
        row_copy(chip ^ i, chip ^ i).wait()
        return carry
    with jax.named_scope("wait_rows"):
        lax.fori_loop(1, CHIPS, wait_row, 0)
        own_row.wait()

    with jax.named_scope("select"):
        for s in range(SLOTS):
            if s < 14:
                h = published[s]
                rows = recv[jnp.minimum((h >> 3) * 4 + (h & 3), 4 * CHIPS - 1)]
                sel[16 * s:16 * s + 16, :] = jnp.where(((h >> 2) & 1) == core, rows, jnp.zeros_like(rows))
            else:
                sel[16 * s:16 * s + 16, :] = jnp.zeros((16, LANES), jnp.bfloat16)
        swap = remote(sel, other, p_sem.at[0], p_sem.at[1], partner)
        swap.start()
        swap.wait()
    with jax.named_scope("publish"):
        moved = jnp.dot(perm, sel[...] + other[...], preferred_element_type=jnp.float32).astype(jnp.bfloat16)
        rows = jnp.concatenate([moved[16 * j:16 * j + 16] for j in range(16)], axis=1)
        gq = jnp.dot(rows, w_buf[0], preferred_element_type=jnp.float32)
        gq = jnp.concatenate([gq[t:t + 1, LANES * j:LANES * j + LANES] for t in range(2) for j in range(PAIRS)], axis=0)
        gath_q[0, coord[2], coord[1], coord[0]] = gq.astype(jnp.bfloat16)
        out = [jnp.dot(rows, w_buf[i], preferred_element_type=jnp.float32) for i in (1, 2)]
        for j in range(PAIRS):
            cols = slice(LANES * j, LANES * j + LANES)
            kv = jnp.concatenate([out[0][:, cols], out[1][:, cols]], axis=1)
            gath[j, coord[2], coord[1], coord[0]] = kv.astype(jnp.bfloat16)

    def copies(j, stage, receive):
        order = ORDERS[j % 3]
        axis = order[stage]
        out = []
        for k in NEAR if stage == 2 and j < PAIRS else (1, 2, 3):
            to = lax.rem(coord[axis] + k, 4)
            at = list(coord)
            if receive:
                at[axis] = lax.rem(coord[axis] + 4 - k, 4)
            buf, at_j = (gath, j) if j < PAIRS else (gath_q, 0)
            ref = buf.at[(at_j,) + tuple(slice(None) if a in order[:stage] else at[a] for a in (2, 1, 0))]
            out.append(remote(ref, ref, g_send.at[j, stage, k - 1], g_recv.at[j, stage, k - 1],
                              dev + 2 * scale[axis] * (to - coord[axis])))
        return out

    def passed(j, receive):
        order = ORDERS[j % 3]
        axis = order[2]
        out = []
        for half, k in enumerate(NEAR):
            at = list(coord)
            at[axis] = lax.rem(coord[axis] + (2 if receive else 4 - k), 4)
            ref = gath.at[(j,) + tuple(slice(None) if a in order[:2] else at[a] for a in (2, 1, 0)) + (slice(8 * half, 8 * half + 8),)]
            to = lax.rem(coord[axis] + k, 4)
            out.append(remote(ref, ref, g_send.at[j, 3, half], g_recv.at[j, 3, half], dev + 2 * scale[axis] * (to - coord[axis])))
        return out

    def pass_on(chunks):
        for j in chunks:
            for got, nxt in zip(copies(j, 2, True), passed(j, False)):
                got.wait_recv()
                nxt.start()

    def arrived(j):
        for c in passed(j, True):
            c.wait_recv()

    def advance(j, stage):
        if stage:
            for c in copies(j, stage - 1, True):
                c.wait_recv()
        if stage < 3:
            for c in copies(j, stage, False):
                c.start()

    with jax.named_scope("gather0"):
        for j in ALL:
            advance(j, 0)
    with jax.named_scope("gather1"):
        for j in ALL:
            advance(j, 1)
    with jax.named_scope("gather2"):
        for j in ALL[:7]:
            advance(j, 2)

    with jax.named_scope("wait_queries"):
        advance(PAIRS, 3)

    def unpack_queries(z, carry):
        moved = jnp.dot(perm, gath_q[0, z].reshape(TILE, LANES), preferred_element_type=jnp.float32).astype(jnp.bfloat16)
        for s in range(SLOTS):
            queries_t[s, aligned(z, 16), :] = moved[16 * s:16 * s + 16]
        return carry

    def glob_part(wave, carry):
        sums, tops = [], []
        for t in range(2):
            j = 2 * wave + t
            cols = aligned(j, LANES)
            gq = jnp.concatenate([queries_t[j], queries_t[PAIRS + j]], axis=0)
            queries = split_heads(gq, LANES) * jnp.bfloat16(0.125)
            scores = lax.dot_general(k_ref[BLK:9 * BLK, cols], queries, NT, preferred_element_type=jnp.float32)
            top = jnp.max(scores, axis=0, keepdims=True)
            probs = jnp.exp(scores - top)
            total = jnp.sum(probs, axis=0, keepdims=True)
            out = lax.dot_general(probs.astype(jnp.bfloat16), v_ref[BLK:9 * BLK, cols], TN, preferred_element_type=jnp.float32)
            part[wave, :, LANES * t:LANES * t + LANES] = join_heads(out, LANES)
            for h in range(2):
                sums.append(total[:, LANES * h:LANES * h + LANES])
                tops.append(top[:, LANES * h:LANES * h + LANES])
        stats = jnp.concatenate(sums + tops + [jnp.zeros((120, LANES), jnp.float32)], axis=0)
        part[wave, :, TILE:384] = stats.T

        def start_part(i, carry):
            to = 16 * wave + (i ^ (chip & 15))

            @pl.when(to != chip)
            def _():
                part_copy(to, chip).start()
            return carry
        lax.fori_loop(0, 16, start_part, carry)

        @pl.when(wave == 1)
        def _():
            pass_on((0, 1, 2))
            for j in ALL[7:]:
                advance(j, 2)

        @pl.when(wave == 3)
        def _():
            pass_on((3, 4, 5))
        return carry

    def part_copy(dst_chip, slot):
        return remote(part.at[dst_chip >> 4, aligned(dst_chip & 15, 8)], parts.at[slot], c_send, c_recv.at[slot], 2 * dst_chip + core)

    with jax.named_scope("globpart"):
        lax.fori_loop(0, 4, unpack_queries, 0)
        lax.fori_loop(0, 4, glob_part, 0)
        own_part = pltpu.make_async_copy(part.at[chip >> 4, aligned(chip & 15, 8)], parts.at[chip], loc.at[1])
        own_part.start()

    with jax.named_scope("halo"):
        for kv in range(2):
            for side in range(2):
                halo(kv, side).wait()

    key = lax.broadcasted_iota(jnp.int32, (3 * BLK, 1), 0)

    def o_copy(wave, rows_of, cols_of):
        return remote(o_ref.at[aligned(rows_of, TILE), aligned(wave, TILE)],
                      full_ref.at[:, aligned(cols_of * 4 + wave, TILE)], o_send.at[wave], o_recv.at[wave], partner)

    def one_wave(wave, carry):
        with jax.named_scope("wait_wave"):
            for w in range(4):
                @pl.when(wave == w)
                def _():
                    if w == 1:
                        pass_on((6, 7))
                    for j in (2 * w, 2 * w + 1):
                        arrived(j)

        def unpack(z, carry):
            for t in range(2):
                rows = gath[2 * wave + t, z].reshape(TILE, TILE)
                moved = jnp.dot(perm, rows, preferred_element_type=jnp.float32).astype(jnp.bfloat16)
                for s in range(14):
                    hot[2 * wave + t, s, aligned(z, 16), :] = moved[s * 16:s * 16 + 16]
            return carry
        with jax.named_scope("unpack"):
            lax.fori_loop(0, 4, unpack, 0)

        with jax.named_scope("blocks"):
            for b in range(8):
                named = [0, 1] + [slot_s[3 * b + t] for t in range(3)]
                rows = slice(b * BLK, b * BLK + BLK)
                near = slice(b * BLK, b * BLK + 3 * BLK)
                for t in range(2):
                    j = 2 * wave + t
                    cols = aligned(j, LANES)
                    queries = split_heads(q_ref[rows, cols], BLK) * jnp.bfloat16(0.125)
                    keys = jnp.concatenate([k_ref[near, cols]] + [hot[j, s, :, 0:LANES] for s in named], axis=0)
                    vals = jnp.concatenate([v_ref[near, cols]] + [hot[j, s, :, LANES:TILE] for s in named], axis=0)
                    scores = lax.dot_general(keys, queries, NT, preferred_element_type=jnp.float32)
                    if b == 2:
                        bias = jnp.where((key < BLK) & (chip == 0), NEG, 0.0)
                    elif b == 7:
                        bias = jnp.where((key >= 2 * BLK) & (chip == CHIPS - 1), NEG, 0.0)
                    if b in (2, 7):
                        scores = jnp.concatenate([scores[:3 * BLK] + bias, scores[3 * BLK:]], axis=0)
                    top = jnp.max(scores, axis=0, keepdims=True)
                    probs = jnp.exp(scores - top)
                    probs = probs * (1.0 / jnp.sum(probs, axis=0, keepdims=True))
                    out = lax.dot_general(probs.astype(jnp.bfloat16), vals, TN, preferred_element_type=jnp.float32)
                    o_ref[rows, cols] = join_heads(out, BLK).astype(jnp.bfloat16)
        own_o(wave).start()
        o_copy(wave, 1 - core, core).start()
        return carry

    def own_o(wave):
        return pltpu.make_async_copy(o_ref.at[aligned(core, TILE), aligned(wave, TILE)], full_ref.at[:, aligned(4 * core + wave, TILE)], own_sem.at[wave])

    lax.fori_loop(0, 4, one_wave, 0)

    with jax.named_scope("local"):
        for j in ALL:
            for stage in range(3):
                for c in copies(j, stage, False):
                    c.wait_send()
            if j < PAIRS:
                for c in passed(j, False):
                    c.wait_send()

    def wait_part(i, carry):
        part_copy(chip ^ i, chip ^ i).wait()
        return carry
    with jax.named_scope("wait_parts"):
        lax.fori_loop(1, CHIPS, wait_part, 0)
        own_part.wait()

    with jax.named_scope("combine"):
        top = lax.fori_loop(0, CHIPS, lambda i, t: jnp.maximum(t, parts[i, :, TILE:384]), jnp.full((8, LANES), NEG, jnp.float32), unroll=8)

        def add(i, carry):
            num, den = carry
            weight = pltpu.roll(jnp.exp(parts[i, :, TILE:384] - top), 124, 1)
            wide = jnp.concatenate([jnp.broadcast_to(weight[:, t:t + 1], (8, HEAD_DIM)) for t in range(4)], axis=1)
            return num + wide * parts[i, :, 0:TILE], den + weight * parts[i, :, TILE:384]
        num, den = lax.fori_loop(0, CHIPS, add, (jnp.zeros((8, TILE), jnp.float32), jnp.zeros((8, LANES), jnp.float32)), unroll=8)
        wide = jnp.concatenate([jnp.broadcast_to(den[:, t:t + 1], (8, HEAD_DIM)) for t in range(4)], axis=1)
        piece[...] = (num / wide).astype(jnp.bfloat16)

    def glob_slice(src_chip, src_core):
        return glob.at[aligned(src_chip % 16, 8), aligned(src_core * 4 + src_chip // 16, TILE)]

    def glob_copy(src_chip, src_core):
        return remote(piece, glob_slice(src_chip, src_core), e_send, e_recv.at[2 * src_chip + src_core], 0)

    @pl.when(dev != 0)
    def _():
        glob_copy(chip, core).start()

    def y_copy(half, t):
        at = (pl.ds(LANES * half, LANES), aligned(t, TILE))
        return pltpu.make_async_copy(y_buf.at[at], y_ref.at[at], y_sem.at[half, t])

    def project_out(t, carry):
        cols = aligned(t, TILE)
        y_buf[:, cols] = lax.dot_general(full_ref[...], wo_buf[cols, :], NT, preferred_element_type=jnp.float32).astype(jnp.bfloat16)
        y_copy(1, t).start()

        @pl.when(dev != 0)
        def _():
            y_copy(0, t).start()
        return carry

    def project_glob(t, carry):
        cols = aligned(t, TILE)
        y_buf[0:LANES, cols] = lax.dot_general(glob[...], wo_buf[cols, :], NT, preferred_element_type=jnp.float32).astype(jnp.bfloat16)
        y_copy(0, t).start()
        return carry

    with jax.named_scope("wait_o"):
        wo_copy.wait()
        for wave in range(4):
            own_o(wave).wait()
            o_copy(wave, 1 - core, core).wait_send()
            o_copy(wave, core, 1 - core).wait_recv()
    with jax.named_scope("out"):
        lax.fori_loop(0, PAIRS, project_out, 0)

    with jax.named_scope("tail"):
        @pl.when(dev != 0)
        def _():
            glob_copy(chip, core).wait_send()

        @pl.when(dev == 0)
        def _():
            copy = pltpu.make_async_copy(piece, glob_slice(0, 0), loc.at[0])
            copy.start()
            copy.wait()

            def wait_glob(i, carry):
                glob_copy(i // 2, i % 2).wait_recv()
                return carry
            lax.fori_loop(1, LANES, wait_glob, 0)
            lax.fori_loop(0, PAIRS, project_glob, 0)

        def written(t, carry):
            y_copy(0, t).wait()
            y_copy(1, t).wait()
            return carry
        lax.fori_loop(0, PAIRS, written, 0)


def attend(x, rand_idx, wq, wk, wv, wo):
    vmem = pl.BlockSpec(memory_space=VMEM)
    hbm = pl.BlockSpec(memory_space=pl.ANY)
    dma = pltpu.SemaphoreType.DMA
    bf16, f32 = jnp.bfloat16, jnp.float32
    return pl.pallas_call(
        kernel,
        out_shape=jax.ShapeDtypeStruct((TILE, WIDTH), bf16),
        in_specs=[vmem, pl.BlockSpec(memory_space=pltpu.SMEM), hbm, hbm, hbm, hbm], out_specs=hbm,
        scratch_shapes=[
            VMEM((1, LANES), jnp.int32), VMEM((TILE, WIDTH), bf16), VMEM((WIDTH, WIDTH), bf16),
            VMEM((CHIPS, 4, 16, LANES), bf16), VMEM((512, WIDTH), bf16), VMEM((4 * CHIPS, 16, LANES), bf16),
            VMEM((3, WIDTH, HALF), bf16), VMEM((2, CHIPS, 1, LANES), jnp.int32), VMEM((TILE, LANES), bf16), VMEM((TILE, LANES), bf16),
            VMEM((512, HALF), bf16), VMEM((640, HALF), bf16), VMEM((640, HALF), bf16),
            VMEM((PAIRS, 4, 4, 4, SLOTS, TILE), bf16), VMEM((PAIRS, SLOTS, BLK, TILE), bf16), VMEM((512, HALF), bf16),
            VMEM((4, LANES, 384), f32), VMEM((CHIPS, 8, 384), f32), VMEM((LANES, WIDTH), bf16), VMEM((8, TILE), bf16),
            pltpu.SMEM((2, 1, LANES), jnp.int32), pltpu.SMEM((24,), jnp.int32),
            VMEM((1, 4, 4, 4, SLOTS, LANES), bf16), VMEM((SLOTS, BLK, LANES), bf16), VMEM((TILE, WIDTH), bf16),
            dma, dma((CHIPS,)), dma((3,)), dma((CHIPS,)), dma((2,)), dma((2, 2)), dma((2, 2)), dma((3,)), dma((3, 4)), dma((2,)),
            dma((PAIRS + 1, 4, 3)), dma((PAIRS + 1, 4, 3)), dma, dma((CHIPS,)), dma((4,)), dma((4,)), dma, dma((LANES,)), dma, dma((4,)), dma((2, PAIRS))],
        compiler_params=pltpu.CompilerParams(has_side_effects=True, collective_id=0, vmem_limit_bytes=62 * 1024 * 1024), name="attend",
    )(x, rand_idx, wq, wk, wv, wo)


def solution(mesh):
    row_spec = P(("batch", "seq"), None)
    rep_spec = P(None, None)

    def local_fn(tokens, w_query, w_key, w_value, w_out, rand_idx):
        return attend(tokens, rand_idx, w_query, w_key, w_value, w_out)

    return jax.shard_map(local_fn, mesh=mesh, in_specs=(row_spec, rep_spec, rep_spec, rep_spec, rep_spec, row_spec), out_specs=row_spec, check_vma=False)
```

```python
import jax
import jax.numpy as jnp
from jax import lax
from jax.experimental import pallas as pl
from jax.experimental.pallas import tpu as pltpu
from jax.sharding import PartitionSpec as P

HEAD_DIM = 64
BLK = 64
SLOTS = 16
WIDTH = 2048
HALF = 1024
CHIPS = 64
PAIRS = 8
ALL = (PAIRS,) + tuple(range(PAIRS))
NEG = -1e30
FAR = 1 << 20
MESH = pl.DeviceIdType.MESH
VMEM = pltpu.VMEM
ORDERS = ((0, 1, 2), (1, 2, 0), (2, 0, 1))
TILE = 256
LANES = 128
NT = (((1,), (1,)), ((), ()))
TN = (((0,), (0,)), ((), ()))


def permutation():
    row = lax.broadcasted_iota(jnp.int32, (TILE, TILE), 0)
    col = lax.broadcasted_iota(jnp.int32, (TILE, TILE), 1)
    return jnp.where(col == (row & 15) * 16 + (row >> 4), 1.0, 0.0).astype(jnp.bfloat16)


def split_heads(pair, rows):
    lane = lax.broadcasted_iota(jnp.int32, (rows, LANES), 1)
    zero = jnp.zeros_like(pair)
    return jnp.concatenate([jnp.where(lane < HEAD_DIM, pair, zero), jnp.where(lane < HEAD_DIM, zero, pair)], axis=0)


def join_heads(out, rows):
    lane = lax.broadcasted_iota(jnp.int32, (rows, LANES), 1)
    return jnp.where(lane < HEAD_DIM, out[:rows], out[rows:])


def aligned(i, n):
    return pl.ds(pl.multiple_of(i * n, n), n)


def remote(src, dst, send, recv, dev):
    return pltpu.make_async_remote_copy(src_ref=src, dst_ref=dst, send_sem=send, recv_sem=recv,
                                        device_id={"seq": dev}, device_id_type=MESH)


def kernel(x_ref, rand_ref, wq_ref, wk_ref, wv_ref, full_ref,
           idx_ref, xs, xc, recv, w_buf, idx_all, sel, other, q_ref, k_ref, v_ref, gath, hot, o_ref, part, parts, glob, piece, near_s, slot_s, gath_q, queries_t,
           s_send, s_recv, i_send, i_recv, x_sem, h_send, h_recv, loc, w_sem, p_sem, g_send, g_recv,
           c_send, c_recv, o_send, o_recv, e_send, e_recv, own_sem):
    dev = lax.axis_index("seq")
    chip, core = dev // 2, dev % 2
    partner = dev + 1 - 2 * core
    coord = (chip % 4, (chip // 4) % 4, chip // 16)
    scale = (1, 4, 16)
    perm = permutation()

    barrier = pltpu.get_barrier_semaphore()

    def greet(i, carry):
        pl.semaphore_signal(barrier, inc=1, device_id={"seq": dev ^ i}, device_id_type=MESH)
        return carry
    with jax.named_scope("greet"):
        lax.fori_loop(1, LANES, greet, 0, unroll=8)

    def w_copy(i, t):
        w = (wq_ref, wk_ref, wv_ref)[i]
        return pltpu.make_async_copy(w.at[:, aligned(core * 4 + t, TILE)], w_buf.at[i, :, aligned(t, TILE)], w_sem.at[i, t])

    def x_swap(which):
        return remote(x_ref, xc.at[aligned(which, TILE)], x_sem.at[0], x_sem.at[1], partner)

    def idx_copy(dst_chip, slot):
        return remote(idx_ref, idx_all.at[core, slot], i_send.at[0], i_recv.at[slot], 2 * dst_chip + core)

    def idx_swap(which):
        return remote(idx_all.at[core], idx_all.at[which], i_send.at[1], i_send.at[2], partner)

    def row_copy(dst_chip, slot):
        return remote(xs.at[dst_chip], recv.at[pl.ds(4 * slot, 4)], s_send, s_recv.at[slot], 2 * dst_chip + core)

    def halo(kv, side):
        ref = (k_ref, v_ref)[kv]
        to = lax.rem(chip + 1 + side * (CHIPS - 2), CHIPS)
        return remote(ref.at[pl.ds((8 - 7 * side) * BLK, BLK)], ref.at[pl.ds(9 * side * BLK, BLK)],
                      h_send.at[kv, side], h_recv.at[kv, side], 2 * to + core)


    with jax.named_scope("issue"):
        for t in range(4):
            for i in range(3):
                w_copy(i, t).start()
        own_x = pltpu.make_async_copy(x_ref, xc.at[aligned(core, TILE)], loc.at[1])
        own_x.start()
        named_lane = lax.broadcasted_iota(jnp.int32, (1, LANES), 1)
        line = jnp.full((1, LANES), FAR, jnp.int32)
        for e in range(12):
            line = jnp.where(named_lane == e, rand_ref[e // 3, e % 3], line)
        idx_ref[...] = line
        idx_all[core, chip] = line

    def relayout(step, carry):
        blk, group = step >> 2, step & 3
        rows = x_ref[aligned(step, 16), :]
        rows = jnp.concatenate([rows[:, LANES * c:LANES * c + LANES] for c in range(16)], axis=0)
        moved = jnp.dot(perm, rows, preferred_element_type=jnp.float32).astype(jnp.bfloat16)
        for a in range(16):
            xs[16 * group + a, blk] = moved[16 * a:16 * a + 16]
        return carry
    with jax.named_scope("relayout"):
        lax.fori_loop(0, 16, relayout, 0)

    def start_idx(i, carry):
        idx_copy(chip ^ i, chip).start()
        return carry

    def start_row(i, carry):
        row_copy(chip ^ i, chip).start()
        return carry
    with jax.named_scope("barrier"):
        pl.semaphore_wait(barrier, 127)
    with jax.named_scope("issue_rows"):
        x_swap(core).start()
        lax.fori_loop(1, CHIPS, start_idx, 0, unroll=7)
        lax.fori_loop(1, CHIPS, start_row, 0, unroll=7)
        own_row = pltpu.make_async_copy(xs.at[chip], recv.at[pl.ds(4 * chip, 4)], loc.at[0])
        own_row.start()

    with jax.named_scope("wait_x"):
        own_x.wait()
        x_swap(core).wait_send()
        x_swap(1 - core).wait_recv()

    def project(t, carry):
        cols = aligned(t, TILE)
        for i in range(3):
            w_copy(i, t).wait()
        rows = xc[...]
        q_ref[:, cols] = jnp.dot(rows, w_buf[0, :, cols], preferred_element_type=jnp.float32).astype(jnp.bfloat16)
        k_ref[BLK:9 * BLK, cols] = jnp.dot(rows, w_buf[1, :, cols], preferred_element_type=jnp.float32).astype(jnp.bfloat16)
        v_ref[BLK:9 * BLK, cols] = jnp.dot(rows, w_buf[2, :, cols], preferred_element_type=jnp.float32).astype(jnp.bfloat16)
        return carry
    with jax.named_scope("project"):
        lax.fori_loop(0, 4, project, 0)

    def wait_idx(i, carry):
        idx_copy(chip ^ i, chip ^ i).wait()
        return carry
    with jax.named_scope("wait_idx"):
        lax.fori_loop(1, CHIPS, wait_idx, 0)
        idx_swap(core).start()
        idx_swap(core).wait_send()
        idx_swap(1 - core).wait_recv()
    with jax.named_scope("names"):
        ids = jnp.concatenate([idx_all[0, :, 0, :], idx_all[1, :, 0, :]], axis=0)
        published = [jnp.int32(0), jnp.int32(1), jnp.min(ids)]
        for s in range(3, 14):
            published.append(jnp.min(jnp.where(ids > published[-1], ids, FAR)))

    with jax.named_scope("slots"):
        near = [pltpu.make_async_copy(idx_all.at[c, chip], near_s.at[c], loc.at[1 + c]) for c in range(2)]
        for n in near:
            n.start()
        for n in near:
            n.wait()
        for b in range(8):
            for t in range(3):
                named = near_s[b // 4, 0, 3 * (b % 4) + t]
                at = jnp.int32(2)
                for h in published[2:]:
                    at = at + jnp.where(h < named, 1, 0)
                slot_s[3 * b + t] = at

    with jax.named_scope("issue_halos"):
        for kv in range(2):
            for side in range(2):
                halo(kv, side).start()

    def wait_row(i, carry):
        row_copy(chip ^ i, chip ^ i).wait()
        return carry
    with jax.named_scope("wait_rows"):
        lax.fori_loop(1, CHIPS, wait_row, 0)
        own_row.wait()

    with jax.named_scope("select"):
        for s in range(SLOTS):
            if s < 14:
                h = published[s]
                rows = recv[jnp.minimum((h >> 3) * 4 + (h & 3), 4 * CHIPS - 1)]
                sel[16 * s:16 * s + 16, :] = jnp.where(((h >> 2) & 1) == core, rows, jnp.zeros_like(rows))
            else:
                sel[16 * s:16 * s + 16, :] = jnp.zeros((16, LANES), jnp.bfloat16)
        swap = remote(sel, other, p_sem.at[0], p_sem.at[1], partner)
        swap.start()
        swap.wait()
    with jax.named_scope("publish"):
        moved = jnp.dot(perm, sel[...] + other[...], preferred_element_type=jnp.float32).astype(jnp.bfloat16)
        rows = jnp.concatenate([moved[16 * j:16 * j + 16] for j in range(16)], axis=1)
        gq = jnp.dot(rows, w_buf[0], preferred_element_type=jnp.float32)
        gq = jnp.concatenate([gq[t:t + 1, LANES * j:LANES * j + LANES] for t in range(2) for j in range(PAIRS)], axis=0)
        gath_q[0, coord[2], coord[1], coord[0]] = gq.astype(jnp.bfloat16)
        out = [jnp.dot(rows, w_buf[i], preferred_element_type=jnp.float32) for i in (1, 2)]
        for j in range(PAIRS):
            cols = slice(LANES * j, LANES * j + LANES)
            kv = jnp.concatenate([out[0][:, cols], out[1][:, cols]], axis=1)
            gath[j, coord[2], coord[1], coord[0]] = kv.astype(jnp.bfloat16)

    def copies(j, stage, receive):
        order = ORDERS[j % 3]
        axis = order[stage]
        out = []
        for k in (1, 2, 3):
            to = lax.rem(coord[axis] + k, 4)
            at = list(coord)
            if receive:
                at[axis] = lax.rem(coord[axis] + 4 - k, 4)
            buf, at_j = (gath, j) if j < PAIRS else (gath_q, 0)
            ref = buf.at[(at_j,) + tuple(slice(None) if a in order[:stage] else at[a] for a in (2, 1, 0))]
            out.append(remote(ref, ref, g_send.at[j, stage, k - 1], g_recv.at[j, stage, k - 1],
                              dev + 2 * scale[axis] * (to - coord[axis])))
        return out

    def advance(j, stage):
        if stage:
            for c in copies(j, stage - 1, True):
                c.wait_recv()
        if stage < 3:
            for c in copies(j, stage, False):
                c.start()

    with jax.named_scope("gather0"):
        for j in ALL:
            advance(j, 0)
    with jax.named_scope("gather1"):
        for j in ALL:
            advance(j, 1)
    with jax.named_scope("gather2"):
        for j in ALL:
            advance(j, 2)

    with jax.named_scope("wait_queries"):
        advance(PAIRS, 3)

    def unpack_queries(z, carry):
        moved = jnp.dot(perm, gath_q[0, z].reshape(TILE, LANES), preferred_element_type=jnp.float32).astype(jnp.bfloat16)
        for s in range(SLOTS):
            queries_t[s, aligned(z, 16), :] = moved[16 * s:16 * s + 16]
        return carry

    def glob_part(step, carry):
        sums, tops = [], []
        for t in range(4):
            j = 4 * step + t
            wave = 2 * step + t // 2
            cols = aligned(j, LANES)
            gq = jnp.concatenate([queries_t[j], queries_t[PAIRS + j]], axis=0)
            queries = split_heads(gq, LANES) * jnp.bfloat16(0.125)
            scores = lax.dot_general(k_ref[BLK:9 * BLK, cols], queries, NT, preferred_element_type=jnp.float32)
            top = jnp.max(scores, axis=0, keepdims=True)
            probs = jnp.exp(scores - top)
            total = jnp.sum(probs, axis=0, keepdims=True)
            out = lax.dot_general(probs.astype(jnp.bfloat16), v_ref[BLK:9 * BLK, cols], TN, preferred_element_type=jnp.float32)
            part[wave, :, LANES * (t % 2):LANES * (t % 2) + LANES] = join_heads(out, LANES)
            sums += [total[:, 0:LANES], total[:, LANES:TILE]]
            tops += [top[:, 0:LANES], top[:, LANES:TILE]]
        pad = [jnp.zeros((120, LANES), jnp.float32)]
        for u in range(2):
            stats = jnp.concatenate(sums[4 * u:4 * u + 4] + tops[4 * u:4 * u + 4] + pad, axis=0)
            part[2 * step + u, :, TILE:384] = stats.T

        def start_part(i, carry):
            to = 32 * step + (i ^ (chip & 31))

            @pl.when(to != chip)
            def _():
                part_copy(to, chip).start()
            return carry
        return lax.fori_loop(0, 32, start_part, carry)

    def part_copy(dst_chip, slot):
        return remote(part.at[dst_chip >> 4, aligned(dst_chip & 15, 8)], parts.at[slot], c_send, c_recv.at[slot], 2 * dst_chip + core)

    with jax.named_scope("globpart"):
        lax.fori_loop(0, 4, unpack_queries, 0)
        lax.fori_loop(0, 2, glob_part, 0)
        own_part = pltpu.make_async_copy(part.at[chip >> 4, aligned(chip & 15, 8)], parts.at[chip], loc.at[1])
        own_part.start()

    with jax.named_scope("halo"):
        for kv in range(2):
            for side in range(2):
                halo(kv, side).wait()

    key = lax.broadcasted_iota(jnp.int32, (3 * BLK, 1), 0)

    def o_copy(wave, rows_of, cols_of):
        return remote(o_ref.at[aligned(rows_of, TILE), aligned(wave, TILE)],
                      full_ref.at[:, aligned(cols_of * 4 + wave, TILE)], o_send.at[wave], o_recv.at[wave], partner)

    def one_wave(wave, carry):
        with jax.named_scope("wait_wave"):
            for w in range(4):
                @pl.when(wave == w)
                def _():
                    for j in (2 * w, 2 * w + 1):
                        advance(j, 3)

        def unpack(z, carry):
            for t in range(2):
                rows = gath[2 * wave + t, z].reshape(TILE, TILE)
                moved = jnp.dot(perm, rows, preferred_element_type=jnp.float32).astype(jnp.bfloat16)
                for s in range(14):
                    hot[2 * wave + t, s, 16 * z:16 * z + 16, :] = moved[s * 16:s * 16 + 16]
            return carry
        with jax.named_scope("unpack"):
            for z in range(4):
                unpack(z, 0)

        with jax.named_scope("blocks"):
            for b in range(8):
                named = [0, 1] + [slot_s[3 * b + t] for t in range(3)]
                rows = slice(b * BLK, b * BLK + BLK)
                near = slice(b * BLK, b * BLK + 3 * BLK)
                for t in range(2):
                    j = 2 * wave + t
                    cols = aligned(j, LANES)
                    queries = split_heads(q_ref[rows, cols], BLK) * jnp.bfloat16(0.125)
                    keys = jnp.concatenate([k_ref[near, cols]] + [hot[j, s, :, 0:LANES] for s in named], axis=0)
                    vals = jnp.concatenate([v_ref[near, cols]] + [hot[j, s, :, LANES:TILE] for s in named], axis=0)
                    scores = lax.dot_general(keys, queries, NT, preferred_element_type=jnp.float32)
                    if b == 2:
                        bias = jnp.where((key < BLK) & (chip == 0), NEG, 0.0)
                    elif b == 7:
                        bias = jnp.where((key >= 2 * BLK) & (chip == CHIPS - 1), NEG, 0.0)
                    if b in (2, 7):
                        scores = jnp.concatenate([scores[:3 * BLK] + bias, scores[3 * BLK:]], axis=0)
                    top = jnp.max(scores, axis=0, keepdims=True)
                    probs = jnp.exp(scores - top)
                    probs = probs * (1.0 / jnp.sum(probs, axis=0, keepdims=True))
                    out = lax.dot_general(probs.astype(jnp.bfloat16), vals, TN, preferred_element_type=jnp.float32)
                    o_ref[rows, cols] = join_heads(out, BLK).astype(jnp.bfloat16)
        own_o(wave).start()
        o_copy(wave, 1 - core, core).start()
        return carry

    def own_o(wave):
        return pltpu.make_async_copy(o_ref.at[aligned(core, TILE), aligned(wave, TILE)], full_ref.at[:, aligned(4 * core + wave, TILE)], own_sem.at[wave])

    lax.fori_loop(0, 4, one_wave, 0)

    with jax.named_scope("local"):
        for j in ALL:
            for stage in range(3):
                for c in copies(j, stage, False):
                    c.wait_send()

    def wait_part(i, carry):
        part_copy(chip ^ i, chip ^ i).wait()
        return carry
    with jax.named_scope("wait_parts"):
        lax.fori_loop(1, CHIPS, wait_part, 0)
        own_part.wait()

    with jax.named_scope("combine"):
        top = lax.fori_loop(0, CHIPS, lambda i, t: jnp.maximum(t, parts[i, :, TILE:384]), jnp.full((8, LANES), NEG, jnp.float32), unroll=8)

        def add(i, carry):
            num, den = carry
            weight = pltpu.roll(jnp.exp(parts[i, :, TILE:384] - top), 124, 1)
            wide = jnp.concatenate([jnp.broadcast_to(weight[:, t:t + 1], (8, HEAD_DIM)) for t in range(4)], axis=1)
            return num + wide * parts[i, :, 0:TILE], den + weight * parts[i, :, TILE:384]
        num, den = lax.fori_loop(0, CHIPS, add, (jnp.zeros((8, TILE), jnp.float32), jnp.zeros((8, LANES), jnp.float32)), unroll=8)
        wide = jnp.concatenate([jnp.broadcast_to(den[:, t:t + 1], (8, HEAD_DIM)) for t in range(4)], axis=1)
        piece[...] = (num / wide).astype(jnp.bfloat16)

    def glob_slice(src_chip, src_core):
        return glob.at[aligned(src_chip % 16, 8), aligned(src_core * 4 + src_chip // 16, TILE)]

    def glob_copy(src_chip, src_core):
        return remote(piece, glob_slice(src_chip, src_core), e_send, e_recv.at[2 * src_chip + src_core], 0)

    @pl.when(dev != 0)
    def _():
        glob_copy(chip, core).start()

    with jax.named_scope("wait_o"):
        for wave in range(4):
            own_o(wave).wait()
            o_copy(wave, 1 - core, core).wait_send()
            o_copy(wave, core, 1 - core).wait_recv()
    with jax.named_scope("tail"):
        @pl.when(dev != 0)
        def _():
            glob_copy(chip, core).wait_send()

        @pl.when(dev == 0)
        def _():
            copy = pltpu.make_async_copy(piece, glob_slice(0, 0), loc.at[0])
            copy.start()
            copy.wait()

            def wait_glob(i, carry):
                glob_copy(i // 2, i % 2).wait_recv()
                return carry
            lax.fori_loop(1, LANES, wait_glob, 0)
            full_ref[0:LANES, :] = glob[...]


def out_kernel(rows_ref, w_ref, y_ref):
    y_ref[...] = lax.dot_general(rows_ref[...], w_ref[...], NT, preferred_element_type=jnp.float32).astype(jnp.bfloat16)


def project_out(rows, wo):
    tile = TILE
    return pl.pallas_call(
        out_kernel, grid=(WIDTH // tile,),
        in_specs=[pl.BlockSpec(rows.shape, lambda j: (0, 0)), pl.BlockSpec((tile, WIDTH), lambda j: (j, 0))],
        out_specs=pl.BlockSpec((rows.shape[0], tile), lambda j: (0, j)),
        out_shape=jax.ShapeDtypeStruct(rows.shape, jnp.bfloat16), name="project_out",
        compiler_params=pltpu.CompilerParams(vmem_limit_bytes=16 << 20),
        cost_estimate=pl.CostEstimate(flops=2 * rows.shape[0] * WIDTH * WIDTH, bytes_accessed=10 << 20, transcendentals=0),
    )(rows, wo)


def attend(x, rand_idx, wq, wk, wv):
    vmem = pl.BlockSpec(memory_space=VMEM)
    hbm = pl.BlockSpec(memory_space=pl.ANY)
    dma = pltpu.SemaphoreType.DMA
    bf16, f32 = jnp.bfloat16, jnp.float32
    return pl.pallas_call(
        kernel,
        out_shape=jax.ShapeDtypeStruct((TILE, WIDTH), bf16),
        in_specs=[vmem, pl.BlockSpec(memory_space=pltpu.SMEM), hbm, hbm, hbm], out_specs=vmem,
        scratch_shapes=[
            VMEM((1, LANES), jnp.int32),
            VMEM((CHIPS, 4, 16, LANES), bf16), VMEM((512, WIDTH), bf16), VMEM((4 * CHIPS, 16, LANES), bf16),
            VMEM((3, WIDTH, HALF), bf16), VMEM((2, CHIPS, 1, LANES), jnp.int32), VMEM((TILE, LANES), bf16), VMEM((TILE, LANES), bf16),
            VMEM((512, HALF), bf16), VMEM((640, HALF), bf16), VMEM((640, HALF), bf16),
            VMEM((PAIRS, 4, 4, 4, SLOTS, TILE), bf16), VMEM((PAIRS, SLOTS, BLK, TILE), bf16), VMEM((512, HALF), bf16),
            VMEM((4, LANES, 384), f32), VMEM((CHIPS, 8, 384), f32), VMEM((LANES, WIDTH), bf16), VMEM((8, TILE), bf16),
            pltpu.SMEM((2, 1, LANES), jnp.int32), pltpu.SMEM((24,), jnp.int32),
            VMEM((1, 4, 4, 4, SLOTS, LANES), bf16), VMEM((SLOTS, BLK, LANES), bf16),
            dma, dma((CHIPS,)), dma((3,)), dma((CHIPS,)), dma((2,)), dma((2, 2)), dma((2, 2)), dma((3,)), dma((3, 4)), dma((2,)),
            dma((PAIRS + 1, 3, 3)), dma((PAIRS + 1, 3, 3)), dma, dma((CHIPS,)), dma((4,)), dma((4,)), dma, dma((LANES,)), dma((4,))],
        compiler_params=pltpu.CompilerParams(has_side_effects=True, collective_id=0, vmem_limit_bytes=44 << 20), name="attend",
    )(x, rand_idx, wq, wk, wv)


def solution(mesh):
    row_spec = P(("batch", "seq"), None)
    rep_spec = P(None, None)

    def local_fn(tokens, w_query, w_key, w_value, w_out, rand_idx):
        return project_out(attend(tokens, rand_idx, w_query, w_key, w_value), w_out)

    return jax.shard_map(local_fn, mesh=mesh, in_specs=(row_spec, rep_spec, rep_spec, rep_spec, rep_spec, row_spec), out_specs=row_spec, check_vma=False)
```

```python
import jax
import jax.numpy as jnp
from jax import lax
from jax.experimental import pallas as pl
from jax.experimental.pallas import tpu as pltpu
from jax.sharding import PartitionSpec as P

HEAD_DIM = 64
BLK = 64
SLOTS = 16
WIDTH = 2048
HALF = 1024
CHIPS = 64
PAIRS = 8
ALL = tuple(range(PAIRS)) + (PAIRS,)
NEG = -1e30
FAR = 1 << 20
MESH = pl.DeviceIdType.MESH
VMEM = pltpu.VMEM
ORDERS = ((0, 1, 2), (1, 2, 0), (2, 0, 1))
TILE = 256
LANES = 128
NT = (((1,), (1,)), ((), ()))
TN = (((0,), (0,)), ((), ()))


def permutation():
    row = lax.broadcasted_iota(jnp.int32, (TILE, TILE), 0)
    col = lax.broadcasted_iota(jnp.int32, (TILE, TILE), 1)
    return jnp.where(col == (row & 15) * 16 + (row >> 4), 1.0, 0.0).astype(jnp.bfloat16)


def split_heads(pair, rows):
    lane = lax.broadcasted_iota(jnp.int32, (rows, LANES), 1)
    zero = jnp.zeros_like(pair)
    return jnp.concatenate([jnp.where(lane < HEAD_DIM, pair, zero), jnp.where(lane < HEAD_DIM, zero, pair)], axis=0)


def join_heads(out, rows):
    lane = lax.broadcasted_iota(jnp.int32, (rows, LANES), 1)
    return jnp.where(lane < HEAD_DIM, out[:rows], out[rows:])


def aligned(i, n):
    return pl.ds(pl.multiple_of(i * n, n), n)


def remote(src, dst, send, recv, dev):
    return pltpu.make_async_remote_copy(src_ref=src, dst_ref=dst, send_sem=send, recv_sem=recv,
                                        device_id={"seq": dev}, device_id_type=MESH)


def kernel(x_ref, rand_ref, wq_ref, wk_ref, wv_ref, full_ref,
           idx_ref, xs, xc, recv, w_buf, idx_all, sel, other, q_ref, k_ref, v_ref, gath, hot, o_ref, part, parts, glob, piece, near_s, slot_s, gath_q, queries_t,
           s_send, s_recv, i_send, i_recv, x_sem, h_send, h_recv, loc, w_sem, p_sem, g_send, g_recv,
           c_send, c_recv, o_send, o_recv, e_send, e_recv, own_sem):
    dev = lax.axis_index("seq")
    chip, core = dev // 2, dev % 2
    partner = dev + 1 - 2 * core
    coord = (chip % 4, (chip // 4) % 4, chip // 16)
    scale = (1, 4, 16)
    perm = permutation()

    barrier = pltpu.get_barrier_semaphore()

    def greet(i, carry):
        pl.semaphore_signal(barrier, inc=1, device_id={"seq": dev ^ i}, device_id_type=MESH)
        return carry
    with jax.named_scope("greet"):
        lax.fori_loop(1, LANES, greet, 0, unroll=8)

    def w_copy(i, t):
        w = (wq_ref, wk_ref, wv_ref)[i]
        return pltpu.make_async_copy(w.at[:, aligned(core * 4 + t, TILE)], w_buf.at[i, :, aligned(t, TILE)], w_sem.at[i, t])

    def x_swap(which):
        return remote(x_ref, xc.at[aligned(which, TILE)], x_sem.at[0], x_sem.at[1], partner)

    def idx_copy(dst_chip, slot):
        return remote(idx_ref, idx_all.at[core, slot], i_send.at[0], i_recv.at[slot], 2 * dst_chip + core)

    def idx_swap(which):
        return remote(idx_all.at[core], idx_all.at[which], i_send.at[1], i_send.at[2], partner)

    def row_copy(dst_chip, slot):
        return remote(xs.at[dst_chip], recv.at[pl.ds(4 * slot, 4)], s_send, s_recv.at[slot], 2 * dst_chip + core)

    def halo(kv, side):
        ref = (k_ref, v_ref)[kv]
        to = lax.rem(chip + 1 + side * (CHIPS - 2), CHIPS)
        return remote(ref.at[pl.ds((8 - 7 * side) * BLK, BLK)], ref.at[pl.ds(9 * side * BLK, BLK)],
                      h_send.at[kv, side], h_recv.at[kv, side], 2 * to + core)


    with jax.named_scope("issue"):
        for t in range(4):
            for i in range(3):
                w_copy(i, t).start()
        own_x = pltpu.make_async_copy(x_ref, xc.at[aligned(core, TILE)], loc.at[1])
        own_x.start()
        named_lane = lax.broadcasted_iota(jnp.int32, (1, LANES), 1)
        line = jnp.full((1, LANES), FAR, jnp.int32)
        for e in range(12):
            line = jnp.where(named_lane == e, rand_ref[e // 3, e % 3], line)
        idx_ref[...] = line
        idx_all[core, chip] = line

    def relayout(step, carry):
        blk, group = step >> 2, step & 3
        rows = x_ref[aligned(step, 16), :]
        rows = jnp.concatenate([rows[:, LANES * c:LANES * c + LANES] for c in range(16)], axis=0)
        moved = jnp.dot(perm, rows, preferred_element_type=jnp.float32).astype(jnp.bfloat16)
        for a in range(16):
            xs[16 * group + a, blk] = moved[16 * a:16 * a + 16]
        return carry
    with jax.named_scope("relayout"):
        lax.fori_loop(0, 16, relayout, 0)

    def start_idx(i, carry):
        idx_copy(chip ^ i, chip).start()
        return carry

    def start_row(i, carry):
        row_copy(chip ^ i, chip).start()
        return carry
    with jax.named_scope("barrier"):
        pl.semaphore_wait(barrier, 127)
    with jax.named_scope("issue_rows"):
        x_swap(core).start()
        lax.fori_loop(1, CHIPS, start_idx, 0, unroll=7)
        lax.fori_loop(1, CHIPS, start_row, 0, unroll=7)
        own_row = pltpu.make_async_copy(xs.at[chip], recv.at[pl.ds(4 * chip, 4)], loc.at[0])
        own_row.start()

    with jax.named_scope("wait_x"):
        own_x.wait()
        x_swap(core).wait_send()
        x_swap(1 - core).wait_recv()

    def project(t, carry):
        cols = aligned(t, TILE)
        for i in range(3):
            w_copy(i, t).wait()
        rows = xc[...]
        q_ref[:, cols] = jnp.dot(rows, w_buf[0, :, cols], preferred_element_type=jnp.float32).astype(jnp.bfloat16)
        k_ref[BLK:9 * BLK, cols] = jnp.dot(rows, w_buf[1, :, cols], preferred_element_type=jnp.float32).astype(jnp.bfloat16)
        v_ref[BLK:9 * BLK, cols] = jnp.dot(rows, w_buf[2, :, cols], preferred_element_type=jnp.float32).astype(jnp.bfloat16)
        return carry
    with jax.named_scope("project"):
        lax.fori_loop(0, 4, project, 0)

    def wait_idx(i, carry):
        idx_copy(chip ^ i, chip ^ i).wait()
        return carry
    with jax.named_scope("wait_idx"):
        lax.fori_loop(1, CHIPS, wait_idx, 0)
        idx_swap(core).start()
        idx_swap(core).wait_send()
        idx_swap(1 - core).wait_recv()
    with jax.named_scope("names"):
        ids = jnp.concatenate([idx_all[0, :, 0, :], idx_all[1, :, 0, :]], axis=0)
        published = [jnp.int32(0), jnp.int32(1), jnp.min(ids)]
        for s in range(3, 14):
            published.append(jnp.min(jnp.where(ids > published[-1], ids, FAR)))

    with jax.named_scope("slots"):
        near = [pltpu.make_async_copy(idx_all.at[c, chip], near_s.at[c], loc.at[1 + c]) for c in range(2)]
        for n in near:
            n.start()
        for n in near:
            n.wait()
        for b in range(8):
            for t in range(3):
                named = near_s[b // 4, 0, 3 * (b % 4) + t]
                at = jnp.int32(2)
                for h in published[2:]:
                    at = at + jnp.where(h < named, 1, 0)
                slot_s[3 * b + t] = at

    with jax.named_scope("issue_halos"):
        for kv in range(2):
            for side in range(2):
                halo(kv, side).start()

    def wait_row(i, carry):
        row_copy(chip ^ i, chip ^ i).wait()
        return carry
    with jax.named_scope("wait_rows"):
        lax.fori_loop(1, CHIPS, wait_row, 0)
        own_row.wait()

    with jax.named_scope("select"):
        for s in range(SLOTS):
            if s < 14:
                h = published[s]
                rows = recv[jnp.minimum((h >> 3) * 4 + (h & 3), 4 * CHIPS - 1)]
                sel[16 * s:16 * s + 16, :] = jnp.where(((h >> 2) & 1) == core, rows, jnp.zeros_like(rows))
            else:
                sel[16 * s:16 * s + 16, :] = jnp.zeros((16, LANES), jnp.bfloat16)
        swap = remote(sel, other, p_sem.at[0], p_sem.at[1], partner)
        swap.start()
        swap.wait()
    with jax.named_scope("publish"):
        moved = jnp.dot(perm, sel[...] + other[...], preferred_element_type=jnp.float32).astype(jnp.bfloat16)
        rows = jnp.concatenate([moved[16 * j:16 * j + 16] for j in range(16)], axis=1)
        out = [jnp.dot(rows, w_buf[i], preferred_element_type=jnp.float32) for i in (1, 2)]
        for j in range(PAIRS):
            cols = slice(LANES * j, LANES * j + LANES)
            kv = jnp.concatenate([out[0][:, cols], out[1][:, cols]], axis=1)
            gath[j, coord[2], coord[1], coord[0]] = kv.astype(jnp.bfloat16)

    def copies(j, stage, receive):
        order = ORDERS[j % 3]
        axis = order[stage]
        out = []
        for k in (1, 2, 3):
            to = lax.rem(coord[axis] + k, 4)
            at = list(coord)
            if receive:
                at[axis] = lax.rem(coord[axis] + 4 - k, 4)
            buf, at_j = (gath, j) if j < PAIRS else (gath_q, 0)
            ref = buf.at[(at_j,) + tuple(slice(None) if a in order[:stage] else at[a] for a in (2, 1, 0))]
            out.append(remote(ref, ref, g_send.at[j, stage, k - 1], g_recv.at[j, stage, k - 1],
                              dev + 2 * scale[axis] * (to - coord[axis])))
        return out

    def advance(j, stage):
        if stage:
            for c in copies(j, stage - 1, True):
                c.wait_recv()
        if stage < 3:
            for c in copies(j, stage, False):
                c.start()

    with jax.named_scope("gather0"):
        for j in range(PAIRS):
            advance(j, 0)
    with jax.named_scope("publish_queries"):
        gq = jnp.dot(rows, w_buf[0], preferred_element_type=jnp.float32)
        gq = jnp.concatenate([gq[t:t + 1, LANES * j:LANES * j + LANES] for t in range(2) for j in range(PAIRS)], axis=0)
        gath_q[0, coord[2], coord[1], coord[0]] = gq.astype(jnp.bfloat16)
        advance(PAIRS, 0)
    with jax.named_scope("gather1"):
        for j in ALL:
            advance(j, 1)
    with jax.named_scope("gather2"):
        for j in ALL:
            advance(j, 2)

    with jax.named_scope("wait_queries"):
        advance(PAIRS, 3)

    def unpack_queries(z, carry):
        moved = jnp.dot(perm, gath_q[0, z].reshape(TILE, LANES), preferred_element_type=jnp.float32).astype(jnp.bfloat16)
        for s in range(SLOTS):
            queries_t[s, aligned(z, 16), :] = moved[16 * s:16 * s + 16]
        return carry

    def glob_part(step, carry):
        sums, tops = [], []
        for t in range(4):
            j = 4 * step + t
            wave = 2 * step + t // 2
            cols = aligned(j, LANES)
            gq = jnp.concatenate([queries_t[j], queries_t[PAIRS + j]], axis=0)
            queries = split_heads(gq, LANES) * jnp.bfloat16(0.125)
            scores = lax.dot_general(k_ref[BLK:9 * BLK, cols], queries, NT, preferred_element_type=jnp.float32)
            top = jnp.max(scores, axis=0, keepdims=True)
            probs = jnp.exp(scores - top)
            total = jnp.sum(probs, axis=0, keepdims=True)
            out = lax.dot_general(probs.astype(jnp.bfloat16), v_ref[BLK:9 * BLK, cols], TN, preferred_element_type=jnp.float32)
            part[wave, :, LANES * (t % 2):LANES * (t % 2) + LANES] = join_heads(out, LANES)
            sums += [total[:, 0:LANES], total[:, LANES:TILE]]
            tops += [top[:, 0:LANES], top[:, LANES:TILE]]
        pad = [jnp.zeros((120, LANES), jnp.float32)]
        for u in range(2):
            stats = jnp.concatenate(sums[4 * u:4 * u + 4] + tops[4 * u:4 * u + 4] + pad, axis=0)
            part[2 * step + u, :, TILE:384] = stats.T

        def start_part(i, carry):
            to = 32 * step + (i ^ (chip & 31))

            @pl.when(to != chip)
            def _():
                part_copy(to, chip).start()
            return carry
        return lax.fori_loop(0, 32, start_part, carry)

    def part_copy(dst_chip, slot):
        return remote(part.at[dst_chip >> 4, aligned(dst_chip & 15, 8)], parts.at[slot], c_send, c_recv.at[slot], 2 * dst_chip + core)

    with jax.named_scope("globpart"):
        lax.fori_loop(0, 4, unpack_queries, 0)
        lax.fori_loop(0, 2, glob_part, 0)
        own_part = pltpu.make_async_copy(part.at[chip >> 4, aligned(chip & 15, 8)], parts.at[chip], loc.at[1])
        own_part.start()

    with jax.named_scope("halo"):
        for kv in range(2):
            for side in range(2):
                halo(kv, side).wait()

    key = lax.broadcasted_iota(jnp.int32, (3 * BLK, 1), 0)

    def o_copy(wave, rows_of, cols_of):
        return remote(o_ref.at[aligned(rows_of, TILE), aligned(wave, TILE)],
                      full_ref.at[:, aligned(cols_of * 4 + wave, TILE)], o_send.at[wave], o_recv.at[wave], partner)

    def one_wave(wave, carry):
        with jax.named_scope("wait_wave"):
            for w in range(4):
                @pl.when(wave == w)
                def _():
                    for j in (2 * w, 2 * w + 1):
                        advance(j, 3)

        def unpack(z, carry):
            for t in range(2):
                rows = gath[2 * wave + t, z].reshape(TILE, TILE)
                moved = jnp.dot(perm, rows, preferred_element_type=jnp.float32).astype(jnp.bfloat16)
                for s in range(14):
                    hot[2 * wave + t, s, 16 * z:16 * z + 16, :] = moved[s * 16:s * 16 + 16]
            return carry
        with jax.named_scope("unpack"):
            for z in range(4):
                unpack(z, 0)

        with jax.named_scope("blocks"):
            for b in range(8):
                named = [0, 1] + [slot_s[3 * b + t] for t in range(3)]
                rows = slice(b * BLK, b * BLK + BLK)
                near = slice(b * BLK, b * BLK + 3 * BLK)
                for t in range(2):
                    j = 2 * wave + t
                    cols = aligned(j, LANES)
                    queries = split_heads(q_ref[rows, cols], BLK) * jnp.bfloat16(0.125)
                    keys = jnp.concatenate([k_ref[near, cols]] + [hot[j, s, :, 0:LANES] for s in named], axis=0)
                    vals = jnp.concatenate([v_ref[near, cols]] + [hot[j, s, :, LANES:TILE] for s in named], axis=0)
                    scores = lax.dot_general(keys, queries, NT, preferred_element_type=jnp.float32)
                    if b == 2:
                        bias = jnp.where((key < BLK) & (chip == 0), NEG, 0.0)
                    elif b == 7:
                        bias = jnp.where((key >= 2 * BLK) & (chip == CHIPS - 1), NEG, 0.0)
                    if b in (2, 7):
                        scores = jnp.concatenate([scores[:3 * BLK] + bias, scores[3 * BLK:]], axis=0)
                    top = jnp.max(scores, axis=0, keepdims=True)
                    probs = jnp.exp(scores - top)
                    probs = probs * (1.0 / jnp.sum(probs, axis=0, keepdims=True))
                    out = lax.dot_general(probs.astype(jnp.bfloat16), vals, TN, preferred_element_type=jnp.float32)
                    o_ref[rows, cols] = join_heads(out, BLK).astype(jnp.bfloat16)
        own_o(wave).start()
        o_copy(wave, 1 - core, core).start()
        return carry

    def own_o(wave):
        return pltpu.make_async_copy(o_ref.at[aligned(core, TILE), aligned(wave, TILE)], full_ref.at[:, aligned(4 * core + wave, TILE)], own_sem.at[wave])

    lax.fori_loop(0, 4, one_wave, 0)

    with jax.named_scope("local"):
        for j in ALL:
            for stage in range(3):
                for c in copies(j, stage, False):
                    c.wait_send()

    def wait_part(i, carry):
        part_copy(chip ^ i, chip ^ i).wait()
        return carry
    with jax.named_scope("wait_parts"):
        lax.fori_loop(1, CHIPS, wait_part, 0)
        own_part.wait()

    with jax.named_scope("combine"):
        top = lax.fori_loop(0, CHIPS, lambda i, t: jnp.maximum(t, parts[i, :, TILE:384]), jnp.full((8, LANES), NEG, jnp.float32), unroll=8)

        def add(i, carry):
            num, den = carry
            weight = pltpu.roll(jnp.exp(parts[i, :, TILE:384] - top), 124, 1)
            wide = jnp.concatenate([jnp.broadcast_to(weight[:, t:t + 1], (8, HEAD_DIM)) for t in range(4)], axis=1)
            return num + wide * parts[i, :, 0:TILE], den + weight * parts[i, :, TILE:384]
        num, den = lax.fori_loop(0, CHIPS, add, (jnp.zeros((8, TILE), jnp.float32), jnp.zeros((8, LANES), jnp.float32)), unroll=8)
        wide = jnp.concatenate([jnp.broadcast_to(den[:, t:t + 1], (8, HEAD_DIM)) for t in range(4)], axis=1)
        piece[...] = (num / wide).astype(jnp.bfloat16)

    def glob_slice(src_chip, src_core):
        return glob.at[aligned(src_chip % 16, 8), aligned(src_core * 4 + src_chip // 16, TILE)]

    def glob_copy(src_chip, src_core):
        return remote(piece, glob_slice(src_chip, src_core), e_send, e_recv.at[2 * src_chip + src_core], 0)

    @pl.when(dev != 0)
    def _():
        glob_copy(chip, core).start()

    with jax.named_scope("wait_o"):
        for wave in range(4):
            own_o(wave).wait()
            o_copy(wave, 1 - core, core).wait_send()
            o_copy(wave, core, 1 - core).wait_recv()
    with jax.named_scope("tail"):
        @pl.when(dev != 0)
        def _():
            glob_copy(chip, core).wait_send()

        @pl.when(dev == 0)
        def _():
            copy = pltpu.make_async_copy(piece, glob_slice(0, 0), loc.at[0])
            copy.start()
            copy.wait()

            def wait_glob(i, carry):
                glob_copy(i // 2, i % 2).wait_recv()
                return carry
            lax.fori_loop(1, LANES, wait_glob, 0)
            full_ref[0:LANES, :] = glob[...]


def out_kernel(rows_ref, w_ref, y_ref):
    y_ref[...] = lax.dot_general(rows_ref[...], w_ref[...], NT, preferred_element_type=jnp.float32).astype(jnp.bfloat16)


def project_out(rows, wo):
    tile = TILE
    return pl.pallas_call(
        out_kernel, grid=(WIDTH // tile,),
        in_specs=[pl.BlockSpec(rows.shape, lambda j: (0, 0)), pl.BlockSpec((tile, WIDTH), lambda j: (j, 0))],
        out_specs=pl.BlockSpec((rows.shape[0], tile), lambda j: (0, j)),
        out_shape=jax.ShapeDtypeStruct(rows.shape, jnp.bfloat16), name="project_out",
        compiler_params=pltpu.CompilerParams(vmem_limit_bytes=16 << 20),
        cost_estimate=pl.CostEstimate(flops=2 * rows.shape[0] * WIDTH * WIDTH, bytes_accessed=10 << 20, transcendentals=0),
    )(rows, wo)


def attend(x, rand_idx, wq, wk, wv):
    vmem = pl.BlockSpec(memory_space=VMEM)
    hbm = pl.BlockSpec(memory_space=pl.ANY)
    dma = pltpu.SemaphoreType.DMA
    bf16, f32 = jnp.bfloat16, jnp.float32
    return pl.pallas_call(
        kernel,
        out_shape=jax.ShapeDtypeStruct((TILE, WIDTH), bf16),
        in_specs=[vmem, pl.BlockSpec(memory_space=pltpu.SMEM), hbm, hbm, hbm], out_specs=vmem,
        scratch_shapes=[
            VMEM((1, LANES), jnp.int32),
            VMEM((CHIPS, 4, 16, LANES), bf16), VMEM((512, WIDTH), bf16), VMEM((4 * CHIPS, 16, LANES), bf16),
            VMEM((3, WIDTH, HALF), bf16), VMEM((2, CHIPS, 1, LANES), jnp.int32), VMEM((TILE, LANES), bf16), VMEM((TILE, LANES), bf16),
            VMEM((512, HALF), bf16), VMEM((640, HALF), bf16), VMEM((640, HALF), bf16),
            VMEM((PAIRS, 4, 4, 4, SLOTS, TILE), bf16), VMEM((PAIRS, SLOTS, BLK, TILE), bf16), VMEM((512, HALF), bf16),
            VMEM((4, LANES, 384), f32), VMEM((CHIPS, 8, 384), f32), VMEM((LANES, WIDTH), bf16), VMEM((8, TILE), bf16),
            pltpu.SMEM((2, 1, LANES), jnp.int32), pltpu.SMEM((24,), jnp.int32),
            VMEM((1, 4, 4, 4, SLOTS, LANES), bf16), VMEM((SLOTS, BLK, LANES), bf16),
            dma, dma((CHIPS,)), dma((3,)), dma((CHIPS,)), dma((2,)), dma((2, 2)), dma((2, 2)), dma((3,)), dma((3, 4)), dma((2,)),
            dma((PAIRS + 1, 3, 3)), dma((PAIRS + 1, 3, 3)), dma, dma((CHIPS,)), dma((4,)), dma((4,)), dma, dma((LANES,)), dma((4,))],
        compiler_params=pltpu.CompilerParams(has_side_effects=True, collective_id=0, vmem_limit_bytes=62 << 20), name="attend",
    )(x, rand_idx, wq, wk, wv)


def solution(mesh):
    row_spec = P(("batch", "seq"), None)
    rep_spec = P(None, None)

    def local_fn(tokens, w_query, w_key, w_value, w_out, rand_idx):
        return project_out(attend(tokens, rand_idx, w_query, w_key, w_value), w_out)

    return jax.shard_map(local_fn, mesh=mesh, in_specs=(row_spec, rep_spec, rep_spec, rep_spec, rep_spec, row_spec), out_specs=row_spec, check_vma=False)
```

```python
import jax
import jax.numpy as jnp
from jax import lax
from jax.experimental import pallas as pl
from jax.experimental.pallas import tpu as pltpu
from jax.sharding import PartitionSpec as P

HEAD_DIM = 64
BLK = 64
SLOTS = 16
WIDTH = 2048
HALF = 1024
CHIPS = 64
PAIRS = 8
ALL = (PAIRS,) + tuple(range(PAIRS))
NEG = -1e30
FAR = 1 << 20
MESH = pl.DeviceIdType.MESH
VMEM = pltpu.VMEM
ORDERS = ((0, 1, 2), (1, 2, 0), (2, 0, 1))
TILE = 256
LANES = 128
NT = (((1,), (1,)), ((), ()))
TN = (((0,), (0,)), ((), ()))


def permutation():
    row = lax.broadcasted_iota(jnp.int32, (TILE, TILE), 0)
    col = lax.broadcasted_iota(jnp.int32, (TILE, TILE), 1)
    return jnp.where(col == (row & 15) * 16 + (row >> 4), 1.0, 0.0).astype(jnp.bfloat16)


def split_heads(pair, rows):
    lane = lax.broadcasted_iota(jnp.int32, (rows, LANES), 1)
    zero = jnp.zeros_like(pair)
    return jnp.concatenate([jnp.where(lane < HEAD_DIM, pair, zero), jnp.where(lane < HEAD_DIM, zero, pair)], axis=0)


def join_heads(out, rows):
    lane = lax.broadcasted_iota(jnp.int32, (rows, LANES), 1)
    return jnp.where(lane < HEAD_DIM, out[:rows], out[rows:])


def aligned(i, n):
    return pl.ds(pl.multiple_of(i * n, n), n)


def remote(src, dst, send, recv, dev):
    return pltpu.make_async_remote_copy(src_ref=src, dst_ref=dst, send_sem=send, recv_sem=recv,
                                        device_id={"seq": dev}, device_id_type=MESH)


def kernel(x_ref, rand_ref, wq_ref, wk_ref, wv_ref, full_ref,
           idx_ref, xs, xc, recv, w_buf, idx_all, sel, other, q_ref, k_ref, v_ref, gath, hot, o_ref, part, parts, glob, piece, near_s, slot_s, gath_q, queries_t,
           s_send, s_recv, i_send, i_recv, x_sem, h_send, h_recv, loc, w_sem, p_sem, g_send, g_recv,
           c_send, c_recv, o_send, o_recv, e_send, e_recv, own_sem):
    dev = lax.axis_index("seq")
    chip, core = dev // 2, dev % 2
    partner = dev + 1 - 2 * core
    coord = (chip % 4, (chip // 4) % 4, chip // 16)
    scale = (1, 4, 16)
    perm = permutation()

    barrier = pltpu.get_barrier_semaphore()

    def greet(i, carry):
        pl.semaphore_signal(barrier, inc=1, device_id={"seq": dev ^ i}, device_id_type=MESH)
        return carry
    with jax.named_scope("greet"):
        lax.fori_loop(1, LANES, greet, 0, unroll=8)

    def w_copy(i, t):
        w = (wq_ref, wk_ref, wv_ref)[i]
        return pltpu.make_async_copy(w.at[:, aligned(core * 4 + t, TILE)], w_buf.at[i, :, aligned(t, TILE)], w_sem.at[i, t])

    def x_swap(which):
        return remote(x_ref, xc.at[aligned(which, TILE)], x_sem.at[0], x_sem.at[1], partner)

    def idx_copy(dst_chip, slot):
        return remote(idx_ref, idx_all.at[core, slot], i_send.at[0], i_recv.at[slot], 2 * dst_chip + core)

    def idx_swap(which):
        return remote(idx_all.at[core], idx_all.at[which], i_send.at[1], i_send.at[2], partner)

    def row_copy(dst_chip, slot):
        return remote(xs.at[dst_chip], recv.at[pl.ds(4 * slot, 4)], s_send, s_recv.at[slot], 2 * dst_chip + core)

    def halo(kv, side):
        ref = (k_ref, v_ref)[kv]
        to = lax.rem(chip + 1 + side * (CHIPS - 2), CHIPS)
        return remote(ref.at[pl.ds((8 - 7 * side) * BLK, BLK)], ref.at[pl.ds(9 * side * BLK, BLK)],
                      h_send.at[kv, side], h_recv.at[kv, side], 2 * to + core)


    with jax.named_scope("issue"):
        for t in range(4):
            for i in range(3):
                w_copy(i, t).start()
        own_x = pltpu.make_async_copy(x_ref, xc.at[aligned(core, TILE)], loc.at[1])
        own_x.start()
        named_lane = lax.broadcasted_iota(jnp.int32, (1, LANES), 1)
        line = jnp.full((1, LANES), FAR, jnp.int32)
        for e in range(12):
            line = jnp.where(named_lane == e, rand_ref[e // 3, e % 3], line)
        idx_ref[...] = line
        idx_all[core, chip] = line

    def relayout(step, carry):
        blk, group = step >> 2, step & 3
        rows = x_ref[aligned(step, 16), :]
        rows = jnp.concatenate([rows[:, LANES * c:LANES * c + LANES] for c in range(16)], axis=0)
        moved = jnp.dot(perm, rows, preferred_element_type=jnp.float32).astype(jnp.bfloat16)
        for a in range(16):
            xs[16 * group + a, blk] = moved[16 * a:16 * a + 16]
        return carry
    with jax.named_scope("relayout"):
        lax.fori_loop(0, 16, relayout, 0)

    def start_idx(i, carry):
        idx_copy(chip ^ i, chip).start()
        return carry

    def start_row(i, carry):
        row_copy(chip ^ i, chip).start()
        return carry
    with jax.named_scope("barrier"):
        pl.semaphore_wait(barrier, 127)
    with jax.named_scope("issue_rows"):
        x_swap(core).start()
        lax.fori_loop(1, CHIPS, start_idx, 0, unroll=7)
        lax.fori_loop(1, CHIPS, start_row, 0, unroll=7)
        own_row = pltpu.make_async_copy(xs.at[chip], recv.at[pl.ds(4 * chip, 4)], loc.at[0])
        own_row.start()

    with jax.named_scope("wait_x"):
        own_x.wait()
        x_swap(core).wait_send()
        x_swap(1 - core).wait_recv()

    def project(t, carry):
        cols = aligned(t, TILE)
        for i in range(3):
            w_copy(i, t).wait()
        rows = xc[...]
        q_ref[:, cols] = jnp.dot(rows, w_buf[0, :, cols], preferred_element_type=jnp.float32).astype(jnp.bfloat16)
        k_ref[BLK:9 * BLK, cols] = jnp.dot(rows, w_buf[1, :, cols], preferred_element_type=jnp.float32).astype(jnp.bfloat16)
        v_ref[BLK:9 * BLK, cols] = jnp.dot(rows, w_buf[2, :, cols], preferred_element_type=jnp.float32).astype(jnp.bfloat16)
        return carry
    with jax.named_scope("project"):
        lax.fori_loop(0, 4, project, 0)

    def wait_idx(i, carry):
        idx_copy(chip ^ i, chip ^ i).wait()
        return carry
    with jax.named_scope("wait_idx"):
        lax.fori_loop(1, CHIPS, wait_idx, 0)
        idx_swap(core).start()
        idx_swap(core).wait_send()
        idx_swap(1 - core).wait_recv()
    with jax.named_scope("names"):
        ids = jnp.concatenate([idx_all[0, :, 0, :], idx_all[1, :, 0, :]], axis=0)
        published = [jnp.int32(0), jnp.int32(1), jnp.min(ids)]
        for s in range(3, 14):
            published.append(jnp.min(jnp.where(ids > published[-1], ids, FAR)))

    with jax.named_scope("slots"):
        near = [pltpu.make_async_copy(idx_all.at[c, chip], near_s.at[c], loc.at[1 + c]) for c in range(2)]
        for n in near:
            n.start()
        for n in near:
            n.wait()
        for b in range(8):
            for t in range(3):
                named = near_s[b // 4, 0, 3 * (b % 4) + t]
                at = jnp.int32(2)
                for h in published[2:]:
                    at = at + jnp.where(h < named, 1, 0)
                slot_s[3 * b + t] = at

    with jax.named_scope("issue_halos"):
        for kv in range(2):
            for side in range(2):
                halo(kv, side).start()

    def wait_row(i, carry):
        row_copy(chip ^ i, chip ^ i).wait()
        return carry
    with jax.named_scope("wait_rows"):
        lax.fori_loop(1, CHIPS, wait_row, 0)
        own_row.wait()

    with jax.named_scope("select"):
        for s in range(SLOTS):
            if s < 14:
                h = published[s]
                rows = recv[jnp.minimum((h >> 3) * 4 + (h & 3), 4 * CHIPS - 1)]
                sel[16 * s:16 * s + 16, :] = jnp.where(((h >> 2) & 1) == core, rows, jnp.zeros_like(rows))
            else:
                sel[16 * s:16 * s + 16, :] = jnp.zeros((16, LANES), jnp.bfloat16)
        swap = remote(sel, other, p_sem.at[0], p_sem.at[1], partner)
        swap.start()
        swap.wait()
    with jax.named_scope("publish"):
        moved = jnp.dot(perm, sel[...] + other[...], preferred_element_type=jnp.float32).astype(jnp.bfloat16)
        rows = jnp.concatenate([moved[16 * j:16 * j + 16] for j in range(16)], axis=1)
        out = [jnp.dot(rows, w_buf[i], preferred_element_type=jnp.float32) for i in (1, 2)]
        for j in range(PAIRS):
            cols = slice(LANES * j, LANES * j + LANES)
            kv = jnp.concatenate([out[0][:, cols], out[1][:, cols]], axis=1)
            gath[j, coord[2], coord[1], coord[0]] = kv.astype(jnp.bfloat16)

    def copies(j, stage, receive):
        order = ORDERS[j % 3]
        axis = order[stage]
        out = []
        for k in (1, 2, 3):
            to = lax.rem(coord[axis] + k, 4)
            at = list(coord)
            if receive:
                at[axis] = lax.rem(coord[axis] + 4 - k, 4)
            buf, at_j = (gath, j) if j < PAIRS else (gath_q, 0)
            ref = buf.at[(at_j,) + tuple(slice(None) if a in order[:stage] else at[a] for a in (2, 1, 0))]
            out.append(remote(ref, ref, g_send.at[j, stage, k - 1], g_recv.at[j, stage, k - 1],
                              dev + 2 * scale[axis] * (to - coord[axis])))
        return out

    def advance(j, stage):
        if stage:
            for c in copies(j, stage - 1, True):
                c.wait_recv()
        if stage < 3:
            for c in copies(j, stage, False):
                c.start()

    with jax.named_scope("gather0"):
        for j in range(PAIRS):
            advance(j, 0)
    with jax.named_scope("publish_queries"):
        gq = jnp.dot(rows, w_buf[0], preferred_element_type=jnp.float32)
        gq = jnp.concatenate([gq[t:t + 1, LANES * j:LANES * j + LANES] for t in range(2) for j in range(PAIRS)], axis=0)
        gath_q[0, coord[2], coord[1], coord[0]] = gq.astype(jnp.bfloat16)
        advance(PAIRS, 0)
    with jax.named_scope("gather1"):
        for j in ALL:
            advance(j, 1)
    with jax.named_scope("gather2"):
        for j in ALL:
            advance(j, 2)

    with jax.named_scope("wait_queries"):
        advance(PAIRS, 3)

    def unpack_queries(z, carry):
        moved = jnp.dot(perm, gath_q[0, z].reshape(TILE, LANES), preferred_element_type=jnp.float32).astype(jnp.bfloat16)
        for s in range(SLOTS):
            queries_t[s, aligned(z, 16), :] = moved[16 * s:16 * s + 16]
        return carry

    def glob_part(step, carry):
        sums, tops = [], []
        for t in range(4):
            j = 4 * step + t
            wave = 2 * step + t // 2
            cols = aligned(j, LANES)
            gq = jnp.concatenate([queries_t[j], queries_t[PAIRS + j]], axis=0)
            queries = split_heads(gq, LANES) * jnp.bfloat16(0.125)
            scores = lax.dot_general(k_ref[BLK:9 * BLK, cols], queries, NT, preferred_element_type=jnp.float32)
            top = jnp.max(scores, axis=0, keepdims=True)
            probs = jnp.exp(scores - top)
            total = jnp.sum(probs, axis=0, keepdims=True)
            out = lax.dot_general(probs.astype(jnp.bfloat16), v_ref[BLK:9 * BLK, cols], TN, preferred_element_type=jnp.float32)
            part[wave, :, LANES * (t % 2):LANES * (t % 2) + LANES] = join_heads(out, LANES)
            sums += [total[:, 0:LANES], total[:, LANES:TILE]]
            tops += [top[:, 0:LANES], top[:, LANES:TILE]]
        pad = [jnp.zeros((120, LANES), jnp.float32)]
        for u in range(2):
            stats = jnp.concatenate(sums[4 * u:4 * u + 4] + tops[4 * u:4 * u + 4] + pad, axis=0)
            part[2 * step + u, :, TILE:384] = stats.T

        def start_part(i, carry):
            to = 32 * step + (i ^ (chip & 31))

            @pl.when(to != chip)
            def _():
                part_copy(to, chip).start()
            return carry
        return lax.fori_loop(0, 32, start_part, carry)

    def part_copy(dst_chip, slot):
        return remote(part.at[dst_chip >> 4, aligned(dst_chip & 15, 8)], parts.at[slot], c_send, c_recv.at[slot], 2 * dst_chip + core)

    with jax.named_scope("globpart"):
        lax.fori_loop(0, 4, unpack_queries, 0)
        lax.fori_loop(0, 2, glob_part, 0)
        own_part = pltpu.make_async_copy(part.at[chip >> 4, aligned(chip & 15, 8)], parts.at[chip], loc.at[1])
        own_part.start()

    with jax.named_scope("halo"):
        for kv in range(2):
            for side in range(2):
                halo(kv, side).wait()

    key = lax.broadcasted_iota(jnp.int32, (3 * BLK, 1), 0)

    def o_copy(wave, rows_of, cols_of):
        return remote(o_ref.at[aligned(rows_of, TILE), aligned(wave, TILE)],
                      full_ref.at[:, aligned(cols_of * 4 + wave, TILE)], o_send.at[wave], o_recv.at[wave], partner)

    def one_wave(wave, carry):
        with jax.named_scope("wait_wave"):
            for w in range(4):
                @pl.when(wave == w)
                def _():
                    for j in (2 * w, 2 * w + 1):
                        advance(j, 3)

        def unpack(z, carry):
            for t in range(2):
                rows = gath[2 * wave + t, z].reshape(TILE, TILE)
                moved = jnp.dot(perm, rows, preferred_element_type=jnp.float32).astype(jnp.bfloat16)
                for s in range(14):
                    hot[2 * wave + t, s, 16 * z:16 * z + 16, :] = moved[s * 16:s * 16 + 16]
            return carry
        with jax.named_scope("unpack"):
            for z in range(4):
                unpack(z, 0)

        with jax.named_scope("blocks"):
            for b in range(8):
                named = [0, 1] + [slot_s[3 * b + t] for t in range(3)]
                rows = slice(b * BLK, b * BLK + BLK)
                near = slice(b * BLK, b * BLK + 3 * BLK)
                for t in range(2):
                    j = 2 * wave + t
                    cols = aligned(j, LANES)
                    queries = split_heads(q_ref[rows, cols], BLK) * jnp.bfloat16(0.125)
                    keys = jnp.concatenate([k_ref[near, cols]] + [hot[j, s, :, 0:LANES] for s in named], axis=0)
                    vals = jnp.concatenate([v_ref[near, cols]] + [hot[j, s, :, LANES:TILE] for s in named], axis=0)
                    scores = lax.dot_general(keys, queries, NT, preferred_element_type=jnp.float32)
                    if b == 2:
                        bias = jnp.where((key < BLK) & (chip == 0), NEG, 0.0)
                    elif b == 7:
                        bias = jnp.where((key >= 2 * BLK) & (chip == CHIPS - 1), NEG, 0.0)
                    if b in (2, 7):
                        scores = jnp.concatenate([scores[:3 * BLK] + bias, scores[3 * BLK:]], axis=0)
                    top = jnp.max(scores, axis=0, keepdims=True)
                    probs = jnp.exp(scores - top)
                    probs = probs * (1.0 / jnp.sum(probs, axis=0, keepdims=True))
                    out = lax.dot_general(probs.astype(jnp.bfloat16), vals, TN, preferred_element_type=jnp.float32)
                    o_ref[rows, cols] = join_heads(out, BLK).astype(jnp.bfloat16)
        own_o(wave).start()
        o_copy(wave, 1 - core, core).start()
        return carry

    def own_o(wave):
        return pltpu.make_async_copy(o_ref.at[aligned(core, TILE), aligned(wave, TILE)], full_ref.at[:, aligned(4 * core + wave, TILE)], own_sem.at[wave])

    lax.fori_loop(0, 4, one_wave, 0)

    with jax.named_scope("local"):
        for j in ALL:
            for stage in range(3):
                for c in copies(j, stage, False):
                    c.wait_send()

    def wait_part(i, carry):
        part_copy(chip ^ i, chip ^ i).wait()
        return carry
    with jax.named_scope("wait_parts"):
        lax.fori_loop(1, CHIPS, wait_part, 0)
        own_part.wait()

    with jax.named_scope("combine"):
        top = lax.fori_loop(0, CHIPS, lambda i, t: jnp.maximum(t, parts[i, :, TILE:384]), jnp.full((8, LANES), NEG, jnp.float32), unroll=8)

        def add(i, carry):
            num, den = carry
            weight = pltpu.roll(jnp.exp(parts[i, :, TILE:384] - top), 124, 1)
            wide = jnp.concatenate([jnp.broadcast_to(weight[:, t:t + 1], (8, HEAD_DIM)) for t in range(4)], axis=1)
            return num + wide * parts[i, :, 0:TILE], den + weight * parts[i, :, TILE:384]
        num, den = lax.fori_loop(0, CHIPS, add, (jnp.zeros((8, TILE), jnp.float32), jnp.zeros((8, LANES), jnp.float32)), unroll=8)
        wide = jnp.concatenate([jnp.broadcast_to(den[:, t:t + 1], (8, HEAD_DIM)) for t in range(4)], axis=1)
        piece[...] = (num / wide).astype(jnp.bfloat16)

    def glob_slice(src_chip, src_core):
        return glob.at[aligned(src_chip % 16, 8), aligned(src_core * 4 + src_chip // 16, TILE)]

    def glob_copy(src_chip, src_core):
        return remote(piece, glob_slice(src_chip, src_core), e_send, e_recv.at[2 * src_chip + src_core], 0)

    @pl.when(dev != 0)
    def _():
        glob_copy(chip, core).start()

    with jax.named_scope("wait_o"):
        for wave in range(4):
            own_o(wave).wait()
            o_copy(wave, 1 - core, core).wait_send()
            o_copy(wave, core, 1 - core).wait_recv()
    with jax.named_scope("tail"):
        @pl.when(dev != 0)
        def _():
            glob_copy(chip, core).wait_send()

        @pl.when(dev == 0)
        def _():
            copy = pltpu.make_async_copy(piece, glob_slice(0, 0), loc.at[0])
            copy.start()
            copy.wait()

            def wait_glob(i, carry):
                glob_copy(i // 2, i % 2).wait_recv()
                return carry
            lax.fori_loop(1, LANES, wait_glob, 0)
            full_ref[0:LANES, :] = glob[...]


def out_kernel(rows_ref, w_ref, y_ref):
    y_ref[...] = lax.dot_general(rows_ref[...], w_ref[...], NT, preferred_element_type=jnp.float32).astype(jnp.bfloat16)


def project_out(rows, wo):
    tile = TILE
    return pl.pallas_call(
        out_kernel, grid=(WIDTH // tile,),
        in_specs=[pl.BlockSpec(rows.shape, lambda j: (0, 0)), pl.BlockSpec((tile, WIDTH), lambda j: (j, 0))],
        out_specs=pl.BlockSpec((rows.shape[0], tile), lambda j: (0, j)),
        out_shape=jax.ShapeDtypeStruct(rows.shape, jnp.bfloat16), name="project_out",
        compiler_params=pltpu.CompilerParams(vmem_limit_bytes=62 << 20),
        cost_estimate=pl.CostEstimate(flops=2 * rows.shape[0] * WIDTH * WIDTH, bytes_accessed=10 << 20, transcendentals=0),
    )(rows, wo)


def attend(x, rand_idx, wq, wk, wv):
    vmem = pl.BlockSpec(memory_space=VMEM)
    hbm = pl.BlockSpec(memory_space=pl.ANY)
    dma = pltpu.SemaphoreType.DMA
    bf16, f32 = jnp.bfloat16, jnp.float32
    return pl.pallas_call(
        kernel,
        out_shape=jax.ShapeDtypeStruct((TILE, WIDTH), bf16),
        in_specs=[vmem, pl.BlockSpec(memory_space=pltpu.SMEM), hbm, hbm, hbm], out_specs=vmem,
        scratch_shapes=[
            VMEM((1, LANES), jnp.int32),
            VMEM((CHIPS, 4, 16, LANES), bf16), VMEM((512, WIDTH), bf16), VMEM((4 * CHIPS, 16, LANES), bf16),
            VMEM((3, WIDTH, HALF), bf16), VMEM((2, CHIPS, 1, LANES), jnp.int32), VMEM((TILE, LANES), bf16), VMEM((TILE, LANES), bf16),
            VMEM((512, HALF), bf16), VMEM((640, HALF), bf16), VMEM((640, HALF), bf16),
            VMEM((PAIRS, 4, 4, 4, SLOTS, TILE), bf16), VMEM((PAIRS, SLOTS, BLK, TILE), bf16), VMEM((512, HALF), bf16),
            VMEM((4, LANES, 384), f32), VMEM((CHIPS, 8, 384), f32), VMEM((LANES, WIDTH), bf16), VMEM((8, TILE), bf16),
            pltpu.SMEM((2, 1, LANES), jnp.int32), pltpu.SMEM((24,), jnp.int32),
            VMEM((1, 4, 4, 4, SLOTS, LANES), bf16), VMEM((SLOTS, BLK, LANES), bf16),
            dma, dma((CHIPS,)), dma((3,)), dma((CHIPS,)), dma((2,)), dma((2, 2)), dma((2, 2)), dma((3,)), dma((3, 4)), dma((2,)),
            dma((PAIRS + 1, 3, 3)), dma((PAIRS + 1, 3, 3)), dma, dma((CHIPS,)), dma((4,)), dma((4,)), dma, dma((LANES,)), dma((4,))],
        compiler_params=pltpu.CompilerParams(has_side_effects=True, collective_id=0, vmem_limit_bytes=62 << 20), name="attend",
    )(x, rand_idx, wq, wk, wv)


def solution(mesh):
    row_spec = P(("batch", "seq"), None)
    rep_spec = P(None, None)

    def local_fn(tokens, w_query, w_key, w_value, w_out, rand_idx):
        return project_out(attend(tokens, rand_idx, w_query, w_key, w_value), w_out)

    return jax.shard_map(local_fn, mesh=mesh, in_specs=(row_spec, rep_spec, rep_spec, rep_spec, rep_spec, row_spec), out_specs=row_spec, check_vma=False)
```

```python
import jax
import jax.numpy as jnp
from jax import lax
from jax.experimental import pallas as pl
from jax.experimental.pallas import tpu as pltpu
from jax.sharding import PartitionSpec as P

HEAD_DIM = 64
BLK = 64
SLOTS = 16
WIDTH = 2048
HALF = 1024
CHIPS = 64
PAIRS = 8
ALL = (PAIRS,) + tuple(range(PAIRS))
NEG = -1e30
FAR = 1 << 20
MESH = pl.DeviceIdType.MESH
VMEM = pltpu.VMEM
ORDERS = ((0, 1, 2), (1, 2, 0), (2, 0, 1))
TILE = 256
LANES = 128
NT = (((1,), (1,)), ((), ()))
TN = (((0,), (0,)), ((), ()))


def permutation():
    row = lax.broadcasted_iota(jnp.int32, (TILE, TILE), 0)
    col = lax.broadcasted_iota(jnp.int32, (TILE, TILE), 1)
    return jnp.where(col == (row & 15) * 16 + (row >> 4), 1.0, 0.0).astype(jnp.bfloat16)


def split_heads(pair, rows):
    lane = lax.broadcasted_iota(jnp.int32, (rows, LANES), 1)
    zero = jnp.zeros_like(pair)
    return jnp.concatenate([jnp.where(lane < HEAD_DIM, pair, zero), jnp.where(lane < HEAD_DIM, zero, pair)], axis=0)


def join_heads(out, rows):
    lane = lax.broadcasted_iota(jnp.int32, (rows, LANES), 1)
    return jnp.where(lane < HEAD_DIM, out[:rows], out[rows:])


def aligned(i, n):
    return pl.ds(pl.multiple_of(i * n, n), n)


def remote(src, dst, send, recv, dev):
    return pltpu.make_async_remote_copy(src_ref=src, dst_ref=dst, send_sem=send, recv_sem=recv,
                                        device_id={"seq": dev}, device_id_type=MESH)


def kernel(x_ref, rand_ref, wq_ref, wk_ref, wv_ref, full_ref,
           idx_ref, xs, xc, recv, w_buf, idx_all, sel, other, q_ref, k_ref, v_ref, gath, hot, o_ref, part, parts, glob, piece, near_s, slot_s, gath_q, queries_t,
           s_send, s_recv, i_send, i_recv, x_sem, h_send, h_recv, loc, w_sem, p_sem, g_send, g_recv,
           c_send, c_recv, o_send, o_recv, e_send, e_recv, own_sem):
    dev = lax.axis_index("seq")
    chip, core = dev // 2, dev % 2
    partner = dev + 1 - 2 * core
    coord = (chip % 4, (chip // 4) % 4, chip // 16)
    scale = (1, 4, 16)
    perm = permutation()

    barrier = pltpu.get_barrier_semaphore()

    def greet(i, carry):
        pl.semaphore_signal(barrier, inc=1, device_id={"seq": dev ^ i}, device_id_type=MESH)
        return carry
    with jax.named_scope("greet"):
        lax.fori_loop(1, LANES, greet, 0, unroll=8)

    def w_copy(i, t):
        w = (wq_ref, wk_ref, wv_ref)[i]
        return pltpu.make_async_copy(w.at[:, aligned(core * 4 + t, TILE)], w_buf.at[i, :, aligned(t, TILE)], w_sem.at[i, t])

    def x_swap(which):
        return remote(x_ref, xc.at[aligned(which, TILE)], x_sem.at[0], x_sem.at[1], partner)

    def idx_copy(dst_chip, slot):
        return remote(idx_ref, idx_all.at[core, slot], i_send.at[0], i_recv.at[slot], 2 * dst_chip + core)

    def idx_swap(which):
        return remote(idx_all.at[core], idx_all.at[which], i_send.at[1], i_send.at[2], partner)

    def row_copy(dst_chip, slot):
        return remote(xs.at[dst_chip], recv.at[pl.ds(4 * slot, 4)], s_send, s_recv.at[slot], 2 * dst_chip + core)

    def halo(kv, side):
        ref = (k_ref, v_ref)[kv]
        to = lax.rem(chip + 1 + side * (CHIPS - 2), CHIPS)
        return remote(ref.at[pl.ds((8 - 7 * side) * BLK, BLK)], ref.at[pl.ds(9 * side * BLK, BLK)],
                      h_send.at[kv, side], h_recv.at[kv, side], 2 * to + core)


    with jax.named_scope("issue"):
        for t in range(4):
            for i in range(3):
                w_copy(i, t).start()
        own_x = pltpu.make_async_copy(x_ref, xc.at[aligned(core, TILE)], loc.at[1])
        own_x.start()
        named_lane = lax.broadcasted_iota(jnp.int32, (1, LANES), 1)
        line = jnp.full((1, LANES), FAR, jnp.int32)
        for e in range(12):
            line = jnp.where(named_lane == e, rand_ref[e // 3, e % 3], line)
        idx_ref[...] = line
        idx_all[core, chip] = line

    def relayout(step, carry):
        blk, group = step >> 2, step & 3
        rows = x_ref[aligned(step, 16), :]
        rows = jnp.concatenate([rows[:, LANES * c:LANES * c + LANES] for c in range(16)], axis=0)
        moved = jnp.dot(perm, rows, preferred_element_type=jnp.float32).astype(jnp.bfloat16)
        for a in range(16):
            xs[16 * group + a, blk] = moved[16 * a:16 * a + 16]
        return carry
    with jax.named_scope("relayout"):
        lax.fori_loop(0, 16, relayout, 0)

    def start_idx(i, carry):
        idx_copy(chip ^ i, chip).start()
        return carry

    def start_row(i, carry):
        row_copy(chip ^ i, chip).start()
        return carry
    with jax.named_scope("barrier"):
        pl.semaphore_wait(barrier, 127)
    with jax.named_scope("issue_rows"):
        x_swap(core).start()
        lax.fori_loop(1, CHIPS, start_idx, 0, unroll=7)
        lax.fori_loop(1, CHIPS, start_row, 0, unroll=7)
        own_row = pltpu.make_async_copy(xs.at[chip], recv.at[pl.ds(4 * chip, 4)], loc.at[0])
        own_row.start()

    with jax.named_scope("wait_x"):
        own_x.wait()
        x_swap(core).wait_send()
        x_swap(1 - core).wait_recv()

    def project(t, carry):
        cols = aligned(t, TILE)
        for i in range(3):
            w_copy(i, t).wait()
        rows = xc[...]
        q_ref[:, cols] = jnp.dot(rows, w_buf[0, :, cols], preferred_element_type=jnp.float32).astype(jnp.bfloat16)
        k_ref[BLK:9 * BLK, cols] = jnp.dot(rows, w_buf[1, :, cols], preferred_element_type=jnp.float32).astype(jnp.bfloat16)
        v_ref[BLK:9 * BLK, cols] = jnp.dot(rows, w_buf[2, :, cols], preferred_element_type=jnp.float32).astype(jnp.bfloat16)
        return carry
    with jax.named_scope("project"):
        lax.fori_loop(0, 4, project, 0)

    def wait_idx(i, carry):
        idx_copy(chip ^ i, chip ^ i).wait()
        return carry
    with jax.named_scope("wait_idx"):
        lax.fori_loop(1, CHIPS, wait_idx, 0)
        idx_swap(core).start()
        idx_swap(core).wait_send()
        idx_swap(1 - core).wait_recv()
    with jax.named_scope("names"):
        ids = jnp.concatenate([idx_all[0, :, 0, :], idx_all[1, :, 0, :]], axis=0)
        published = [jnp.int32(0), jnp.int32(1), jnp.min(ids)]
        for s in range(3, 14):
            published.append(jnp.min(jnp.where(ids > published[-1], ids, FAR)))

    with jax.named_scope("slots"):
        near = [pltpu.make_async_copy(idx_all.at[c, chip], near_s.at[c], loc.at[1 + c]) for c in range(2)]
        for n in near:
            n.start()
        for n in near:
            n.wait()
        for b in range(8):
            for t in range(3):
                named = near_s[b // 4, 0, 3 * (b % 4) + t]
                at = jnp.int32(2)
                for h in published[2:]:
                    at = at + jnp.where(h < named, 1, 0)
                slot_s[3 * b + t] = at

    with jax.named_scope("issue_halos"):
        for kv in range(2):
            for side in range(2):
                halo(kv, side).start()

    def wait_row(i, carry):
        row_copy(chip ^ i, chip ^ i).wait()
        return carry
    with jax.named_scope("wait_rows"):
        lax.fori_loop(1, CHIPS, wait_row, 0)
        own_row.wait()

    with jax.named_scope("select"):
        for s in range(SLOTS):
            if s < 14:
                h = published[s]
                rows = recv[jnp.minimum((h >> 3) * 4 + (h & 3), 4 * CHIPS - 1)]
                sel[16 * s:16 * s + 16, :] = jnp.where(((h >> 2) & 1) == core, rows, jnp.zeros_like(rows))
            else:
                sel[16 * s:16 * s + 16, :] = jnp.zeros((16, LANES), jnp.bfloat16)
        swap = remote(sel, other, p_sem.at[0], p_sem.at[1], partner)
        swap.start()
        swap.wait()
    with jax.named_scope("publish"):
        moved = jnp.dot(perm, sel[...] + other[...], preferred_element_type=jnp.float32).astype(jnp.bfloat16)
        rows = jnp.concatenate([moved[16 * j:16 * j + 16] for j in range(16)], axis=1)
        out = [jnp.dot(rows, w_buf[i], preferred_element_type=jnp.float32) for i in (1, 2)]
        for j in range(PAIRS):
            cols = slice(LANES * j, LANES * j + LANES)
            kv = jnp.concatenate([out[0][:, cols], out[1][:, cols]], axis=1)
            gath[j, coord[2], coord[1], coord[0]] = kv.astype(jnp.bfloat16)

    def copies(j, stage, receive):
        order = ORDERS[j % 3]
        axis = order[stage]
        out = []
        for k in (1, 2, 3):
            to = lax.rem(coord[axis] + k, 4)
            at = list(coord)
            if receive:
                at[axis] = lax.rem(coord[axis] + 4 - k, 4)
            buf, at_j = (gath, j) if j < PAIRS else (gath_q, 0)
            ref = buf.at[(at_j,) + tuple(slice(None) if a in order[:stage] else at[a] for a in (2, 1, 0))]
            out.append(remote(ref, ref, g_send.at[j, stage, k - 1], g_recv.at[j, stage, k - 1],
                              dev + 2 * scale[axis] * (to - coord[axis])))
        return out

    def advance(j, stage):
        if stage:
            for c in copies(j, stage - 1, True):
                c.wait_recv()
        if stage < 3:
            for c in copies(j, stage, False):
                c.start()

    with jax.named_scope("gather0"):
        for j in range(PAIRS):
            advance(j, 0)
    with jax.named_scope("publish_queries"):
        gq = jnp.dot(rows, w_buf[0], preferred_element_type=jnp.float32)
        gq = jnp.concatenate([gq[t:t + 1, LANES * j:LANES * j + LANES] for t in range(2) for j in range(PAIRS)], axis=0)
        gath_q[0, coord[2], coord[1], coord[0]] = gq.astype(jnp.bfloat16)
        advance(PAIRS, 0)
    with jax.named_scope("gather1"):
        for j in ALL:
            advance(j, 1)
    with jax.named_scope("gather2"):
        for j in ALL:
            advance(j, 2)

    with jax.named_scope("wait_queries"):
        advance(PAIRS, 3)

    def unpack_queries(z, carry):
        moved = jnp.dot(perm, gath_q[0, z].reshape(TILE, LANES), preferred_element_type=jnp.float32).astype(jnp.bfloat16)
        for s in range(SLOTS):
            queries_t[s, aligned(z, 16), :] = moved[16 * s:16 * s + 16]
        return carry

    def glob_part(step, carry):
        sums, tops = [], []
        for t in range(4):
            j = 4 * step + t
            wave = 2 * step + t // 2
            cols = aligned(j, LANES)
            gq = jnp.concatenate([queries_t[j], queries_t[PAIRS + j]], axis=0)
            queries = split_heads(gq, LANES) * jnp.bfloat16(0.125)
            scores = lax.dot_general(k_ref[BLK:9 * BLK, cols], queries, NT, preferred_element_type=jnp.float32)
            top = jnp.max(scores, axis=0, keepdims=True)
            probs = jnp.exp(scores - top)
            total = jnp.sum(probs, axis=0, keepdims=True)
            out = lax.dot_general(probs.astype(jnp.bfloat16), v_ref[BLK:9 * BLK, cols], TN, preferred_element_type=jnp.float32)
            part[wave, :, LANES * (t % 2):LANES * (t % 2) + LANES] = join_heads(out, LANES)
            sums += [total[:, 0:LANES], total[:, LANES:TILE]]
            tops += [top[:, 0:LANES], top[:, LANES:TILE]]
        pad = [jnp.zeros((120, LANES), jnp.float32)]
        for u in range(2):
            stats = jnp.concatenate(sums[4 * u:4 * u + 4] + tops[4 * u:4 * u + 4] + pad, axis=0)
            part[2 * step + u, :, TILE:384] = stats.T

        def start_part(i, carry):
            to = 32 * step + (i ^ (chip & 31))

            @pl.when(to != chip)
            def _():
                part_copy(to, chip).start()
            return carry
        return lax.fori_loop(0, 32, start_part, carry)

    def part_copy(dst_chip, slot):
        return remote(part.at[dst_chip >> 4, aligned(dst_chip & 15, 8)], parts.at[slot], c_send, c_recv.at[slot], 2 * dst_chip + core)

    with jax.named_scope("globpart"):
        lax.fori_loop(0, 4, unpack_queries, 0)
        lax.fori_loop(0, 2, glob_part, 0)
        own_part = pltpu.make_async_copy(part.at[chip >> 4, aligned(chip & 15, 8)], parts.at[chip], loc.at[1])
        own_part.start()

    with jax.named_scope("halo"):
        for kv in range(2):
            for side in range(2):
                halo(kv, side).wait()

    key = lax.broadcasted_iota(jnp.int32, (3 * BLK, 1), 0)

    def o_copy(wave, rows_of, cols_of):
        return remote(o_ref.at[aligned(rows_of, TILE), aligned(wave, TILE)],
                      full_ref.at[:, aligned(cols_of * 4 + wave, TILE)], o_send.at[wave], o_recv.at[wave], partner)

    def one_wave(wave, carry):
        with jax.named_scope("wait_wave"):
            for w in range(4):
                @pl.when(wave == w)
                def _():
                    for j in (2 * w, 2 * w + 1):
                        advance(j, 3)

        def unpack(z, carry):
            for t in range(2):
                rows = gath[2 * wave + t, z].reshape(TILE, TILE)
                moved = jnp.dot(perm, rows, preferred_element_type=jnp.float32).astype(jnp.bfloat16)
                for s in range(14):
                    hot[2 * wave + t, s, 16 * z:16 * z + 16, :] = moved[s * 16:s * 16 + 16]
            return carry
        with jax.named_scope("unpack"):
            for z in range(4):
                unpack(z, 0)

        with jax.named_scope("blocks"):
            for b in range(8):
                named = [0, 1] + [slot_s[3 * b + t] for t in range(3)]
                rows = slice(b * BLK, b * BLK + BLK)
                near = slice(b * BLK, b * BLK + 3 * BLK)
                for t in range(2):
                    j = 2 * wave + t
                    cols = aligned(j, LANES)
                    queries = split_heads(q_ref[rows, cols], BLK) * jnp.bfloat16(0.125)
                    keys = jnp.concatenate([k_ref[near, cols]] + [hot[j, s, :, 0:LANES] for s in named], axis=0)
                    vals = jnp.concatenate([v_ref[near, cols]] + [hot[j, s, :, LANES:TILE] for s in named], axis=0)
                    scores = lax.dot_general(keys, queries, NT, preferred_element_type=jnp.float32)
                    if b == 2:
                        bias = jnp.where((key < BLK) & (chip == 0), NEG, 0.0)
                    elif b == 7:
                        bias = jnp.where((key >= 2 * BLK) & (chip == CHIPS - 1), NEG, 0.0)
                    if b in (2, 7):
                        scores = jnp.concatenate([scores[:3 * BLK] + bias, scores[3 * BLK:]], axis=0)
                    top = jnp.max(scores, axis=0, keepdims=True)
                    probs = jnp.exp(scores - top)
                    probs = probs * (1.0 / jnp.sum(probs, axis=0, keepdims=True))
                    out = lax.dot_general(probs.astype(jnp.bfloat16), vals, TN, preferred_element_type=jnp.float32)
                    o_ref[rows, cols] = join_heads(out, BLK).astype(jnp.bfloat16)
        own_o(wave).start()
        o_copy(wave, 1 - core, core).start()
        return carry

    def own_o(wave):
        return pltpu.make_async_copy(o_ref.at[aligned(core, TILE), aligned(wave, TILE)], full_ref.at[:, aligned(4 * core + wave, TILE)], own_sem.at[wave])

    lax.fori_loop(0, 4, one_wave, 0)

    with jax.named_scope("local"):
        for j in ALL:
            for stage in range(3):
                for c in copies(j, stage, False):
                    c.wait_send()

    def wait_part(i, carry):
        part_copy(chip ^ i, chip ^ i).wait()
        return carry
    with jax.named_scope("wait_parts"):
        lax.fori_loop(1, CHIPS, wait_part, 0)
        own_part.wait()

    with jax.named_scope("combine"):
        top = lax.fori_loop(0, CHIPS, lambda i, t: jnp.maximum(t, parts[i, :, TILE:384]), jnp.full((8, LANES), NEG, jnp.float32), unroll=8)

        def add(i, carry):
            num, den = carry
            weight = pltpu.roll(jnp.exp(parts[i, :, TILE:384] - top), 124, 1)
            wide = jnp.concatenate([jnp.broadcast_to(weight[:, t:t + 1], (8, HEAD_DIM)) for t in range(4)], axis=1)
            return num + wide * parts[i, :, 0:TILE], den + weight * parts[i, :, TILE:384]
        num, den = lax.fori_loop(0, CHIPS, add, (jnp.zeros((8, TILE), jnp.float32), jnp.zeros((8, LANES), jnp.float32)), unroll=8)
        wide = jnp.concatenate([jnp.broadcast_to(den[:, t:t + 1], (8, HEAD_DIM)) for t in range(4)], axis=1)
        piece[...] = (num / wide).astype(jnp.bfloat16)

    def glob_slice(src_chip, src_core):
        return glob.at[aligned(src_chip % 16, 8), aligned(src_core * 4 + src_chip // 16, TILE)]

    def glob_copy(src_chip, src_core):
        return remote(piece, glob_slice(src_chip, src_core), e_send, e_recv.at[2 * src_chip + src_core], 0)

    @pl.when(dev != 0)
    def _():
        glob_copy(chip, core).start()

    with jax.named_scope("wait_o"):
        for wave in range(4):
            own_o(wave).wait()
            o_copy(wave, 1 - core, core).wait_send()
            o_copy(wave, core, 1 - core).wait_recv()
    with jax.named_scope("tail"):
        @pl.when(dev != 0)
        def _():
            glob_copy(chip, core).wait_send()

        @pl.when(dev == 0)
        def _():
            copy = pltpu.make_async_copy(piece, glob_slice(0, 0), loc.at[0])
            copy.start()
            copy.wait()

            def wait_glob(i, carry):
                glob_copy(i // 2, i % 2).wait_recv()
                return carry
            lax.fori_loop(1, LANES, wait_glob, 0)
            full_ref[0:LANES, :] = glob[...]


def out_kernel(rows_ref, w_ref, y_ref):
    y_ref[...] = lax.dot_general(rows_ref[...], w_ref[...], NT, preferred_element_type=jnp.float32).astype(jnp.bfloat16)


def project_out(rows, wo):
    tile = TILE
    return pl.pallas_call(
        out_kernel, grid=(WIDTH // tile,),
        in_specs=[pl.BlockSpec(rows.shape, lambda j: (0, 0)), pl.BlockSpec((tile, WIDTH), lambda j: (j, 0))],
        out_specs=pl.BlockSpec((rows.shape[0], tile), lambda j: (0, j)),
        out_shape=jax.ShapeDtypeStruct(rows.shape, jnp.bfloat16), name="project_out",
        compiler_params=pltpu.CompilerParams(vmem_limit_bytes=16 << 20),
        cost_estimate=pl.CostEstimate(flops=2 * rows.shape[0] * WIDTH * WIDTH, bytes_accessed=10 << 20, transcendentals=0),
    )(rows, wo)


def attend(x, rand_idx, wq, wk, wv):
    vmem = pl.BlockSpec(memory_space=VMEM)
    hbm = pl.BlockSpec(memory_space=pl.ANY)
    dma = pltpu.SemaphoreType.DMA
    bf16, f32 = jnp.bfloat16, jnp.float32
    return pl.pallas_call(
        kernel,
        out_shape=jax.ShapeDtypeStruct((TILE, WIDTH), bf16),
        in_specs=[vmem, pl.BlockSpec(memory_space=pltpu.SMEM), hbm, hbm, hbm], out_specs=vmem,
        scratch_shapes=[
            VMEM((1, LANES), jnp.int32),
            VMEM((CHIPS, 4, 16, LANES), bf16), VMEM((512, WIDTH), bf16), VMEM((4 * CHIPS, 16, LANES), bf16),
            VMEM((3, WIDTH, HALF), bf16), VMEM((2, CHIPS, 1, LANES), jnp.int32), VMEM((TILE, LANES), bf16), VMEM((TILE, LANES), bf16),
            VMEM((512, HALF), bf16), VMEM((640, HALF), bf16), VMEM((640, HALF), bf16),
            VMEM((PAIRS, 4, 4, 4, SLOTS, TILE), bf16), VMEM((PAIRS, SLOTS, BLK, TILE), bf16), VMEM((512, HALF), bf16),
            VMEM((4, LANES, 384), f32), VMEM((CHIPS, 8, 384), f32), VMEM((LANES, WIDTH), bf16), VMEM((8, TILE), bf16),
            pltpu.SMEM((2, 1, LANES), jnp.int32), pltpu.SMEM((24,), jnp.int32),
            VMEM((1, 4, 4, 4, SLOTS, LANES), bf16), VMEM((SLOTS, BLK, LANES), bf16),
            dma, dma((CHIPS,)), dma((3,)), dma((CHIPS,)), dma((2,)), dma((2, 2)), dma((2, 2)), dma((3,)), dma((3, 4)), dma((2,)),
            dma((PAIRS + 1, 3, 3)), dma((PAIRS + 1, 3, 3)), dma, dma((CHIPS,)), dma((4,)), dma((4,)), dma, dma((LANES,)), dma((4,))],
        compiler_params=pltpu.CompilerParams(has_side_effects=True, collective_id=0, vmem_limit_bytes=44 << 20), name="attend",
    )(x, rand_idx, wq, wk, wv)


def solution(mesh):
    row_spec = P(("batch", "seq"), None)
    rep_spec = P(None, None)

    def local_fn(tokens, w_query, w_key, w_value, w_out, rand_idx):
        return project_out(attend(tokens, rand_idx, w_query, w_key, w_value), w_out)

    return jax.shard_map(local_fn, mesh=mesh, in_specs=(row_spec, rep_spec, rep_spec, rep_spec, rep_spec, row_spec), out_specs=row_spec, check_vma=False)
```
